32 devices in a mesh: grp: 2 (over x), ma: 16 (over z, y, core).
Axes of the slice: x: 2, y: 2, z: 4, core: 2. Of those that a mesh axis runs over, the one named last changes fastest.
Arguments:
- tbar_alm: bfloat16 [128, 8, 2, 257], P('ma', 'grp'), parts along dimension 1, may hold values from -6 to 6
- twf_alm: bfloat16 [128, 8, 2, 257], P('ma', 'grp'), parts along dimension 1, may hold values from -6 to 6
- legendre: bfloat16 [128, 257, 16], P('ma'), may hold values from -0.375 to 0.375
- m_slots: int32 [128], replicated, may hold values from 0 to 127, each once
- cycle_order: int32 [16], replicated, may hold values from 0 to 15, each once
- colatitude: float32 [16], replicated, may hold values from 0.35 to 2.79
- cycle_weight: float32 [16], replicated, may hold values from 0.25 to 1
- pixel_mask: int32 [16, 4096], P('ma'), may hold values from 0 to 3
Outputs:
- gradient: float32 [128, 8, 2, 257], P('ma', 'grp'), parts along dimension 1
- curl: float32 [128, 8, 2, 257], P('ma', 'grp'), parts along dimension 1
The draws below stay inside these ranges and needn't reach their ends.
There are 2 independent parts, one for each index of `grp`. The reference program is written for one: setup_inputs(seed, part) draws one part's arguments, and reference() takes and returns one part's arrays. A program takes and returns all parts, laid end to end along the dimension named above; an argument that names none is the same for every part. Nothing has to cross between parts.
Inputs may be any that keep to these rules, and one draw needn't show every extreme that they name: Pair p holds the orders m_slots[p] and 255 - m_slots[p]; each value appears once. Cycle slot i holds cycle cycle_order[i]; each value appears once.
All inputs are finite; a program needn't handle non-finite values.
Results may differ from the reference program's by a relative error of at most 0.017.
Values may be sent and summed in bfloat16 or wider, within the bound.
A program may use at most 128 MiB of HBM per device.

```python
import math
import jax
import jax.numpy as jnp
from jax import lax

MODES = 256
PAIRS = 128
ROWS = 257
CYCLES = 16
NPHI = 4096
SIMS = 4


def touch_ends(drawn, stream_key, smallest, high):
    extent = drawn.shape
    spot = [jax.random.randint(jax.random.fold_in(stream_key, axis), (), 0, extent[axis]) for axis in range(len(extent))]
    drawn = drawn.at[tuple(spot)].set(smallest)
    longest = extent.index(max(extent))
    spot[longest] = (spot[longest] + 1) % extent[longest]
    return drawn.at[tuple(spot)].set(high)


def levels(stream_key, extent, split, low, largest):
    level, own = 1.0, jax.random.fold_in(stream_key, 6)
    for position, parts in split:
        steps = jnp.exp(jax.random.uniform(jax.random.fold_in(own, position), (parts,), jnp.float32, low / len(split), largest / len(split)))
        level = level * jnp.repeat(steps, extent[position] // parts).reshape([-1 if axis == position else 1 for axis in range(len(extent))])
    return level


def scatter_about(stream_key, extent, deviation, reach, split=(), dtype=jnp.bfloat16):
    drawn = deviation * jax.random.normal(stream_key, extent, jnp.float32)
    if split:
        drawn = drawn * levels(stream_key, extent, split, -0.22, 0.18)
    return jnp.clip(drawn, -reach, reach).astype(dtype)


def setup_inputs(seed: int = 0, part: int = 0) -> dict:
    seeds = jax.random.split(jax.random.key(seed), 9)
    part_splits = jax.random.split(jax.random.fold_in(seeds[8], part), 9)
    tbar_alm = scatter_about(part_splits[0], (PAIRS, SIMS, 2, ROWS), 1.0, 6.0, ((0, 16),))
    twf_alm = scatter_about(part_splits[1], (PAIRS, SIMS, 2, ROWS), 1.0, 6.0, ((0, 16),))
    legendre = scatter_about(seeds[2], (PAIRS, ROWS, CYCLES), ROWS ** -0.5, 0.375, ((0, 16),))
    m_slots = jax.random.permutation(seeds[3], PAIRS).astype(jnp.int32)
    cycle_order = jax.random.permutation(seeds[4], CYCLES).astype(jnp.int32)
    colatitude = jnp.clip(jax.random.uniform(seeds[5], (CYCLES,), jnp.float32, 0.35, 2.79), 0.35, 2.79)
    cycle_weight = jnp.clip(jnp.exp(jax.random.uniform(seeds[6], (CYCLES,), jnp.float32, math.log(0.25), math.log(1.0))), 0.25, 1.0)
    pixel_mask = touch_ends(jax.random.randint(seeds[7], (CYCLES, NPHI), 0, 4), jax.random.fold_in(seeds[7], 1), 0, 3).astype(jnp.int32)
    return {"tbar_alm": tbar_alm, "twf_alm": twf_alm, "legendre": legendre, "m_slots": m_slots, "cycle_order": cycle_order, "colatitude": colatitude, "cycle_weight": cycle_weight, "pixel_mask": pixel_mask}


def rounded(values):
    return lax.optimization_barrier(values.astype(jnp.bfloat16)).astype(jnp.float32)

def pair_layout(small_orders, mode_count):
    row_index = lax.broadcasted_iota(jnp.int32, (small_orders.shape[0], mode_count + 1), 1)
    smaller = small_orders[:, None]
    upper_half = row_index >= mode_count - smaller
    degree = jnp.where(upper_half, row_index - 1, smaller + row_index)
    orders = jnp.where(upper_half, mode_count - 1 - smaller, smaller + 0 * row_index)
    return (upper_half, degree.astype(jnp.float32), orders.astype(jnp.float32))

def raising(degree, orders):
    square = (degree * degree - orders * orders) * (2.0 * degree + 1.0) / jnp.maximum(2.0 * degree - 1.0, 1.0)
    return jnp.where(degree > orders, jnp.sqrt(jnp.where(degree > orders, square, 0.0)), 0.0)

def synthesis_sets(tbar_alm, twf_alm, degree, raising_factor, mode_count):
    wiener = twf_alm.astype(jnp.float32)
    scaled = (raising_factor / mode_count)[:, None, None, :] * wiener
    raised = jnp.concatenate([scaled[..., 1:], jnp.zeros_like(scaled[..., :1])], axis=-1)
    stacked = jnp.stack([tbar_alm.astype(jnp.float32), wiener, (degree / mode_count)[:, None, None, :] * wiener, raised], axis=2)
    return stacked.reshape(stacked.shape[0], stacked.shape[1], 8, stacked.shape[4]).astype(jnp.bfloat16)

def mode_columns(small_orders, mode_count):
    return jnp.stack([small_orders, mode_count - 1 - small_orders], axis=1).reshape(-1)

def fourier_table(orders_int, pixel_count):
    pixel_index = lax.broadcasted_iota(jnp.int32, (orders_int.shape[0], pixel_count), 1)
    turns = orders_int[:, None] * pixel_index % pixel_count
    radians = turns.astype(jnp.float32) * (2.0 * math.pi / pixel_count)
    return jnp.stack([jnp.cos(radians), -jnp.sin(radians)], axis=0).astype(jnp.bfloat16)

def combine_modes(legendre_sums, orders_int, cos_cycle, sin_cycle, mode_count):
    orders_real = orders_int.astype(jnp.float32)
    inv_sin = 1.0 / sin_cycle
    ratio = (orders_real / mode_count)[:, None]
    theta_real = (cos_cycle * legendre_sums[:, 4] - legendre_sums[:, 6]) * inv_sin
    theta_imag = (cos_cycle * legendre_sums[:, 5] - legendre_sums[:, 7]) * inv_sin
    phi_real = -ratio * legendre_sums[:, 3] * inv_sin
    phi_imag = ratio * legendre_sums[:, 2] * inv_sin
    weight = (jnp.where(orders_int == 0, 1.0, 2.0) * mode_count ** (-0.5))[:, None]
    stacked = jnp.stack([legendre_sums[:, 0], legendre_sums[:, 1], theta_real, theta_imag, phi_real, phi_imag], axis=1)
    return (stacked * weight).astype(jnp.bfloat16)

def analysis_sets(spectra, colatitude, cycle_weight):
    with_cos = cycle_weight * jnp.cos(colatitude) / jnp.sin(colatitude)
    with_sin = cycle_weight / jnp.sin(colatitude)
    stacked = jnp.stack([spectra[:, 0] * with_cos, spectra[:, 0] * with_sin, spectra[:, 1] * with_cos, spectra[:, 1] * with_sin], axis=1)
    return stacked.reshape(spectra.shape[0], 8, spectra.shape[3], spectra.shape[4]).astype(jnp.bfloat16)

def estimate(merged, degree, orders, raising_factor, mode_count, cycle_count):
    level = degree[:, None, :]
    azimuth = orders[:, None, :]
    factor = raising_factor[:, None, :]

    def previous(values):
        return jnp.concatenate([jnp.zeros_like(values[..., :1]), values[..., :-1]], axis=-1)
    grad_real = level * merged[:, :, 0] - factor * previous(merged[:, :, 2]) + azimuth * merged[:, :, 7]
    grad_imag = level * merged[:, :, 1] - factor * previous(merged[:, :, 3]) - azimuth * merged[:, :, 6]
    curl_real = level * merged[:, :, 4] - factor * previous(merged[:, :, 6]) - azimuth * merged[:, :, 3]
    curl_imag = level * merged[:, :, 5] - factor * previous(merged[:, :, 7]) + azimuth * merged[:, :, 2]
    scale = (mode_count / cycle_count) ** 0.5 / jnp.sqrt(jnp.maximum(level * (level + 1.0), 1.0))
    scale = scale[:, :, None, :]
    return (jnp.stack([grad_real, grad_imag], axis=2) * scale, jnp.stack([curl_real, curl_imag], axis=2) * scale)

def reference(tbar_alm, twf_alm, legendre, m_slots, cycle_order, colatitude, cycle_weight, pixel_mask):
    upper_half, degree, orders = pair_layout(m_slots, MODES)
    raising_factor = raising(degree, orders)
    coeff_sets = rounded(synthesis_sets(tbar_alm, twf_alm, degree, raising_factor, MODES))
    halves = jnp.stack([jnp.logical_not(upper_half), upper_half], axis=1).astype(jnp.float32)
    blocks = PAIRS // 8

    def synth_block(block_items):
        block_sets, block_halves, block_table = block_items
        masked = block_sets[:, None] * block_halves[:, :, None, None, :]
        return jnp.einsum('phsck,pkr->scphr', masked, block_table.astype(jnp.float32))
    legendre_sums = lax.map(synth_block, (coeff_sets.reshape(blocks, 8, SIMS, 8, ROWS), halves.reshape(blocks, 8, 2, ROWS), legendre.reshape(blocks, 8, ROWS, CYCLES)))
    legendre_sums = jnp.transpose(legendre_sums, (1, 2, 0, 3, 4, 5)).reshape(SIMS, 8, MODES, CYCLES)
    legendre_sums = jnp.take(legendre_sums, cycle_order, axis=3)
    slot_theta = jnp.take(colatitude, cycle_order)
    orders_all = mode_columns(m_slots, MODES)
    fourier = combine_modes(legendre_sums, orders_all, jnp.cos(slot_theta), jnp.sin(slot_theta), MODES)
    fourier = rounded(fourier).reshape(SIMS, 3, 2, MODES, CYCLES)
    dft_table = rounded(fourier_table(orders_all, NPHI))
    cycle_maps = jnp.einsum('sqemr,emj->sqrj', fourier, dft_table)
    products = rounded(pixel_mask.astype(jnp.float32) * cycle_maps[:, 0:1] * cycle_maps[:, 1:3])
    spectra = rounded(jnp.einsum('sqrj,emj->sqemr', products, dft_table) * NPHI ** (-0.5))
    inverse = jnp.zeros((CYCLES,), jnp.int32).at[cycle_order].set(lax.iota(jnp.int32, CYCLES))
    spectra = jnp.take(spectra, inverse, axis=4)
    weighted = rounded(analysis_sets(spectra, colatitude, cycle_weight))
    weighted = jnp.moveaxis(weighted.reshape(SIMS, 8, blocks, 8, 2, CYCLES), 2, 0)

    def analysis_block(block_items):
        block_weighted, block_table, block_halves, block_degree, block_orders, block_raising = block_items
        projected = jnp.einsum('scphr,pkr->phsck', block_weighted, block_table.astype(jnp.float32))
        merged = lax.optimization_barrier(jnp.sum(projected * block_halves[:, :, None, None, :], axis=1))
        return estimate(merged, block_degree, block_orders, block_raising, MODES, CYCLES)
    gradient, curl = lax.map(analysis_block, (weighted, legendre.reshape(blocks, 8, ROWS, CYCLES), halves.reshape(blocks, 8, 2, ROWS), degree.reshape(blocks, 8, ROWS), orders.reshape(blocks, 8, ROWS), raising_factor.reshape(blocks, 8, ROWS)))
    return (gradient.reshape(PAIRS, SIMS, 2, ROWS), curl.reshape(PAIRS, SIMS, 2, ROWS))
```

```python
import math

import functools

import jax
import jax.numpy as jnp
import numpy as np
from jax import lax
from jax.experimental import pallas as pl
from jax.experimental.pallas import tpu as pltpu
from jax.sharding import PartitionSpec as P


def pair_layout(small_orders, mode_count):
    row_index = lax.broadcasted_iota(jnp.int32, (small_orders.shape[0], mode_count + 1), 1)
    smaller = small_orders[:, None]
    upper_half = row_index >= mode_count - smaller
    degree = jnp.where(upper_half, row_index - 1, smaller + row_index)
    orders = jnp.where(upper_half, mode_count - 1 - smaller, smaller + 0 * row_index)
    return (upper_half, degree.astype(jnp.float32), orders.astype(jnp.float32))


def raising(degree, orders):
    square = (
        (degree * degree - orders * orders)
        * (2.0 * degree + 1.0)
        / jnp.maximum(2.0 * degree - 1.0, 1.0)
    )
    return jnp.where(degree > orders, jnp.sqrt(jnp.where(degree > orders, square, 0.0)), 0.0)


def synthesis_sets(tbar_alm, twf_alm, degree, raising_factor, mode_count):
    wiener = twf_alm.astype(jnp.float32)
    scaled = (raising_factor / mode_count)[:, None, None, :] * wiener
    raised = jnp.concatenate([scaled[..., 1:], jnp.zeros_like(scaled[..., :1])], axis=-1)
    stacked = jnp.stack(
        [
            tbar_alm.astype(jnp.float32),
            wiener,
            (degree / mode_count)[:, None, None, :] * wiener,
            raised,
        ],
        axis=2,
    )
    return stacked.reshape(stacked.shape[0], stacked.shape[1], 8, stacked.shape[4]).astype(
        jnp.bfloat16
    )


def mode_columns(small_orders, mode_count):
    return jnp.stack([small_orders, mode_count - 1 - small_orders], axis=1).reshape(-1)


def fourier_table(orders_int, pixel_count):
    pixel_index = lax.broadcasted_iota(jnp.int32, (orders_int.shape[0], pixel_count), 1)
    turns = orders_int[:, None] * pixel_index % pixel_count
    radians = turns.astype(jnp.float32) * (2.0 * math.pi / pixel_count)
    return jnp.stack([jnp.cos(radians), -jnp.sin(radians)], axis=0).astype(jnp.bfloat16)


def combine_modes(legendre_sums, orders_int, cos_cycle, sin_cycle, mode_count):
    orders_real = orders_int.astype(jnp.float32)
    inv_sin = 1.0 / sin_cycle
    ratio = (orders_real / mode_count)[:, None]
    theta_real = (cos_cycle * legendre_sums[:, 4] - legendre_sums[:, 6]) * inv_sin
    theta_imag = (cos_cycle * legendre_sums[:, 5] - legendre_sums[:, 7]) * inv_sin
    phi_real = -ratio * legendre_sums[:, 3] * inv_sin
    phi_imag = ratio * legendre_sums[:, 2] * inv_sin
    weight = (jnp.where(orders_int == 0, 1.0, 2.0) * mode_count ** (-0.5))[:, None]
    stacked = jnp.stack(
        [legendre_sums[:, 0], legendre_sums[:, 1], theta_real, theta_imag, phi_real, phi_imag],
        axis=1,
    )
    return (stacked * weight).astype(jnp.bfloat16)


def analysis_sets(spectra, colatitude, cycle_weight):
    with_cos = cycle_weight * jnp.cos(colatitude) / jnp.sin(colatitude)
    with_sin = cycle_weight / jnp.sin(colatitude)
    stacked = jnp.stack(
        [
            spectra[:, 0] * with_cos,
            spectra[:, 0] * with_sin,
            spectra[:, 1] * with_cos,
            spectra[:, 1] * with_sin,
        ],
        axis=1,
    )
    return stacked.reshape(spectra.shape[0], 8, spectra.shape[3], spectra.shape[4]).astype(
        jnp.bfloat16
    )


def estimate(merged, degree, orders, raising_factor, mode_count, cycle_count):
    level = degree[:, None, :]
    azimuth = orders[:, None, :]
    factor = raising_factor[:, None, :]

    def previous(values):
        return jnp.concatenate([jnp.zeros_like(values[..., :1]), values[..., :-1]], axis=-1)

    grad_real = (
        level * merged[:, :, 0] - factor * previous(merged[:, :, 2]) + azimuth * merged[:, :, 7]
    )
    grad_imag = (
        level * merged[:, :, 1] - factor * previous(merged[:, :, 3]) - azimuth * merged[:, :, 6]
    )
    curl_real = (
        level * merged[:, :, 4] - factor * previous(merged[:, :, 6]) - azimuth * merged[:, :, 3]
    )
    curl_imag = (
        level * merged[:, :, 5] - factor * previous(merged[:, :, 7]) + azimuth * merged[:, :, 2]
    )
    scale = (mode_count / cycle_count) ** 0.5 / jnp.sqrt(jnp.maximum(level * (level + 1.0), 1.0))
    scale = scale[:, :, None, :]
    return (
        jnp.stack([grad_real, grad_imag], axis=2) * scale,
        jnp.stack([curl_real, curl_imag], axis=2) * scale,
    )


def shards(tbar_alm, twf_alm, legendre, m_slots, cycle_order, colatitude, cycle_weight, pixel_mask):
    pairs_dev = tbar_alm.shape[0]
    row_count = tbar_alm.shape[3]
    mode_count = row_count - 1
    cycle_count = legendre.shape[2]
    cycle_dev = pixel_mask.shape[0]
    pixel_count = pixel_mask.shape[1]
    device_slot = lax.axis_index("ma")
    local_small = lax.dynamic_slice_in_dim(m_slots, device_slot * pairs_dev, pairs_dev)
    upper_half, degree, orders = pair_layout(local_small, mode_count)
    raising_factor = raising(degree, orders)
    coeff_sets = synthesis_sets(tbar_alm, twf_alm, degree, raising_factor, mode_count)
    halves = jnp.stack([jnp.logical_not(upper_half), upper_half], axis=1)
    masked = coeff_sets[:, None] * halves.astype(jnp.bfloat16)[:, :, None, None, :]
    legendre_sums = jnp.einsum(
        "phsck,pkr->scphr", masked, legendre, preferred_element_type=jnp.float32
    )
    legendre_sums = jnp.take(legendre_sums, cycle_order, axis=4)
    legendre_sums = legendre_sums.reshape(legendre_sums.shape[0], 8, 2 * pairs_dev, cycle_count)
    all_orders = mode_columns(m_slots, mode_count)
    dft_table = fourier_table(all_orders, pixel_count)
    pixel_weights = pixel_mask.astype(jnp.float32)
    slot_theta = jnp.take(colatitude, cycle_order)
    local_orders = mode_columns(local_small, mode_count)
    outgoing = combine_modes(
        legendre_sums, local_orders, jnp.cos(slot_theta), jnp.sin(slot_theta), mode_count
    )
    fourier = lax.all_to_all(outgoing, "ma", split_axis=3, concat_axis=2, tiled=True)
    fourier = fourier.reshape(fourier.shape[0], 3, 2, mode_count, cycle_dev)
    cycle_maps = jnp.einsum(
        "sqemr,emj->sqrj", fourier, dft_table, preferred_element_type=jnp.float32
    )
    products = (pixel_weights * cycle_maps[:, 0:1] * cycle_maps[:, 1:3]).astype(jnp.bfloat16)
    spectra = jnp.einsum("sqrj,emj->sqemr", products, dft_table, preferred_element_type=jnp.float32)
    received = (spectra * pixel_count ** (-0.5)).astype(jnp.bfloat16)
    returned = lax.all_to_all(received, "ma", split_axis=3, concat_axis=4, tiled=True)
    inverse = (
        jnp.zeros((cycle_count,), jnp.int32).at[cycle_order].set(lax.iota(jnp.int32, cycle_count))
    )
    spectra = jnp.take(returned, inverse, axis=4).astype(jnp.float32)
    weighted = analysis_sets(spectra, colatitude, cycle_weight)
    weighted = weighted.reshape(weighted.shape[0], 8, pairs_dev, 2, cycle_count)
    projected = jnp.einsum(
        "scphr,pkr->phsck", weighted, legendre, preferred_element_type=jnp.float32
    )
    merged = jnp.sum(projected * halves.astype(jnp.float32)[:, :, None, None, :], axis=1)
    return estimate(merged, degree, orders, raising_factor, mode_count, cycle_count)


LANES = 128
F32 = jnp.float32
BF16 = jnp.bfloat16


def split_tables(mode_count, pixel_count, sims):
    m = np.arange(mode_count)[None, :]
    low = np.arange(LANES)[:, None]
    high = np.repeat(np.arange(pixel_count // LANES), sims)[:, None] * LANES
    fine = (m * low % pixel_count) * (2.0 * math.pi / pixel_count)
    coarse = (m * high % pixel_count) * (2.0 * math.pi / pixel_count)
    cos_high = np.cos(coarse).astype(np.float32)
    sin_high = np.sin(coarse).astype(np.float32)

    def halves(values):
        upper = values.astype(BF16)
        return upper, (values - upper.astype(np.float32)).astype(BF16)

    return np.concatenate(
        [np.cos(fine).astype(BF16), (-np.sin(fine)).astype(BF16)]
        + list(halves(cos_high))
        + list(halves(sin_high)),
        axis=0,
    )


def iota(shape, axis):
    return lax.broadcasted_iota(jnp.int32, shape, axis)


def div(values, size):
    return values >> (size.bit_length() - 1)


def mod(values, size):
    return values & (size - 1)


def one_hot(condition):
    return jnp.where(condition, 1.0, 0.0).astype(BF16)


def dot(left, right):
    return jnp.dot(left, right, preferred_element_type=F32)


def dot_t(left, right):
    return lax.dot_general(left, right, (((1,), (1,)), ((), ())), preferred_element_type=F32)


def fused_kernel(
    n, modes, rows, cycles, pixels, sims,
    slots_hbm, cycle_hbm, colat_hbm, weight_hbm, row_hbm, tbar_hbm, twf_hbm, leg_hbm, mask_hbm,
    table_hbm, grad_ref, curl_ref, slots_s, cycle_s, colat_s, weight_s, slots_v,
    tbar_ref, twf_ref, leg_ref, mask_ref, table_v, leg_all, prev_all, send_f, recv_f, send_p, recv_p,
    load_sem, move_sem,
):
    me = lax.axis_index("ma")
    pairs, padded = tbar_ref.shape[0], rows
    block = 2 * pairs
    comps = 2 * sims
    span = 2 * cycles
    total = pairs * span
    loads = [
        pltpu.make_async_copy(source, target, load_sem.at[at])
        for at, (source, target) in enumerate(
            [(slots_hbm, slots_s), (colat_hbm, colat_s), (cycle_hbm, cycle_s),
             (leg_hbm, leg_ref), (tbar_hbm, tbar_ref), (twf_hbm, twf_ref),
             (table_hbm, table_v), (mask_hbm, mask_ref), (row_hbm, slots_v), (weight_hbm, weight_s)]
        )
    ]
    for load in loads[:6]:
        load.start()
    barrier = pltpu.get_barrier_semaphore()
    for off in range(1, n):
        pl.semaphore_signal(
            barrier, inc=1, device_id={"ma": lax.rem(me + off, n)},
            device_id_type=pl.DeviceIdType.MESH,
        )
    for load in loads[6:]:
        load.start()
    for load in loads[:3]:
        load.wait()

    row_shape = (pairs, padded)
    smaller = jnp.zeros(row_shape, jnp.int32)
    for p in range(pairs):
        smaller = jnp.where(iota(row_shape, 0) == p, slots_s[me * pairs + p], smaller)
    k = iota(row_shape, 1)
    upper = k >= modes - smaller
    degree = jnp.where(upper, k - 1, smaller + k).astype(F32)
    orders = jnp.where(upper, modes - 1 - smaller, smaller).astype(F32)
    eps = raising(degree, orders)
    upper_f = jnp.where(upper, 1.0, 0.0)
    lower_f = 1.0 - upper_f

    colat = jnp.zeros((cycles, 4 * comps), F32)
    for r in range(cycles):
        colat = jnp.where(iota(colat.shape, 0) == r, colat_s[r], colat)
    csc = 1.0 / jnp.sin(colat)
    cot = jnp.cos(colat) * csc
    lane = iota(colat.shape, 1)
    group = div(lane, comps)
    part_a = jnp.where(group == 0, 1.0, jnp.where(group == 1, cot, 0.0))
    part_m = jnp.where(group == 2, csc, 0.0)
    part_b = jnp.where(group == 1, csc, 0.0)

    blank = jnp.zeros((comps, padded), F32)
    pieces = []
    for load in loads[3:6]:
        load.wait()
    for p in range(pairs):
        tbar = jnp.concatenate([tbar_ref[p, s].astype(F32) for s in range(sims)], axis=0)
        twf = jnp.concatenate([twf_ref[p, s].astype(F32) for s in range(sims)], axis=0)
        deg_p, eps_p = degree[p : p + 1] / modes, eps[p : p + 1] / modes
        sets_a = jnp.concatenate([tbar, deg_p * twf, twf, blank], axis=0)
        sets_b = jnp.concatenate([blank, -(eps_p * twf), blank, blank], axis=0)
        leg = leg_ref[p].astype(F32)
        prev = jnp.concatenate([jnp.zeros_like(leg[:, :1]), leg[:, : rows - 1]], axis=1)
        low, high = lower_f[p : p + 1], upper_f[p : p + 1]
        leg = jnp.concatenate([leg * low, leg * high], axis=0).astype(BF16)
        prev = jnp.concatenate([prev * low, prev * high], axis=0).astype(BF16)
        leg_all[pl.ds(p * span, span), :] = leg
        prev_all[pl.ds(p * span, span), :] = prev
        out_a = dot_t(leg, sets_a.astype(BF16))
        out_b = dot_t(prev, sets_b.astype(BF16))
        for h in range(2):
            small = slots_s[me * pairs + p]
            order = modes - 1 - small if h else small
            norm = jnp.where(order == 0, 1.0, 2.0) * modes ** (-0.5)
            ratio = order.astype(F32) / modes
            rng = slice(h * cycles, (h + 1) * cycles)
            pieces.append((out_a[rng] * (part_a + part_m * ratio) + out_b[rng] * part_b) * norm)
    fourier = jnp.concatenate(pieces, axis=0).astype(BF16)

    base_shape = (block, total)
    row = iota(base_shape, 0)
    base = iota(base_shape, 1) - (mod(row, pairs) * span + div(row, pairs) * cycles)
    place = jnp.concatenate(
        [jnp.where(base == cycle_s[i], 1.0, 0.0) for i in range(cycles)], axis=0
    ).astype(BF16)
    placed = dot(place, fourier).astype(BF16)
    send_f[:, :, : 4 * comps] = placed.reshape(n, block, 4 * comps)

    def exchange(send, recv, sem):
        for off in range(1, n):
            to = lax.rem(me + off, n)
            pltpu.make_async_remote_copy(
                src_ref=send.at[to], dst_ref=recv.at[me], send_sem=move_sem.at[2 * sem],
                recv_sem=move_sem.at[2 * sem + 1], device_id={"ma": to},
                device_id_type=pl.DeviceIdType.MESH,
            ).start()
        recv[me] = send[me]

    def settle(buffer, at):
        whole = buffer.at[pl.ds(0, n - 1)]
        pltpu.make_async_copy(whole, whole, move_sem.at[at]).wait()

    pl.semaphore_wait(barrier, n - 1)
    exchange(send_f, recv_f, 0)

    spread_shape = (slots_v.shape[1], n * block)
    col = iota(spread_shape, 1)
    spread = one_hot(
        iota(spread_shape, 0) == div(col, block) * pairs + mod(col, pairs)
    )
    for load in loads[8:]:
        load.wait()
    slots = jnp.broadcast_to(slots_v[...], (8, slots_v.shape[1]))
    high_part = div(slots, 256).astype(F32)
    low_part = mod(slots, 256).astype(F32)
    picked = 256.0 * dot(high_part.astype(BF16), spread) + dot(low_part.astype(BF16), spread)
    flip = mod(iota(picked.shape, 1), block) >= pairs
    picked = jnp.where(flip, modes - 1.0 - picked, picked)[0:1]
    select = one_hot(iota((modes, n * block), 0).astype(F32) == picked)

    hs = pixels // LANES * sims
    for load in loads[6:8]:
        load.wait()
    moved = dot(table_v[...], select)
    fine_cos, fine_sin = moved[:LANES], moved[LANES : 2 * LANES]
    at = 2 * LANES
    cos_t = moved[at : at + hs] + moved[at + hs : at + 2 * hs]
    sin_t = moved[at + 2 * hs : at + 3 * hs] + moved[at + 3 * hs : at + 4 * hs]
    cos_h, sin_h = cos_t.T, sin_t.T
    synth = jnp.concatenate([fine_cos, fine_sin], axis=1).astype(BF16)
    anal = jnp.concatenate([fine_cos.T, fine_sin.T], axis=0).astype(BF16)

    exp_shape = (4 * comps, 6 * hs)
    ecol = iota(exp_shape, 1)
    which = div(ecol, hs)
    comp_q, comp_c = div(which, 2), mod(which, 2)
    source_c = jnp.where(comp_q == 2, 1 - comp_c, comp_c)
    hit = iota(exp_shape, 0) == comp_q * comps + 2 * mod(ecol, sims) + source_c
    sign = jnp.where(jnp.logical_and(comp_q == 2, comp_c == 0), -1.0, 1.0)
    expand = jnp.where(hit, sign, 0.0).astype(BF16)

    sel_shape = (4 * hs, 4 * comps)
    srow, scol = iota(sel_shape, 0), iota(sel_shape, 1)
    row_q, row_c = div(srow, 2 * hs), mod(div(srow, hs), 2)
    out_g, out_c = div(scol, comps), mod(scol, 2)
    want_q = jnp.where(jnp.logical_or(out_g == 1, out_g == 2), 1, 0)
    swap = out_g >= 2
    want_c = jnp.where(swap, 1 - out_c, out_c)
    same_s = mod(srow, sims) == div(mod(scol, comps), 2)
    negative = jnp.logical_or(
        jnp.logical_and(out_g == 2, out_c == 1), jnp.logical_and(out_g == 3, out_c == 0)
    )
    hit = jnp.logical_and(jnp.logical_and(row_q == want_q, row_c == want_c), same_s)
    gather = jnp.where(hit, jnp.where(negative, -1.0, 1.0), 0.0).astype(BF16)

    mask_t = mask_ref[...].astype(F32).T.astype(BF16)
    m_shape = (pixels // LANES, hs)
    mask = dot(mask_t, one_hot(iota(m_shape, 0) == div(iota(m_shape, 1), sims)))

    lane_shape = (8, total)
    cyc = mod(iota(lane_shape, 1), cycles)
    theta_l = jnp.zeros(lane_shape, F32)
    weight_l = jnp.zeros(lane_shape, F32)
    for r in range(cycles):
        theta_l = jnp.where(cyc == r, colat_s[r], theta_l)
        weight_l = jnp.where(cyc == r, weight_s[r], weight_l)
    with_sin = (weight_l / jnp.sin(theta_l))[0:1]
    with_cos = (weight_l * jnp.cos(theta_l) / jnp.sin(theta_l))[0:1]

    settle(recv_f, 1)
    got = recv_f[...].reshape(n * block, LANES)[:, : 4 * comps]
    spread_f = dot(got, expand)
    real, imag = [], []
    for q in range(3):
        re = spread_f[:, 2 * q * hs : (2 * q + 1) * hs]
        im = spread_f[:, (2 * q + 1) * hs : (2 * q + 2) * hs]
        real.append((re * cos_h - im * sin_h).astype(BF16))
        imag.append((re * sin_h + im * cos_h).astype(BF16))
    turned = jnp.concatenate(
        [jnp.concatenate(real, axis=1), jnp.concatenate(imag, axis=1)], axis=0
    )
    maps = dot(synth, turned)
    lead = mask * maps[:, :hs]
    products = jnp.concatenate(
        [lead * maps[:, hs : 2 * hs], lead * maps[:, 2 * hs :]], axis=1
    ).astype(BF16)
    half = dot(anal, products)
    parts = []
    count = n * block
    for q in range(2):
        c_part = half[:count, q * hs : (q + 1) * hs]
        s_part = half[count:, q * hs : (q + 1) * hs]
        parts.append((cos_h * c_part + sin_h * s_part).astype(BF16))
        parts.append((cos_h * s_part - sin_h * c_part).astype(BF16))
    spectra = dot(jnp.concatenate(parts, axis=1), gather) * pixels ** (-0.5)
    send_p[:, :, : 4 * comps] = spectra.astype(BF16).reshape(n, block, 4 * comps)
    exchange(send_p, recv_p, 1)
    scale = (modes / cycles) ** 0.5 / jnp.sqrt(jnp.maximum(degree * (degree + 1.0), 1.0))
    f_level, f_eps, f_order = degree * scale, eps * scale, orders * scale
    settle(recv_p, 3)

    came = recv_p[...].reshape(n * block, LANES)[:, : 4 * comps].astype(F32).T.astype(BF16)
    by_pair = dot(came, place)
    first = jnp.concatenate([by_pair[: 2 * comps] * with_cos, by_pair[2 * comps :] * with_sin], 0)
    second = by_pair[: 2 * comps] * with_sin
    owner = div(iota((1, total), 1), span)
    keep = [jnp.where(owner == p, 1.0, 0.0) for p in range(pairs)]
    first = jnp.concatenate([(first * keep[p]).astype(BF16) for p in range(pairs)], axis=0)
    second = jnp.concatenate([(second * keep[p]).astype(BF16) for p in range(pairs)], axis=0)
    here = dot(first, leg_all[...])
    before = dot(second, prev_all[...])
    for p in range(pairs):
        a, b = 4 * comps * p, 2 * comps * p
        lev, ep, az = f_level[p : p + 1], f_eps[p : p + 1], f_order[p : p + 1]
        grad = (
            lev * here[a : a + comps] - ep * before[b : b + comps]
            + az * here[a + 2 * comps : a + 3 * comps]
        )
        curl = (
            lev * here[a + comps : a + 2 * comps] - ep * before[b + comps : b + 2 * comps]
            + az * here[a + 3 * comps : a + 4 * comps]
        )
        for s in range(sims):
            grad_ref[p, s] = grad[2 * s : 2 * s + 2]
            curl_ref[p, s] = curl[2 * s : 2 * s + 2]
    settle(send_f, 0)
    settle(send_p, 2)


def fused(tbar_alm, twf_alm, legendre, m_slots, cycle_order, colatitude, cycle_weight, pixel_mask, n):
    pairs, sims, _, rows = tbar_alm.shape
    modes = rows - 1
    cycles = legendre.shape[2]
    pixels = pixel_mask.shape[1]
    total = pairs * 2 * cycles
    by_cycle = jnp.transpose(legendre, (0, 2, 1))
    table = jnp.asarray(split_tables(modes, pixels, sims))
    vmem = pl.BlockSpec(memory_space=pltpu.VMEM)
    out = pltpu.VMEM(tbar_alm.shape, F32)
    return pl.pallas_call(
        functools.partial(fused_kernel, n, modes, rows, cycles, pixels, sims),
        out_shape=(out, out),
        in_specs=[pl.BlockSpec(memory_space=pl.ANY)] * 10,
        out_specs=(vmem, vmem),
        scratch_shapes=[
            pltpu.SMEM(m_slots.shape, jnp.int32),
            pltpu.SMEM(cycle_order.shape, jnp.int32),
            pltpu.SMEM(colatitude.shape, F32),
            pltpu.SMEM(cycle_weight.shape, F32),
            pltpu.VMEM((1, m_slots.shape[0]), jnp.int32),
            pltpu.VMEM(tbar_alm.shape, BF16),
            pltpu.VMEM(twf_alm.shape, BF16),
            pltpu.VMEM(by_cycle.shape, BF16),
            pltpu.VMEM((pixels // LANES, LANES), jnp.int32),
            pltpu.VMEM(table.shape, BF16),
            pltpu.VMEM((total, rows), BF16),
            pltpu.VMEM((total, rows), BF16),
        ]
        + [pltpu.VMEM((n, 2 * pairs, LANES), BF16)] * 4
        + [pltpu.SemaphoreType.DMA((10,)), pltpu.SemaphoreType.DMA((4,))],
        compiler_params=pltpu.CompilerParams(collective_id=0, has_side_effects=True),
        name="estimator",
    )(
        m_slots, cycle_order, colatitude, cycle_weight, m_slots.reshape(1, -1), tbar_alm,
        twf_alm, by_cycle, pixel_mask.reshape(pixels // LANES, LANES), table,
    )


def body(n, *args):
    tbar_alm, legendre, pixel_mask = args[0], args[2], args[7]
    pairs, sims, _, rows = tbar_alm.shape
    cycles = legendre.shape[2]
    fits = (
        pairs == 8
        and cycles % 16 == 0
        and pixel_mask.shape[0] == 1
        and pairs * 2 * cycles <= 512
        and rows <= 1025
        and (pixel_mask.shape[1] // LANES * sims) % LANES == 0
        and sims % 4 == 0
        and all(v & (v - 1) == 0 for v in (sims, cycles, pixel_mask.shape[1]))
    )
    return fused(*args, n) if fits else shards(*args)


def solution(mesh):
    return jax.shard_map(
        functools.partial(body, mesh.shape["ma"]),
        mesh=mesh,
        in_specs=(
            P("ma", "grp", None, None),
            P("ma", "grp", None, None),
            P("ma", None, None),
            P(),
            P(),
            P(),
            P(),
            P("ma", None),
        ),
        out_specs=(P("ma", "grp", None, None), P("ma", "grp", None, None)),
        check_vma=False,
    )
```

```python
import math

import functools

import jax
import jax.numpy as jnp
import numpy as np
from jax import lax
from jax.experimental import pallas as pl
from jax.experimental.pallas import tpu as pltpu
from jax.sharding import PartitionSpec as P


def pair_layout(small_orders, mode_count):
    row_index = lax.broadcasted_iota(jnp.int32, (small_orders.shape[0], mode_count + 1), 1)
    smaller = small_orders[:, None]
    upper_half = row_index >= mode_count - smaller
    degree = jnp.where(upper_half, row_index - 1, smaller + row_index)
    orders = jnp.where(upper_half, mode_count - 1 - smaller, smaller + 0 * row_index)
    return (upper_half, degree.astype(jnp.float32), orders.astype(jnp.float32))


def raising(degree, orders):
    square = (
        (degree * degree - orders * orders)
        * (2.0 * degree + 1.0)
        / jnp.maximum(2.0 * degree - 1.0, 1.0)
    )
    return jnp.where(degree > orders, jnp.sqrt(jnp.where(degree > orders, square, 0.0)), 0.0)


def synthesis_sets(tbar_alm, twf_alm, degree, raising_factor, mode_count):
    wiener = twf_alm.astype(jnp.float32)
    scaled = (raising_factor / mode_count)[:, None, None, :] * wiener
    raised = jnp.concatenate([scaled[..., 1:], jnp.zeros_like(scaled[..., :1])], axis=-1)
    stacked = jnp.stack(
        [
            tbar_alm.astype(jnp.float32),
            wiener,
            (degree / mode_count)[:, None, None, :] * wiener,
            raised,
        ],
        axis=2,
    )
    return stacked.reshape(stacked.shape[0], stacked.shape[1], 8, stacked.shape[4]).astype(
        jnp.bfloat16
    )


def mode_columns(small_orders, mode_count):
    return jnp.stack([small_orders, mode_count - 1 - small_orders], axis=1).reshape(-1)


def fourier_table(orders_int, pixel_count):
    pixel_index = lax.broadcasted_iota(jnp.int32, (orders_int.shape[0], pixel_count), 1)
    turns = orders_int[:, None] * pixel_index % pixel_count
    radians = turns.astype(jnp.float32) * (2.0 * math.pi / pixel_count)
    return jnp.stack([jnp.cos(radians), -jnp.sin(radians)], axis=0).astype(jnp.bfloat16)


def combine_modes(legendre_sums, orders_int, cos_cycle, sin_cycle, mode_count):
    orders_real = orders_int.astype(jnp.float32)
    inv_sin = 1.0 / sin_cycle
    ratio = (orders_real / mode_count)[:, None]
    theta_real = (cos_cycle * legendre_sums[:, 4] - legendre_sums[:, 6]) * inv_sin
    theta_imag = (cos_cycle * legendre_sums[:, 5] - legendre_sums[:, 7]) * inv_sin
    phi_real = -ratio * legendre_sums[:, 3] * inv_sin
    phi_imag = ratio * legendre_sums[:, 2] * inv_sin
    weight = (jnp.where(orders_int == 0, 1.0, 2.0) * mode_count ** (-0.5))[:, None]
    stacked = jnp.stack(
        [legendre_sums[:, 0], legendre_sums[:, 1], theta_real, theta_imag, phi_real, phi_imag],
        axis=1,
    )
    return (stacked * weight).astype(jnp.bfloat16)


def analysis_sets(spectra, colatitude, cycle_weight):
    with_cos = cycle_weight * jnp.cos(colatitude) / jnp.sin(colatitude)
    with_sin = cycle_weight / jnp.sin(colatitude)
    stacked = jnp.stack(
        [
            spectra[:, 0] * with_cos,
            spectra[:, 0] * with_sin,
            spectra[:, 1] * with_cos,
            spectra[:, 1] * with_sin,
        ],
        axis=1,
    )
    return stacked.reshape(spectra.shape[0], 8, spectra.shape[3], spectra.shape[4]).astype(
        jnp.bfloat16
    )


def estimate(merged, degree, orders, raising_factor, mode_count, cycle_count):
    level = degree[:, None, :]
    azimuth = orders[:, None, :]
    factor = raising_factor[:, None, :]

    def previous(values):
        return jnp.concatenate([jnp.zeros_like(values[..., :1]), values[..., :-1]], axis=-1)

    grad_real = (
        level * merged[:, :, 0] - factor * previous(merged[:, :, 2]) + azimuth * merged[:, :, 7]
    )
    grad_imag = (
        level * merged[:, :, 1] - factor * previous(merged[:, :, 3]) - azimuth * merged[:, :, 6]
    )
    curl_real = (
        level * merged[:, :, 4] - factor * previous(merged[:, :, 6]) - azimuth * merged[:, :, 3]
    )
    curl_imag = (
        level * merged[:, :, 5] - factor * previous(merged[:, :, 7]) + azimuth * merged[:, :, 2]
    )
    scale = (mode_count / cycle_count) ** 0.5 / jnp.sqrt(jnp.maximum(level * (level + 1.0), 1.0))
    scale = scale[:, :, None, :]
    return (
        jnp.stack([grad_real, grad_imag], axis=2) * scale,
        jnp.stack([curl_real, curl_imag], axis=2) * scale,
    )


def shards(tbar_alm, twf_alm, legendre, m_slots, cycle_order, colatitude, cycle_weight, pixel_mask):
    pairs_dev = tbar_alm.shape[0]
    row_count = tbar_alm.shape[3]
    mode_count = row_count - 1
    cycle_count = legendre.shape[2]
    cycle_dev = pixel_mask.shape[0]
    pixel_count = pixel_mask.shape[1]
    device_slot = lax.axis_index("ma")
    local_small = lax.dynamic_slice_in_dim(m_slots, device_slot * pairs_dev, pairs_dev)
    upper_half, degree, orders = pair_layout(local_small, mode_count)
    raising_factor = raising(degree, orders)
    coeff_sets = synthesis_sets(tbar_alm, twf_alm, degree, raising_factor, mode_count)
    halves = jnp.stack([jnp.logical_not(upper_half), upper_half], axis=1)
    masked = coeff_sets[:, None] * halves.astype(jnp.bfloat16)[:, :, None, None, :]
    legendre_sums = jnp.einsum(
        "phsck,pkr->scphr", masked, legendre, preferred_element_type=jnp.float32
    )
    legendre_sums = jnp.take(legendre_sums, cycle_order, axis=4)
    legendre_sums = legendre_sums.reshape(legendre_sums.shape[0], 8, 2 * pairs_dev, cycle_count)
    all_orders = mode_columns(m_slots, mode_count)
    dft_table = fourier_table(all_orders, pixel_count)
    pixel_weights = pixel_mask.astype(jnp.float32)
    slot_theta = jnp.take(colatitude, cycle_order)
    local_orders = mode_columns(local_small, mode_count)
    outgoing = combine_modes(
        legendre_sums, local_orders, jnp.cos(slot_theta), jnp.sin(slot_theta), mode_count
    )
    fourier = lax.all_to_all(outgoing, "ma", split_axis=3, concat_axis=2, tiled=True)
    fourier = fourier.reshape(fourier.shape[0], 3, 2, mode_count, cycle_dev)
    cycle_maps = jnp.einsum(
        "sqemr,emj->sqrj", fourier, dft_table, preferred_element_type=jnp.float32
    )
    products = (pixel_weights * cycle_maps[:, 0:1] * cycle_maps[:, 1:3]).astype(jnp.bfloat16)
    spectra = jnp.einsum("sqrj,emj->sqemr", products, dft_table, preferred_element_type=jnp.float32)
    received = (spectra * pixel_count ** (-0.5)).astype(jnp.bfloat16)
    returned = lax.all_to_all(received, "ma", split_axis=3, concat_axis=4, tiled=True)
    inverse = (
        jnp.zeros((cycle_count,), jnp.int32).at[cycle_order].set(lax.iota(jnp.int32, cycle_count))
    )
    spectra = jnp.take(returned, inverse, axis=4).astype(jnp.float32)
    weighted = analysis_sets(spectra, colatitude, cycle_weight)
    weighted = weighted.reshape(weighted.shape[0], 8, pairs_dev, 2, cycle_count)
    projected = jnp.einsum(
        "scphr,pkr->phsck", weighted, legendre, preferred_element_type=jnp.float32
    )
    merged = jnp.sum(projected * halves.astype(jnp.float32)[:, :, None, None, :], axis=1)
    return estimate(merged, degree, orders, raising_factor, mode_count, cycle_count)


LANES = 128
TURNS = 2
F32 = jnp.float32
BF16 = jnp.bfloat16


def split_tables(mode_count, pixel_count, sims):
    high_count = LANES // (TURNS * sims)
    low_count = pixel_count // high_count
    m = np.arange(mode_count)[:, None]
    low = np.arange(low_count)[None, :]
    high = (np.arange(LANES) // sims % high_count)[None, :] * low_count
    fine = (m * low % pixel_count) * (2.0 * math.pi / pixel_count)
    coarse = (m * high % pixel_count) * (2.0 * math.pi / pixel_count)

    def halves(values):
        upper = values.astype(np.float32).astype(BF16)
        return [upper, (values.astype(np.float32) - upper.astype(np.float32)).astype(BF16)]

    waves = [np.cos(fine).astype(BF16), (-np.sin(fine)).astype(BF16)]
    by_pixel = np.concatenate([wave.T for wave in waves], axis=0)
    by_mode = np.concatenate(waves + halves(np.cos(coarse)) + halves(np.sin(coarse)), axis=1)
    return by_pixel, by_mode


def spread_table(sims):
    comps = 2 * sims
    quad = LANES // (4 * comps)
    row = np.arange(TURNS * LANES)[:, None]
    col = np.arange(6 * LANES)[None, :]
    high_count = LANES // (TURNS * sims)
    row_t, row_g, row_s, row_c = row // LANES, row // comps % 4, row // 2 % sims, row % 2
    col_q, col_c = col // (2 * LANES), col // LANES % 2
    col_t, col_s = col % LANES // (high_count * sims), col % sims
    group_q = np.array([0, 1, 2, 1])[row_g]
    source_c = np.where(col_q == 2, 1 - col_c, col_c)
    sign = np.where((col_q == 2) & (col_c == 0), -1.0, 1.0)
    hit = (row_t == col_t) & (row_s == col_s) & (group_q == col_q) & (row_c == source_c)
    return np.where(hit, sign, 0.0).astype(BF16)


def gather_table(sims):
    comps = 2 * sims
    quad = LANES // (4 * comps)
    high_count = LANES // (TURNS * sims)
    row = np.arange(quad * 4 * LANES)[:, None]
    col = np.arange(LANES)[None, :]
    hit = row // (4 * LANES) == col // (2 * comps) % quad
    hit &= row // (2 * LANES) % 2 == col // comps % 2
    hit &= row // LANES % 2 == col % 2
    hit &= row % LANES // (high_count * sims) == col // (2 * comps * quad)
    hit &= row % sims == col // 2 % sims
    return np.where(hit, 1.0, 0.0).astype(BF16)


def iota(shape, axis):
    return lax.broadcasted_iota(jnp.int32, shape, axis)


def div(values, size):
    return values >> (size.bit_length() - 1)


def mod(values, size):
    return values & (size - 1)


def one_hot(condition):
    return jnp.where(condition, 1.0, 0.0).astype(BF16)


def dot(left, right):
    return jnp.dot(left, right, preferred_element_type=F32)


def dot_t(left, right):
    return lax.dot_general(left, right, (((1,), (1,)), ((), ())), preferred_element_type=F32)


def fused_kernel(
    n, modes, rows, cycles, pixels, sims,
    slots_hbm, cycle_hbm, colat_hbm, weight_hbm, row_hbm, tbar_hbm, twf_hbm, leg_hbm, mask_hbm,
    pixel_hbm, mode_hbm, spread_hbm, gather_hbm,
    grad_ref, curl_ref,
    slots_s, cycle_s, colat_s, weight_s, slots_v, tbar_ref, twf_ref, leg_ref, mask_ref,
    pixel_v, mode_v, spread_v, gather_v,
    leg_all, prev_all, fs_ref, place_ref, keep_ref, synth_ref, anal_ref, high_ref, pixmask_ref,
    send_m, recv_m, send_f, recv_f, send_p, recv_p, load_sem, move_sem,
):
    me = lax.axis_index("ma")
    work = n // TURNS
    pairs = tbar_ref.shape[0]
    comps = 2 * sims
    quad = LANES // (4 * comps)
    groups = pairs // quad
    span = 2 * cycles
    total = pairs * span
    count = n * 2 * pairs
    gh = 2 * groups
    high_count = LANES // (TURNS * sims)
    fine = pixels // high_count
    is_worker = me < work

    names = [
        (slots_hbm, slots_s), (colat_hbm, colat_s), (cycle_hbm, cycle_s),
        (leg_hbm, leg_ref), (tbar_hbm, tbar_ref), (twf_hbm, twf_ref),
        (mask_hbm, mask_ref), (weight_hbm, weight_s), (row_hbm, slots_v),
        (mode_hbm, mode_v), (pixel_hbm, pixel_v), (spread_hbm, spread_v), (gather_hbm, gather_v),
    ]
    loads = [
        pltpu.make_async_copy(source, target, load_sem.at[at])
        for at, (source, target) in enumerate(names)
    ]
    for load in loads[:6]:
        load.start()
    barrier = pltpu.get_barrier_semaphore()

    @pl.when(is_worker)
    def _():
        for off in range(1, n):
            pl.semaphore_signal(
                barrier, inc=1, device_id={"ma": lax.rem(me + off, n)},
                device_id_type=pl.DeviceIdType.MESH,
            )

    for load in loads[6:8]:
        load.start()

    @pl.when(is_worker)
    def _():
        for load in loads[8:]:
            load.start()

    def remote(source, target, at, to):
        return pltpu.make_async_remote_copy(
            src_ref=source, dst_ref=target, send_sem=move_sem.at[2 * at],
            recv_sem=move_sem.at[2 * at + 1], device_id={"ma": to},
            device_id_type=pl.DeviceIdType.MESH,
        )

    def settle(buffer, at):
        pltpu.make_async_copy(buffer, buffer, move_sem.at[at]).wait()

    @pl.when(jnp.logical_not(is_worker))
    def _():
        pl.semaphore_wait(barrier, work)
        loads[6].wait()
        send_m[...] = mask_ref[...].astype(F32).astype(BF16)
        remote(send_m, recv_m, 2, me - work).start()

    for load in loads[:3]:
        load.wait()

    row_shape = (pairs, rows)
    smaller = jnp.zeros(row_shape, jnp.int32)
    for p in range(pairs):
        smaller = jnp.where(iota(row_shape, 0) == p, slots_s[me * pairs + p], smaller)
    k = iota(row_shape, 1)
    upper = k >= modes - smaller
    degree = jnp.where(upper, k - 1, smaller + k).astype(F32)
    orders = jnp.where(upper, modes - 1 - smaller, smaller).astype(F32)
    eps = raising(degree, orders)
    upper_f = jnp.where(upper, 1.0, 0.0)
    lower_f = 1.0 - upper_f

    colat = jnp.zeros((cycles, LANES), F32)
    for r in range(cycles):
        colat = jnp.where(iota(colat.shape, 0) == r, colat_s[r], colat)
    csc = 1.0 / jnp.sin(colat)
    cot = jnp.cos(colat) * csc
    lane_group = mod(div(iota(colat.shape, 1), comps), 4)
    base = jnp.where(lane_group == 0, 1.0, jnp.where(lane_group == 1, cot, csc))

    for load in loads[3:6]:
        load.wait()
    lane = iota((8, LANES), 1)
    lane_quad = div(lane, 4 * comps)
    is_phi = mod(div(lane, comps), 4) == 2
    for g in range(groups):
        sets, legs = [], []
        small = jnp.zeros((8, LANES), jnp.int32)
        for q in range(quad):
            p = g * quad + q
            small = jnp.where(lane_quad == q, slots_s[me * pairs + p], small)
            tbar = jnp.concatenate([tbar_ref[p, s].astype(F32) for s in range(sims)], axis=0)
            twf = jnp.concatenate([twf_ref[p, s].astype(F32) for s in range(sims)], axis=0)
            deg_p, eps_p = degree[p : p + 1] / modes, eps[p : p + 1] / modes
            scaled = -(eps_p * twf)
            raised = jnp.concatenate([scaled[:, 1:], jnp.zeros_like(scaled[:, :1])], axis=1)
            sets += [tbar, deg_p * twf, twf, raised]
            leg = leg_ref[p].astype(F32)
            low, high = lower_f[p : p + 1], upper_f[p : p + 1]
            legs += [leg * low, leg * high]
        legs = jnp.concatenate(legs, axis=0).astype(BF16)
        leg_all[pl.ds(g * quad * span, quad * span), :] = legs
        out = dot_t(legs, jnp.concatenate(sets, axis=0).astype(BF16))
        picked = out[:span]
        for q in range(1, quad):
            own = div(iota(picked.shape, 1), 4 * comps) == q
            picked = jnp.where(own, out[q * span : (q + 1) * span], picked)
        for h in range(2):
            order = (modes - 1 - small if h else small)[0:1]
            norm = jnp.where(order == 0, 1.0, 2.0) * modes ** (-0.5)
            norm = jnp.where(is_phi[0:1], norm * (order.astype(F32) / modes), norm)
            fs_ref[:, 2 * g + h, :] = picked[h * cycles : (h + 1) * cycles] * (base * norm)

    for t in range(TURNS):
        for w in range(work):
            send_f[t, w] = fs_ref[cycle_s[w + work * t], :gh, :].astype(BF16)

    @pl.when(is_worker)
    def _():
        pl.semaphore_wait(barrier, work - 1)

    for w in range(work):
        @pl.when(me != w)
        def _():
            remote(send_f.at[:, w], recv_f.at[:, me], 0, w).start()

    own = mod(me, work)
    recv_f[:, me] = send_f[:, own]

    place_shape = (work * gh, total)
    place_row, place_lane = iota(place_shape, 0), iota(place_shape, 1)
    lane_pair, lane_half = div(place_lane, span), mod(div(place_lane, cycles), 2)
    match = mod(place_row, gh) == div(lane_pair, quad) * 2 + lane_half
    slot_row = div(place_row, gh)
    for t in range(TURNS):
        cyc = jnp.zeros(place_shape, jnp.int32)
        for w in range(work):
            cyc = jnp.where(slot_row == w, cycle_s[w + work * t], cyc)
        place_ref[t] = one_hot(jnp.logical_and(match, cyc == mod(place_lane, cycles)))

    loads[7].wait()
    lane_shape = (8, total)
    cyc = mod(iota(lane_shape, 1), cycles)
    theta_l = jnp.zeros(lane_shape, F32)
    weight_l = jnp.zeros(lane_shape, F32)
    for r in range(cycles):
        theta_l = jnp.where(cyc == r, colat_s[r], theta_l)
        weight_l = jnp.where(cyc == r, weight_s[r], weight_l)
    with_sin = weight_l / jnp.sin(theta_l)
    with_cos = weight_l * jnp.cos(theta_l) / jnp.sin(theta_l)
    owner = div(iota(lane_shape, 1), span)
    for p in range(pairs):
        keep_ref[p, 0] = jnp.where(owner == p, with_cos, 0.0)
        keep_ref[p, 1] = jnp.where(owner == p, with_sin, 0.0)
    for p in range(pairs):
        leg = leg_ref[p].astype(F32)
        prev = jnp.concatenate([jnp.zeros_like(leg[:, :1]), leg[:, : rows - 1]], axis=1)
        low, high = lower_f[p : p + 1], upper_f[p : p + 1]
        prev_all[pl.ds(p * span, span), :] = jnp.concatenate(
            [prev * low, prev * high], axis=0
        ).astype(BF16)
    scale = (modes / cycles) ** 0.5 / jnp.sqrt(jnp.maximum(degree * (degree + 1.0), 1.0))
    f_level, f_eps, f_order = degree * scale, eps * scale, orders * scale

    @pl.when(is_worker)
    def _():
        for load in loads[8:]:
            load.wait()
        pair_count = slots_v.shape[1]

        def pair_of(at):
            source, inner = mod(div(at, gh), n), mod(at, gh)
            return source * pairs + div(inner, 2) * quad + div(at, n * gh)

        slots = jnp.broadcast_to(slots_v[...], (pair_count, pair_count)).astype(F32).astype(BF16)
        spread = one_hot(iota((pair_count, count), 0) == pair_of(iota((pair_count, count), 1)))
        spread_t = one_hot(iota((count, pair_count), 1) == pair_of(iota((count, pair_count), 0)))
        by_lane = dot(slots[:16], spread)[0:8]
        by_lane = jnp.where(mod(iota(by_lane.shape, 1), 2) == 1, modes - 1.0 - by_lane, by_lane)
        by_row = dot_t(spread_t, slots)
        by_row = jnp.where(mod(iota(by_row.shape, 0), 2) == 1, modes - 1.0 - by_row, by_row)
        select = one_hot(iota((modes, count), 0).astype(F32) == by_lane[0:1])
        select_t = jnp.concatenate(
            [
                one_hot((iota(by_row.shape, 1) + at).astype(F32) == by_row)
                for at in range(0, modes, pair_count)
            ],
            axis=1,
        )
        moved = dot(pixel_v[...], select).astype(BF16)
        synth_ref[:, :count] = moved[:fine]
        synth_ref[:, count:] = moved[fine:]
        moved = dot(select_t, mode_v[...])
        anal_ref[:count] = moved[:, :fine].astype(BF16)
        anal_ref[count:] = moved[:, fine : 2 * fine].astype(BF16)
        at = 2 * fine
        for part in range(2):
            high_ref[part] = moved[:, at : at + LANES] + moved[:, at + LANES : at + 2 * LANES]
            at += 2 * LANES

        loads[6].wait()
        own_mask = mask_ref[...].astype(F32)
        settle(recv_m, 5)
        both = jnp.concatenate([own_mask, recv_m[...].astype(F32)], axis=0)
        cut = fine // LANES
        wide = (both.shape[0], LANES)
        m_turn = div(iota(wide, 1), high_count * sims)
        m_high = mod(div(iota(wide, 1), sims), high_count)
        first_row = (m_turn * high_count + m_high) * cut
        both_t = both.T.astype(BF16)
        for at in range(cut):
            pixmask_ref[pl.ds(at * LANES, LANES), :] = dot(
                both_t, one_hot(iota(wide, 0) == first_row + at)
            )

        settle(recv_f.at[:, pl.ds(0, n - 1)], 1)
        got = jnp.concatenate(
            [recv_f[t].reshape(n * gh, LANES) for t in range(TURNS)], axis=1
        )
        quarter = mod(div(iota((8, TURNS * LANES), 1), 4 * comps), quad)[0:1]
        got = jnp.concatenate(
            [got * one_hot(quarter == q) for q in range(quad)], axis=0
        )
        spread_f = dot(got, spread_v[...])
        cos_h, sin_h = high_ref[0], high_ref[1]
        real, imag = [], []
        for q in range(3):
            re = spread_f[:, 2 * q * LANES : (2 * q + 1) * LANES]
            im = spread_f[:, (2 * q + 1) * LANES : (2 * q + 2) * LANES]
            real.append((re * cos_h - im * sin_h).astype(BF16))
            imag.append((re * sin_h + im * cos_h).astype(BF16))
        turned = jnp.concatenate(
            [jnp.concatenate(real, axis=1), jnp.concatenate(imag, axis=1)], axis=0
        )
        maps = dot(synth_ref[...], turned)
        lead = pixmask_ref[...] * maps[:, :LANES]
        products = jnp.concatenate(
            [lead * maps[:, LANES : 2 * LANES], lead * maps[:, 2 * LANES :]], axis=1
        ).astype(BF16)
        half = dot(anal_ref[...], products)
        parts = []
        for q in range(2):
            c_part = half[:count, q * LANES : (q + 1) * LANES]
            s_part = half[count:, q * LANES : (q + 1) * LANES]
            parts.append((cos_h * c_part + sin_h * s_part).astype(BF16))
            parts.append((cos_h * s_part - sin_h * c_part).astype(BF16))
        parts = jnp.concatenate(parts, axis=1)
        block = n * gh
        wide = jnp.concatenate(
            [parts[q * block : (q + 1) * block] for q in range(quad)], axis=1
        )
        spectra = dot(wide, gather_v[...]) * pixels ** (-0.5)
        send_p[...] = spectra.astype(BF16).reshape(n, gh, LANES)
        for d in range(work):
            @pl.when(me != d)
            def _():
                remote(send_p.at[d], recv_p.at[me], 1, d).start()
        for d in range(work, n):
            remote(send_p.at[d], recv_p.at[me], 1, d).start()
        recv_p[me] = send_p[me]
        settle(recv_p.at[pl.ds(0, work - 1)], 3)

    @pl.when(jnp.logical_not(is_worker))
    def _():
        settle(recv_p, 3)

    came = recv_p[...].astype(F32).reshape(work * gh, LANES)
    odd = mod(iota(came.shape, 1), 2) == 1
    from_phi = mod(div(iota(came.shape, 1), comps), 2) == 1
    swapped = jnp.where(odd, pltpu.roll(came, 1, 1), pltpu.roll(came, LANES - 1, 1))
    swapped = jnp.where(odd == from_phi, -swapped, swapped)
    turned = [came.T.astype(BF16), swapped.T.astype(BF16)]
    side = LANES // TURNS
    by_pair = sum(
        dot(
            jnp.concatenate([half[t * side : (t + 1) * side] for half in turned], axis=0),
            place_ref[t],
        )
        for t in range(TURNS)
    )
    first, second = [], []
    for p in range(pairs):
        at = p % quad * 2 * comps
        theta, phi = by_pair[at : at + comps], by_pair[at + comps : at + 2 * comps]
        at += side
        theta_i, phi_i = by_pair[at : at + comps], by_pair[at + comps : at + 2 * comps]
        with_cos, with_sin = keep_ref[p, 0], keep_ref[p, 1]
        first += [theta * with_cos, phi * with_cos, phi_i * with_sin, theta_i * with_sin]
        second += [theta * with_sin, phi * with_sin]
    here = dot(jnp.concatenate(first, axis=0).astype(BF16), leg_all[...])
    before = dot(jnp.concatenate(second, axis=0).astype(BF16), prev_all[...])
    for p in range(pairs):
        a, b = 4 * comps * p, 2 * comps * p
        lev, ep, az = f_level[p : p + 1], f_eps[p : p + 1], f_order[p : p + 1]
        grad = (
            lev * here[a : a + comps] - ep * before[b : b + comps]
            + az * here[a + 2 * comps : a + 3 * comps]
        )
        curl = (
            lev * here[a + comps : a + 2 * comps] - ep * before[b + comps : b + 2 * comps]
            + az * here[a + 3 * comps : a + 4 * comps]
        )
        for s in range(sims):
            grad_ref[p, s] = grad[2 * s : 2 * s + 2]
            curl_ref[p, s] = curl[2 * s : 2 * s + 2]

    @pl.when(is_worker)
    def _():
        settle(send_f.at[:, pl.ds(0, work - 1)], 0)
        settle(send_p.at[pl.ds(0, n - 1)], 2)

    @pl.when(jnp.logical_not(is_worker))
    def _():
        loads_left = send_f
        settle(loads_left, 0)
        settle(send_m, 4)


def store_kernel(grad_ref, curl_ref, grad_hbm, curl_hbm, sem):
    copies = [
        pltpu.make_async_copy(grad_ref, grad_hbm, sem.at[0]),
        pltpu.make_async_copy(curl_ref, curl_hbm, sem.at[1]),
    ]
    for copy in copies:
        copy.start()
    for copy in copies:
        copy.wait()


def fused(tbar_alm, twf_alm, legendre, m_slots, cycle_order, colatitude, cycle_weight, pixel_mask, n):
    pairs, sims, _, rows = tbar_alm.shape
    modes = rows - 1
    cycles = legendre.shape[2]
    pixels = pixel_mask.shape[1]
    total = pairs * 2 * cycles
    count = n * 2 * pairs
    work = n // TURNS
    gh = 2 * pairs * 8 * sims // LANES
    fine = pixels * TURNS * sims // LANES
    by_cycle = jnp.transpose(legendre, (0, 2, 1))
    by_pixel, by_mode = split_tables(modes, pixels, sims)
    tables = [jnp.asarray(x) for x in (by_pixel, by_mode, spread_table(sims), gather_table(sims))]
    vmem, anywhere = pl.BlockSpec(memory_space=pltpu.VMEM), pl.BlockSpec(memory_space=pl.ANY)
    out = pltpu.VMEM(tbar_alm.shape, F32)
    mask_shape = (pixels // LANES, LANES)
    made = pl.pallas_call(
        functools.partial(fused_kernel, n, modes, rows, cycles, pixels, sims),
        out_shape=(out, out),
        in_specs=[anywhere] * 13,
        out_specs=(vmem, vmem),
        scratch_shapes=[
            pltpu.SMEM(m_slots.shape, jnp.int32),
            pltpu.SMEM(cycle_order.shape, jnp.int32),
            pltpu.SMEM(colatitude.shape, F32),
            pltpu.SMEM(cycle_weight.shape, F32),
            pltpu.VMEM((1, m_slots.shape[0]), jnp.int32),
            pltpu.VMEM(tbar_alm.shape, BF16),
            pltpu.VMEM(twf_alm.shape, BF16),
            pltpu.VMEM(by_cycle.shape, BF16),
            pltpu.VMEM(mask_shape, jnp.int32),
        ]
        + [pltpu.VMEM(table.shape, BF16) for table in tables]
        + [
            pltpu.VMEM((total, rows), BF16),
            pltpu.VMEM((total, rows), BF16),
            pltpu.VMEM((cycles, 8, LANES), F32),
            pltpu.VMEM((TURNS, work * gh, total), BF16),
            pltpu.VMEM((pairs, 2, 8, total), F32),
            pltpu.VMEM((fine, 2 * count), BF16),
            pltpu.VMEM((2 * count, fine), BF16),
            pltpu.VMEM((2, count, LANES), F32),
            pltpu.VMEM((fine, LANES), F32),
            pltpu.VMEM(mask_shape, BF16),
            pltpu.VMEM(mask_shape, BF16),
            pltpu.VMEM((TURNS, work, gh, LANES), BF16),
            pltpu.VMEM((TURNS, n, gh, LANES), BF16),
            pltpu.VMEM((n, gh, LANES), BF16),
            pltpu.VMEM((work, gh, LANES), BF16),
            pltpu.SemaphoreType.DMA((13,)),
            pltpu.SemaphoreType.DMA((6,)),
        ],
        compiler_params=pltpu.CompilerParams(collective_id=0, has_side_effects=True),
        name="estimator",
    )(
        m_slots, cycle_order, colatitude, cycle_weight, m_slots.reshape(1, -1), tbar_alm,
        twf_alm, by_cycle, pixel_mask.reshape(mask_shape), *tables,
    )
    return pl.pallas_call(
        store_kernel,
        out_shape=(jax.ShapeDtypeStruct(tbar_alm.shape, F32),) * 2,
        in_specs=[vmem] * 2,
        out_specs=[anywhere] * 2,
        scratch_shapes=[pltpu.SemaphoreType.DMA((2,))],
        name="store",
    )(*(pltpu.with_memory_space_constraint(x, pltpu.VMEM) for x in made))


def body(n, *args):
    tbar_alm, legendre, pixel_mask = args[0], args[2], args[7]
    pairs, sims, _, rows = tbar_alm.shape
    cycles = legendre.shape[2]
    pixels = pixel_mask.shape[1]
    fits = (
        pairs == 8
        and cycles == n == 16
        and pixel_mask.shape[0] == 1
        and rows == 257
        and pairs * n == LANES
        and sims == 4
        and pixels == 4096
    )
    return fused(*args, n) if fits else shards(*args)


def solution(mesh):
    return jax.shard_map(
        functools.partial(body, mesh.shape["ma"]),
        mesh=mesh,
        in_specs=(
            P("ma", "grp", None, None),
            P("ma", "grp", None, None),
            P("ma", None, None),
            P(),
            P(),
            P(),
            P(),
            P("ma", None),
        ),
        out_specs=(P("ma", "grp", None, None), P("ma", "grp", None, None)),
        check_vma=False,
    )
```

```python
import math

import functools

import jax
import jax.numpy as jnp
import numpy as np
from jax import lax
from jax.experimental import pallas as pl
from jax.experimental.pallas import tpu as pltpu
from jax.sharding import PartitionSpec as P


def pair_layout(small_orders, mode_count):
    row_index = lax.broadcasted_iota(jnp.int32, (small_orders.shape[0], mode_count + 1), 1)
    smaller = small_orders[:, None]
    upper_half = row_index >= mode_count - smaller
    degree = jnp.where(upper_half, row_index - 1, smaller + row_index)
    orders = jnp.where(upper_half, mode_count - 1 - smaller, smaller + 0 * row_index)
    return (upper_half, degree.astype(jnp.float32), orders.astype(jnp.float32))


def raising(degree, orders):
    square = (
        (degree * degree - orders * orders)
        * (2.0 * degree + 1.0)
        / jnp.maximum(2.0 * degree - 1.0, 1.0)
    )
    return jnp.where(degree > orders, jnp.sqrt(jnp.where(degree > orders, square, 0.0)), 0.0)


def synthesis_sets(tbar_alm, twf_alm, degree, raising_factor, mode_count):
    wiener = twf_alm.astype(jnp.float32)
    scaled = (raising_factor / mode_count)[:, None, None, :] * wiener
    raised = jnp.concatenate([scaled[..., 1:], jnp.zeros_like(scaled[..., :1])], axis=-1)
    stacked = jnp.stack(
        [
            tbar_alm.astype(jnp.float32),
            wiener,
            (degree / mode_count)[:, None, None, :] * wiener,
            raised,
        ],
        axis=2,
    )
    return stacked.reshape(stacked.shape[0], stacked.shape[1], 8, stacked.shape[4]).astype(
        jnp.bfloat16
    )


def mode_columns(small_orders, mode_count):
    return jnp.stack([small_orders, mode_count - 1 - small_orders], axis=1).reshape(-1)


def fourier_table(orders_int, pixel_count):
    pixel_index = lax.broadcasted_iota(jnp.int32, (orders_int.shape[0], pixel_count), 1)
    turns = orders_int[:, None] * pixel_index % pixel_count
    radians = turns.astype(jnp.float32) * (2.0 * math.pi / pixel_count)
    return jnp.stack([jnp.cos(radians), -jnp.sin(radians)], axis=0).astype(jnp.bfloat16)


def combine_modes(legendre_sums, orders_int, cos_cycle, sin_cycle, mode_count):
    orders_real = orders_int.astype(jnp.float32)
    inv_sin = 1.0 / sin_cycle
    ratio = (orders_real / mode_count)[:, None]
    theta_real = (cos_cycle * legendre_sums[:, 4] - legendre_sums[:, 6]) * inv_sin
    theta_imag = (cos_cycle * legendre_sums[:, 5] - legendre_sums[:, 7]) * inv_sin
    phi_real = -ratio * legendre_sums[:, 3] * inv_sin
    phi_imag = ratio * legendre_sums[:, 2] * inv_sin
    weight = (jnp.where(orders_int == 0, 1.0, 2.0) * mode_count ** (-0.5))[:, None]
    stacked = jnp.stack(
        [legendre_sums[:, 0], legendre_sums[:, 1], theta_real, theta_imag, phi_real, phi_imag],
        axis=1,
    )
    return (stacked * weight).astype(jnp.bfloat16)


def analysis_sets(spectra, colatitude, cycle_weight):
    with_cos = cycle_weight * jnp.cos(colatitude) / jnp.sin(colatitude)
    with_sin = cycle_weight / jnp.sin(colatitude)
    stacked = jnp.stack(
        [
            spectra[:, 0] * with_cos,
            spectra[:, 0] * with_sin,
            spectra[:, 1] * with_cos,
            spectra[:, 1] * with_sin,
        ],
        axis=1,
    )
    return stacked.reshape(spectra.shape[0], 8, spectra.shape[3], spectra.shape[4]).astype(
        jnp.bfloat16
    )


def estimate(merged, degree, orders, raising_factor, mode_count, cycle_count):
    level = degree[:, None, :]
    azimuth = orders[:, None, :]
    factor = raising_factor[:, None, :]

    def previous(values):
        return jnp.concatenate([jnp.zeros_like(values[..., :1]), values[..., :-1]], axis=-1)

    grad_real = (
        level * merged[:, :, 0] - factor * previous(merged[:, :, 2]) + azimuth * merged[:, :, 7]
    )
    grad_imag = (
        level * merged[:, :, 1] - factor * previous(merged[:, :, 3]) - azimuth * merged[:, :, 6]
    )
    curl_real = (
        level * merged[:, :, 4] - factor * previous(merged[:, :, 6]) - azimuth * merged[:, :, 3]
    )
    curl_imag = (
        level * merged[:, :, 5] - factor * previous(merged[:, :, 7]) + azimuth * merged[:, :, 2]
    )
    scale = (mode_count / cycle_count) ** 0.5 / jnp.sqrt(jnp.maximum(level * (level + 1.0), 1.0))
    scale = scale[:, :, None, :]
    return (
        jnp.stack([grad_real, grad_imag], axis=2) * scale,
        jnp.stack([curl_real, curl_imag], axis=2) * scale,
    )


def shards(tbar_alm, twf_alm, legendre, m_slots, cycle_order, colatitude, cycle_weight, pixel_mask):
    pairs_dev = tbar_alm.shape[0]
    row_count = tbar_alm.shape[3]
    mode_count = row_count - 1
    cycle_count = legendre.shape[2]
    cycle_dev = pixel_mask.shape[0]
    pixel_count = pixel_mask.shape[1]
    device_slot = lax.axis_index("ma")
    local_small = lax.dynamic_slice_in_dim(m_slots, device_slot * pairs_dev, pairs_dev)
    upper_half, degree, orders = pair_layout(local_small, mode_count)
    raising_factor = raising(degree, orders)
    coeff_sets = synthesis_sets(tbar_alm, twf_alm, degree, raising_factor, mode_count)
    halves = jnp.stack([jnp.logical_not(upper_half), upper_half], axis=1)
    masked = coeff_sets[:, None] * halves.astype(jnp.bfloat16)[:, :, None, None, :]
    legendre_sums = jnp.einsum(
        "phsck,pkr->scphr", masked, legendre, preferred_element_type=jnp.float32
    )
    legendre_sums = jnp.take(legendre_sums, cycle_order, axis=4)
    legendre_sums = legendre_sums.reshape(legendre_sums.shape[0], 8, 2 * pairs_dev, cycle_count)
    all_orders = mode_columns(m_slots, mode_count)
    dft_table = fourier_table(all_orders, pixel_count)
    pixel_weights = pixel_mask.astype(jnp.float32)
    slot_theta = jnp.take(colatitude, cycle_order)
    local_orders = mode_columns(local_small, mode_count)
    outgoing = combine_modes(
        legendre_sums, local_orders, jnp.cos(slot_theta), jnp.sin(slot_theta), mode_count
    )
    fourier = lax.all_to_all(outgoing, "ma", split_axis=3, concat_axis=2, tiled=True)
    fourier = fourier.reshape(fourier.shape[0], 3, 2, mode_count, cycle_dev)
    cycle_maps = jnp.einsum(
        "sqemr,emj->sqrj", fourier, dft_table, preferred_element_type=jnp.float32
    )
    products = (pixel_weights * cycle_maps[:, 0:1] * cycle_maps[:, 1:3]).astype(jnp.bfloat16)
    spectra = jnp.einsum("sqrj,emj->sqemr", products, dft_table, preferred_element_type=jnp.float32)
    received = (spectra * pixel_count ** (-0.5)).astype(jnp.bfloat16)
    returned = lax.all_to_all(received, "ma", split_axis=3, concat_axis=4, tiled=True)
    inverse = (
        jnp.zeros((cycle_count,), jnp.int32).at[cycle_order].set(lax.iota(jnp.int32, cycle_count))
    )
    spectra = jnp.take(returned, inverse, axis=4).astype(jnp.float32)
    weighted = analysis_sets(spectra, colatitude, cycle_weight)
    weighted = weighted.reshape(weighted.shape[0], 8, pairs_dev, 2, cycle_count)
    projected = jnp.einsum(
        "scphr,pkr->phsck", weighted, legendre, preferred_element_type=jnp.float32
    )
    merged = jnp.sum(projected * halves.astype(jnp.float32)[:, :, None, None, :], axis=1)
    return estimate(merged, degree, orders, raising_factor, mode_count, cycle_count)


LANES = 128
TURNS = 4
F32 = jnp.float32
BF16 = jnp.bfloat16


def split_tables(mode_count, pixel_count, sims):
    high_count = LANES // (TURNS * sims)
    low_count = pixel_count // high_count
    m = np.arange(mode_count)[:, None]
    low = np.arange(low_count)[None, :]
    high = (np.arange(LANES) // sims % high_count)[None, :] * low_count
    fine = (m * low % pixel_count) * (2.0 * math.pi / pixel_count)
    coarse = (m * high % pixel_count) * (2.0 * math.pi / pixel_count)

    def halves(values):
        upper = values.astype(np.float32).astype(BF16)
        return [upper, (values.astype(np.float32) - upper.astype(np.float32)).astype(BF16)]

    waves = [np.cos(fine).astype(BF16), (-np.sin(fine)).astype(BF16)]
    by_pixel = np.concatenate([wave.T for wave in waves], axis=0)
    by_mode = np.concatenate(waves + halves(np.cos(coarse)) + halves(np.sin(coarse)), axis=1)
    return by_pixel, by_mode


def spread_table(sims):
    comps = 2 * sims
    row = np.arange(LANES)[:, None]
    col = np.arange(6 * LANES)[None, :]
    high_count = LANES // (TURNS * sims)
    row_t, row_g, row_s, row_c = row // (4 * comps), row // comps % 4, row // 2 % sims, row % 2
    col_q, col_c = col // (2 * LANES), col // LANES % 2
    col_t, col_s = col % LANES // (high_count * sims), col % sims
    group_q = np.array([0, 1, 2, 1])[row_g]
    source_c = np.where(col_q == 2, 1 - col_c, col_c)
    sign = np.where((col_q == 2) & (col_c == 0), -1.0, 1.0)
    hit = (row_t == col_t) & (row_s == col_s) & (group_q == col_q) & (row_c == source_c)
    return np.where(hit, sign, 0.0).astype(BF16)


def gather_table(sims):
    comps = 2 * sims
    high_count = LANES // (TURNS * sims)
    row = np.arange(4 * LANES)[:, None]
    col = np.arange(LANES)[None, :]
    hit = row // (2 * LANES) == col // comps % 2
    hit &= row // LANES % 2 == col % 2
    hit &= row % LANES // (high_count * sims) == col // (2 * comps) % TURNS
    hit &= row % sims == col // 2 % sims
    return np.where(hit, 1.0, 0.0).astype(BF16)


def iota(shape, axis):
    return lax.broadcasted_iota(jnp.int32, shape, axis)


def div(values, size):
    return values >> (size.bit_length() - 1)


def mod(values, size):
    return values & (size - 1)


def one_hot(condition):
    return jnp.where(condition, 1.0, 0.0).astype(BF16)


def dot(left, right):
    return jnp.dot(left, right, preferred_element_type=F32)


def dot_t(left, right):
    return lax.dot_general(left, right, (((1,), (1,)), ((), ())), preferred_element_type=F32)


def fused_kernel(
    n, modes, rows, cycles, pixels, sims,
    slots_hbm, cycle_hbm, colat_hbm, weight_hbm, row_hbm, tbar_hbm, twf_hbm, leg_hbm, mask_hbm,
    pixel_hbm, mode_hbm, spread_hbm, gather_hbm,
    grad_ref, curl_ref,
    slots_s, cycle_s, colat_s, weight_s, slots_v, tbar_ref, twf_ref, leg_ref, mask_ref,
    pixel_v, mode_v, spread_v, gather_v,
    leg_all, prev_all, fs_ref, place_ref, keep_ref, synth_ref, anal_ref, high_ref, pixmask_ref,
    send_m, recv_m, send_f, recv_f, send_p, recv_p, load_sem, move_sem,
):
    me = lax.axis_index("ma")
    work = n // TURNS
    pairs = tbar_ref.shape[0]
    comps = 2 * sims
    quad = LANES // (4 * comps)
    groups = pairs // quad
    span = 2 * cycles
    total = pairs * span
    count = n * 2 * pairs
    gh = 2 * groups
    high_count = LANES // (TURNS * sims)
    fine = pixels // high_count
    wide = quad * TURNS * 2 * comps
    seat = lax.rem(lax.div(me, 2), work)
    is_worker = jnp.logical_and(lax.rem(me, 2) == 1, me < 2 * work)

    def slot_of(w, t):
        return 2 * w + t % 2 + t // 2 * 2 * work

    names = [
        (slots_hbm, slots_s), (colat_hbm, colat_s), (cycle_hbm, cycle_s),
        (leg_hbm, leg_ref), (tbar_hbm, tbar_ref), (twf_hbm, twf_ref),
        (mask_hbm, mask_ref), (weight_hbm, weight_s), (row_hbm, slots_v),
        (mode_hbm, mode_v), (pixel_hbm, pixel_v), (spread_hbm, spread_v), (gather_hbm, gather_v),
    ]
    loads = [
        pltpu.make_async_copy(source, target, load_sem.at[at])
        for at, (source, target) in enumerate(names)
    ]
    for load in loads[:6]:
        load.start()
    barrier = pltpu.get_barrier_semaphore()

    @pl.when(is_worker)
    def _():
        for off in range(1, n):
            pl.semaphore_signal(
                barrier, inc=1, device_id={"ma": lax.rem(me + off, n)},
                device_id_type=pl.DeviceIdType.MESH,
            )

    for load in loads[6:8]:
        load.start()

    @pl.when(is_worker)
    def _():
        for load in loads[8:]:
            load.start()

    def remote(source, target, at, to):
        return pltpu.make_async_remote_copy(
            src_ref=source, dst_ref=target, send_sem=move_sem.at[2 * at],
            recv_sem=move_sem.at[2 * at + 1], device_id={"ma": to},
            device_id_type=pl.DeviceIdType.MESH,
        )

    def settle(buffer, at):
        pltpu.make_async_copy(buffer, buffer, move_sem.at[at]).wait()

    @pl.when(jnp.logical_not(is_worker))
    def _():
        pl.semaphore_wait(barrier, work)
        loads[6].wait()
        send_m[...] = mask_ref[...].astype(F32).astype(BF16)
        turn = lax.rem(me, 2) + 2 * lax.div(me, 2 * work)
        remote(send_m, recv_m.at[turn], 2, 2 * lax.div(lax.rem(me, 2 * work), 2) + 1).start()

    for load in loads[:3]:
        load.wait()

    row_shape = (pairs, rows)
    smaller = jnp.zeros(row_shape, jnp.int32)
    for p in range(pairs):
        smaller = jnp.where(iota(row_shape, 0) == p, slots_s[me * pairs + p], smaller)
    k = iota(row_shape, 1)
    upper = k >= modes - smaller
    degree = jnp.where(upper, k - 1, smaller + k).astype(F32)
    orders = jnp.where(upper, modes - 1 - smaller, smaller).astype(F32)
    eps = raising(degree, orders)
    upper_f = jnp.where(upper, 1.0, 0.0)
    lower_f = 1.0 - upper_f

    colat = jnp.zeros((cycles, LANES), F32)
    for r in range(cycles):
        colat = jnp.where(iota(colat.shape, 0) == r, colat_s[r], colat)
    csc = 1.0 / jnp.sin(colat)
    cot = jnp.cos(colat) * csc
    lane_group = mod(div(iota(colat.shape, 1), comps), 4)
    base = jnp.where(lane_group == 0, 1.0, jnp.where(lane_group == 1, cot, csc))

    for load in loads[3:6]:
        load.wait()
    lane = iota((8, LANES), 1)
    lane_quad = div(lane, 4 * comps)
    is_phi = mod(div(lane, comps), 4) == 2
    for g in range(groups):
        sets, legs = [], []
        small = jnp.zeros((8, LANES), jnp.int32)
        for q in range(quad):
            p = g * quad + q
            small = jnp.where(lane_quad == q, slots_s[me * pairs + p], small)
            tbar = jnp.concatenate([tbar_ref[p, s].astype(F32) for s in range(sims)], axis=0)
            twf = jnp.concatenate([twf_ref[p, s].astype(F32) for s in range(sims)], axis=0)
            deg_p, eps_p = degree[p : p + 1] / modes, eps[p : p + 1] / modes
            scaled = -(eps_p * twf)
            raised = jnp.concatenate([scaled[:, 1:], jnp.zeros_like(scaled[:, :1])], axis=1)
            sets += [tbar, deg_p * twf, twf, raised]
            leg = leg_ref[p].astype(F32)
            low, high = lower_f[p : p + 1], upper_f[p : p + 1]
            legs += [leg * low, leg * high]
        legs = jnp.concatenate(legs, axis=0).astype(BF16)
        leg_all[pl.ds(g * quad * span, quad * span), :] = legs
        out = dot_t(legs, jnp.concatenate(sets, axis=0).astype(BF16))
        picked = out[:span]
        for q in range(1, quad):
            own = div(iota(picked.shape, 1), 4 * comps) == q
            picked = jnp.where(own, out[q * span : (q + 1) * span], picked)
        for h in range(2):
            order = (modes - 1 - small if h else small)[0:1]
            norm = jnp.where(order == 0, 1.0, 2.0) * modes ** (-0.5)
            norm = jnp.where(is_phi[0:1], norm * (order.astype(F32) / modes), norm)
            fs_ref[:, 2 * g + h, :] = picked[h * cycles : (h + 1) * cycles] * (base * norm)

    for t in range(TURNS):
        for w in range(work):
            send_f[t, w] = fs_ref[cycle_s[slot_of(w, t)], :gh, :].astype(BF16)

    @pl.when(is_worker)
    def _():
        pl.semaphore_wait(barrier, work - 1)

    for w in range(work):
        @pl.when(me != 2 * w + 1)
        def _():
            remote(send_f.at[:, w], recv_f.at[:, me], 0, 2 * w + 1).start()

    place_shape = (work * gh, total)
    place_row, place_lane = iota(place_shape, 0), iota(place_shape, 1)
    lane_pair, lane_half = div(place_lane, span), mod(div(place_lane, cycles), 2)
    match = mod(place_row, gh) == div(lane_pair, quad) * 2 + lane_half
    slot_row = div(place_row, gh)
    for t in range(TURNS):
        cyc = jnp.zeros(place_shape, jnp.int32)
        for w in range(work):
            cyc = jnp.where(slot_row == w, cycle_s[slot_of(w, t)], cyc)
        place_ref[t] = one_hot(jnp.logical_and(match, cyc == mod(place_lane, cycles)))

    loads[7].wait()
    lane_shape = (8, total)
    cyc = mod(iota(lane_shape, 1), cycles)
    theta_l = jnp.zeros(lane_shape, F32)
    weight_l = jnp.zeros(lane_shape, F32)
    for r in range(cycles):
        theta_l = jnp.where(cyc == r, colat_s[r], theta_l)
        weight_l = jnp.where(cyc == r, weight_s[r], weight_l)
    with_sin = weight_l / jnp.sin(theta_l)
    with_cos = weight_l * jnp.cos(theta_l) / jnp.sin(theta_l)
    owner = div(iota(lane_shape, 1), span)
    for p in range(pairs):
        keep_ref[p, 0] = jnp.where(owner == p, with_cos, 0.0)
        keep_ref[p, 1] = jnp.where(owner == p, with_sin, 0.0)
    for p in range(pairs):
        leg = leg_ref[p].astype(F32)
        prev = jnp.concatenate([jnp.zeros_like(leg[:, :1]), leg[:, : rows - 1]], axis=1)
        low, high = lower_f[p : p + 1], upper_f[p : p + 1]
        prev_all[pl.ds(p * span, span), :] = jnp.concatenate(
            [prev * low, prev * high], axis=0
        ).astype(BF16)
    scale = (modes / cycles) ** 0.5 / jnp.sqrt(jnp.maximum(degree * (degree + 1.0), 1.0))
    f_level, f_eps, f_order = degree * scale, eps * scale, orders * scale

    @pl.when(is_worker)
    def _():
        for load in loads[8:]:
            load.wait()
        pair_count = slots_v.shape[1]

        def pair_of(at):
            source, inner = mod(div(at, gh), n), mod(at, gh)
            return source * pairs + div(inner, 2) * quad + div(at, n * gh)

        slots = jnp.broadcast_to(slots_v[...], (pair_count, pair_count)).astype(F32).astype(BF16)
        spread = one_hot(iota((pair_count, count), 0) == pair_of(iota((pair_count, count), 1)))
        spread_t = one_hot(iota((count, pair_count), 1) == pair_of(iota((count, pair_count), 0)))
        by_lane = dot(slots[:16], spread)[0:8]
        by_lane = jnp.where(mod(iota(by_lane.shape, 1), 2) == 1, modes - 1.0 - by_lane, by_lane)
        by_row = dot_t(spread_t, slots)
        by_row = jnp.where(mod(iota(by_row.shape, 0), 2) == 1, modes - 1.0 - by_row, by_row)
        select = one_hot(iota((modes, count), 0).astype(F32) == by_lane[0:1])
        select_t = jnp.concatenate(
            [
                one_hot((iota(by_row.shape, 1) + at).astype(F32) == by_row)
                for at in range(0, modes, pair_count)
            ],
            axis=1,
        )
        moved = dot(pixel_v[...], select).astype(BF16)
        synth_ref[:, :count] = moved[:fine]
        synth_ref[:, count:] = moved[fine:]
        moved = dot(select_t, mode_v[...])
        anal_ref[:count] = moved[:, :fine].astype(BF16)
        anal_ref[count:] = moved[:, fine : 2 * fine].astype(BF16)
        at = 2 * fine
        for part in range(2):
            high_ref[part] = moved[:, at : at + LANES] + moved[:, at + LANES : at + 2 * LANES]
            at += 2 * LANES

        loads[6].wait()
        recv_f[:, me] = send_f[:, seat]
        recv_m[1] = mask_ref[...].astype(F32).astype(BF16)
        settle(recv_m.at[pl.ds(0, TURNS - 1)], 5)
        both = recv_m[...].astype(F32).reshape(TURNS * mask_ref.shape[0], LANES)
        cut = fine // LANES
        grid = (both.shape[0], LANES)
        m_turn = div(iota(grid, 1), high_count * sims)
        m_high = mod(div(iota(grid, 1), sims), high_count)
        first_row = (m_turn * high_count + m_high) * cut
        both_t = both.T.astype(BF16)
        for at in range(cut):
            pixmask_ref[pl.ds(at * LANES, LANES), :] = dot(
                both_t, one_hot(iota(grid, 0) == first_row + at)
            )

        settle(recv_f.at[:, pl.ds(0, n - 1)], 1)
        turns = [recv_f[t].astype(F32).reshape(n * gh, LANES) for t in range(TURNS)]
        block_lane = div(iota((n * gh, LANES), 1), 4 * comps)
        got = []
        for q in range(quad):
            row = None
            for t in range(TURNS):
                moved_t = turns[t]
                if t != q:
                    moved_t = pltpu.roll(moved_t, (t - q) * 4 * comps % LANES, 1)
                row = moved_t if row is None else jnp.where(block_lane == t, moved_t, row)
            got.append(row.astype(BF16))
        got = jnp.concatenate(got, axis=0)
        spread_f = dot(got, spread_v[...])
        cos_h, sin_h = high_ref[0], high_ref[1]
        real, imag = [], []
        for q in range(3):
            re = spread_f[:, 2 * q * LANES : (2 * q + 1) * LANES]
            im = spread_f[:, (2 * q + 1) * LANES : (2 * q + 2) * LANES]
            real.append((re * cos_h - im * sin_h).astype(BF16))
            imag.append((re * sin_h + im * cos_h).astype(BF16))
        turned = jnp.concatenate(
            [jnp.concatenate(real, axis=1), jnp.concatenate(imag, axis=1)], axis=0
        )
        maps = dot(synth_ref[...], turned)
        lead = pixmask_ref[...] * maps[:, :LANES]
        products = jnp.concatenate(
            [lead * maps[:, LANES : 2 * LANES], lead * maps[:, 2 * LANES :]], axis=1
        ).astype(BF16)
        half = dot(anal_ref[...], products)
        parts = []
        for q in range(2):
            c_part = half[:count, q * LANES : (q + 1) * LANES]
            s_part = half[count:, q * LANES : (q + 1) * LANES]
            parts.append((cos_h * c_part + sin_h * s_part).astype(BF16))
            parts.append((cos_h * s_part - sin_h * c_part).astype(BF16))
        spectra = dot(jnp.concatenate(parts, axis=1), gather_v[...]) * pixels ** (-0.5)
        block = n * gh
        low_half = iota((block, LANES), 1) < LANES // 2
        packed = [
            jnp.where(
                low_half,
                spectra[2 * v * block : (2 * v + 1) * block],
                spectra[(2 * v + 1) * block : (2 * v + 2) * block],
            )
            for v in range(wide // LANES)
        ]
        packed = jnp.concatenate(packed, axis=1).astype(BF16)
        send_p[...] = packed.reshape(n, gh, wide)
        for d in range(n):
            if d % 2 == 0 or d >= 2 * work:
                remote(send_p.at[d], recv_p.at[seat], 1, d).start()
            else:
                @pl.when(me != d)
                def _():
                    remote(send_p.at[d], recv_p.at[seat], 1, d).start()
        recv_p[seat] = send_p[me]
        settle(recv_p.at[pl.ds(0, work - 1)], 3)

    @pl.when(jnp.logical_not(is_worker))
    def _():
        settle(recv_p, 3)

    came = recv_p[...].astype(F32).reshape(work * gh, wide)
    odd = mod(iota(came.shape, 1), 2) == 1
    from_phi = mod(div(iota(came.shape, 1), comps), 2) == 1
    swapped = jnp.where(odd, pltpu.roll(came, 1, 1), pltpu.roll(came, wide - 1, 1))
    swapped = jnp.where(odd == from_phi, -swapped, swapped)
    turned = [came.T.astype(BF16), swapped.T.astype(BF16)]
    step = 2 * comps
    side = quad * step
    by_pair = sum(
        dot(
            jnp.concatenate(
                [
                    half[(q * TURNS + t) * step : (q * TURNS + t + 1) * step]
                    for half in turned
                    for q in range(quad)
                ],
                axis=0,
            ),
            place_ref[t],
        )
        for t in range(TURNS)
    )
    first, second = [], []
    for p in range(pairs):
        at = p % quad * 2 * comps
        theta, phi = by_pair[at : at + comps], by_pair[at + comps : at + 2 * comps]
        at += side
        theta_i, phi_i = by_pair[at : at + comps], by_pair[at + comps : at + 2 * comps]
        with_cos, with_sin = keep_ref[p, 0], keep_ref[p, 1]
        first += [theta * with_cos, phi * with_cos, phi_i * with_sin, theta_i * with_sin]
        second += [theta * with_sin, phi * with_sin]
    here = dot(jnp.concatenate(first, axis=0).astype(BF16), leg_all[...])
    before = dot(jnp.concatenate(second, axis=0).astype(BF16), prev_all[...])
    for p in range(pairs):
        a, b = 4 * comps * p, 2 * comps * p
        lev, ep, az = f_level[p : p + 1], f_eps[p : p + 1], f_order[p : p + 1]
        grad = (
            lev * here[a : a + comps] - ep * before[b : b + comps]
            + az * here[a + 2 * comps : a + 3 * comps]
        )
        curl = (
            lev * here[a + comps : a + 2 * comps] - ep * before[b + comps : b + 2 * comps]
            + az * here[a + 3 * comps : a + 4 * comps]
        )
        for s in range(sims):
            grad_ref[p, s] = grad[2 * s : 2 * s + 2]
            curl_ref[p, s] = curl[2 * s : 2 * s + 2]

    @pl.when(is_worker)
    def _():
        settle(send_f.at[:, pl.ds(0, work - 1)], 0)
        settle(send_p.at[pl.ds(0, n - 1)], 2)

    @pl.when(jnp.logical_not(is_worker))
    def _():
        settle(send_f, 0)
        settle(send_m, 4)


def store_kernel(grad_ref, curl_ref, grad_hbm, curl_hbm, sem):
    copies = [
        pltpu.make_async_copy(grad_ref, grad_hbm, sem.at[0]),
        pltpu.make_async_copy(curl_ref, curl_hbm, sem.at[1]),
    ]
    for copy in copies:
        copy.start()
    for copy in copies:
        copy.wait()


def fused(tbar_alm, twf_alm, legendre, m_slots, cycle_order, colatitude, cycle_weight, pixel_mask, n):
    pairs, sims, _, rows = tbar_alm.shape
    modes = rows - 1
    cycles = legendre.shape[2]
    pixels = pixel_mask.shape[1]
    total = pairs * 2 * cycles
    count = n * 2 * pairs
    work = n // TURNS
    gh = 2 * pairs * 8 * sims // LANES
    fine = pixels * TURNS * sims // LANES
    wide = pairs // (gh // 2) * TURNS * 4 * sims
    by_cycle = jnp.transpose(legendre, (0, 2, 1))
    by_pixel, by_mode = split_tables(modes, pixels, sims)
    tables = [jnp.asarray(x) for x in (by_pixel, by_mode, spread_table(sims), gather_table(sims))]
    vmem, anywhere = pl.BlockSpec(memory_space=pltpu.VMEM), pl.BlockSpec(memory_space=pl.ANY)
    out = pltpu.VMEM(tbar_alm.shape, F32)
    mask_shape = (pixels // LANES, LANES)
    made = pl.pallas_call(
        functools.partial(fused_kernel, n, modes, rows, cycles, pixels, sims),
        out_shape=(out, out),
        in_specs=[anywhere] * 13,
        out_specs=(vmem, vmem),
        scratch_shapes=[
            pltpu.SMEM(m_slots.shape, jnp.int32),
            pltpu.SMEM(cycle_order.shape, jnp.int32),
            pltpu.SMEM(colatitude.shape, F32),
            pltpu.SMEM(cycle_weight.shape, F32),
            pltpu.VMEM((1, m_slots.shape[0]), jnp.int32),
            pltpu.VMEM(tbar_alm.shape, BF16),
            pltpu.VMEM(twf_alm.shape, BF16),
            pltpu.VMEM(by_cycle.shape, BF16),
            pltpu.VMEM(mask_shape, jnp.int32),
        ]
        + [pltpu.VMEM(table.shape, BF16) for table in tables]
        + [
            pltpu.VMEM((total, rows), BF16),
            pltpu.VMEM((total, rows), BF16),
            pltpu.VMEM((cycles, 8, LANES), F32),
            pltpu.VMEM((TURNS, work * gh, total), BF16),
            pltpu.VMEM((pairs, 2, 8, total), F32),
            pltpu.VMEM((fine, 2 * count), BF16),
            pltpu.VMEM((2 * count, fine), BF16),
            pltpu.VMEM((2, count, LANES), F32),
            pltpu.VMEM((fine, LANES), F32),
            pltpu.VMEM(mask_shape, BF16),
            pltpu.VMEM((TURNS,) + mask_shape, BF16),
            pltpu.VMEM((TURNS, work, gh, LANES), BF16),
            pltpu.VMEM((TURNS, n, gh, LANES), BF16),
            pltpu.VMEM((n, gh, wide), BF16),
            pltpu.VMEM((work, gh, wide), BF16),
            pltpu.SemaphoreType.DMA((13,)),
            pltpu.SemaphoreType.DMA((6,)),
        ],
        compiler_params=pltpu.CompilerParams(collective_id=0, has_side_effects=True),
        name="estimator",
    )(
        m_slots, cycle_order, colatitude, cycle_weight, m_slots.reshape(1, -1), tbar_alm,
        twf_alm, by_cycle, pixel_mask.reshape(mask_shape), *tables,
    )
    return pl.pallas_call(
        store_kernel,
        out_shape=(jax.ShapeDtypeStruct(tbar_alm.shape, F32),) * 2,
        in_specs=[vmem] * 2,
        out_specs=[anywhere] * 2,
        scratch_shapes=[pltpu.SemaphoreType.DMA((2,))],
        name="store",
    )(*(pltpu.with_memory_space_constraint(x, pltpu.VMEM) for x in made))


def body(n, *args):
    tbar_alm, legendre, pixel_mask = args[0], args[2], args[7]
    pairs, sims, _, rows = tbar_alm.shape
    cycles = legendre.shape[2]
    pixels = pixel_mask.shape[1]
    fits = (
        pairs == 8
        and cycles == n == 16
        and pixel_mask.shape[0] == 1
        and rows == 257
        and pairs * n == LANES
        and sims == 4
        and pixels == 4096
    )
    return fused(*args, n) if fits else shards(*args)


def solution(mesh):
    return jax.shard_map(
        functools.partial(body, mesh.shape["ma"]),
        mesh=mesh,
        in_specs=(
            P("ma", "grp", None, None),
            P("ma", "grp", None, None),
            P("ma", None, None),
            P(),
            P(),
            P(),
            P(),
            P("ma", None),
        ),
        out_specs=(P("ma", "grp", None, None), P("ma", "grp", None, None)),
        check_vma=False,
    )
```

```python
import math

import functools

import jax
import jax.numpy as jnp
import numpy as np
from jax import lax
from jax.experimental import pallas as pl
from jax.experimental.pallas import tpu as pltpu
from jax.sharding import PartitionSpec as P


def pair_layout(small_orders, mode_count):
    row_index = lax.broadcasted_iota(jnp.int32, (small_orders.shape[0], mode_count + 1), 1)
    smaller = small_orders[:, None]
    upper_half = row_index >= mode_count - smaller
    degree = jnp.where(upper_half, row_index - 1, smaller + row_index)
    orders = jnp.where(upper_half, mode_count - 1 - smaller, smaller + 0 * row_index)
    return (upper_half, degree.astype(jnp.float32), orders.astype(jnp.float32))


def raising(degree, orders):
    square = (
        (degree * degree - orders * orders)
        * (2.0 * degree + 1.0)
        / jnp.maximum(2.0 * degree - 1.0, 1.0)
    )
    return jnp.where(degree > orders, jnp.sqrt(jnp.where(degree > orders, square, 0.0)), 0.0)


def synthesis_sets(tbar_alm, twf_alm, degree, raising_factor, mode_count):
    wiener = twf_alm.astype(jnp.float32)
    scaled = (raising_factor / mode_count)[:, None, None, :] * wiener
    raised = jnp.concatenate([scaled[..., 1:], jnp.zeros_like(scaled[..., :1])], axis=-1)
    stacked = jnp.stack(
        [
            tbar_alm.astype(jnp.float32),
            wiener,
            (degree / mode_count)[:, None, None, :] * wiener,
            raised,
        ],
        axis=2,
    )
    return stacked.reshape(stacked.shape[0], stacked.shape[1], 8, stacked.shape[4]).astype(
        jnp.bfloat16
    )


def mode_columns(small_orders, mode_count):
    return jnp.stack([small_orders, mode_count - 1 - small_orders], axis=1).reshape(-1)


def fourier_table(orders_int, pixel_count):
    pixel_index = lax.broadcasted_iota(jnp.int32, (orders_int.shape[0], pixel_count), 1)
    turns = orders_int[:, None] * pixel_index % pixel_count
    radians = turns.astype(jnp.float32) * (2.0 * math.pi / pixel_count)
    return jnp.stack([jnp.cos(radians), -jnp.sin(radians)], axis=0).astype(jnp.bfloat16)


def combine_modes(legendre_sums, orders_int, cos_cycle, sin_cycle, mode_count):
    orders_real = orders_int.astype(jnp.float32)
    inv_sin = 1.0 / sin_cycle
    ratio = (orders_real / mode_count)[:, None]
    theta_real = (cos_cycle * legendre_sums[:, 4] - legendre_sums[:, 6]) * inv_sin
    theta_imag = (cos_cycle * legendre_sums[:, 5] - legendre_sums[:, 7]) * inv_sin
    phi_real = -ratio * legendre_sums[:, 3] * inv_sin
    phi_imag = ratio * legendre_sums[:, 2] * inv_sin
    weight = (jnp.where(orders_int == 0, 1.0, 2.0) * mode_count ** (-0.5))[:, None]
    stacked = jnp.stack(
        [legendre_sums[:, 0], legendre_sums[:, 1], theta_real, theta_imag, phi_real, phi_imag],
        axis=1,
    )
    return (stacked * weight).astype(jnp.bfloat16)


def analysis_sets(spectra, colatitude, cycle_weight):
    with_cos = cycle_weight * jnp.cos(colatitude) / jnp.sin(colatitude)
    with_sin = cycle_weight / jnp.sin(colatitude)
    stacked = jnp.stack(
        [
            spectra[:, 0] * with_cos,
            spectra[:, 0] * with_sin,
            spectra[:, 1] * with_cos,
            spectra[:, 1] * with_sin,
        ],
        axis=1,
    )
    return stacked.reshape(spectra.shape[0], 8, spectra.shape[3], spectra.shape[4]).astype(
        jnp.bfloat16
    )


def estimate(merged, degree, orders, raising_factor, mode_count, cycle_count):
    level = degree[:, None, :]
    azimuth = orders[:, None, :]
    factor = raising_factor[:, None, :]

    def previous(values):
        return jnp.concatenate([jnp.zeros_like(values[..., :1]), values[..., :-1]], axis=-1)

    grad_real = (
        level * merged[:, :, 0] - factor * previous(merged[:, :, 2]) + azimuth * merged[:, :, 7]
    )
    grad_imag = (
        level * merged[:, :, 1] - factor * previous(merged[:, :, 3]) - azimuth * merged[:, :, 6]
    )
    curl_real = (
        level * merged[:, :, 4] - factor * previous(merged[:, :, 6]) - azimuth * merged[:, :, 3]
    )
    curl_imag = (
        level * merged[:, :, 5] - factor * previous(merged[:, :, 7]) + azimuth * merged[:, :, 2]
    )
    scale = (mode_count / cycle_count) ** 0.5 / jnp.sqrt(jnp.maximum(level * (level + 1.0), 1.0))
    scale = scale[:, :, None, :]
    return (
        jnp.stack([grad_real, grad_imag], axis=2) * scale,
        jnp.stack([curl_real, curl_imag], axis=2) * scale,
    )


def shards(tbar_alm, twf_alm, legendre, m_slots, cycle_order, colatitude, cycle_weight, pixel_mask):
    pairs_dev = tbar_alm.shape[0]
    row_count = tbar_alm.shape[3]
    mode_count = row_count - 1
    cycle_count = legendre.shape[2]
    cycle_dev = pixel_mask.shape[0]
    pixel_count = pixel_mask.shape[1]
    device_slot = lax.axis_index("ma")
    local_small = lax.dynamic_slice_in_dim(m_slots, device_slot * pairs_dev, pairs_dev)
    upper_half, degree, orders = pair_layout(local_small, mode_count)
    raising_factor = raising(degree, orders)
    coeff_sets = synthesis_sets(tbar_alm, twf_alm, degree, raising_factor, mode_count)
    halves = jnp.stack([jnp.logical_not(upper_half), upper_half], axis=1)
    masked = coeff_sets[:, None] * halves.astype(jnp.bfloat16)[:, :, None, None, :]
    legendre_sums = jnp.einsum(
        "phsck,pkr->scphr", masked, legendre, preferred_element_type=jnp.float32
    )
    legendre_sums = jnp.take(legendre_sums, cycle_order, axis=4)
    legendre_sums = legendre_sums.reshape(legendre_sums.shape[0], 8, 2 * pairs_dev, cycle_count)
    all_orders = mode_columns(m_slots, mode_count)
    dft_table = fourier_table(all_orders, pixel_count)
    pixel_weights = pixel_mask.astype(jnp.float32)
    slot_theta = jnp.take(colatitude, cycle_order)
    local_orders = mode_columns(local_small, mode_count)
    outgoing = combine_modes(
        legendre_sums, local_orders, jnp.cos(slot_theta), jnp.sin(slot_theta), mode_count
    )
    fourier = lax.all_to_all(outgoing, "ma", split_axis=3, concat_axis=2, tiled=True)
    fourier = fourier.reshape(fourier.shape[0], 3, 2, mode_count, cycle_dev)
    cycle_maps = jnp.einsum(
        "sqemr,emj->sqrj", fourier, dft_table, preferred_element_type=jnp.float32
    )
    products = (pixel_weights * cycle_maps[:, 0:1] * cycle_maps[:, 1:3]).astype(jnp.bfloat16)
    spectra = jnp.einsum("sqrj,emj->sqemr", products, dft_table, preferred_element_type=jnp.float32)
    received = (spectra * pixel_count ** (-0.5)).astype(jnp.bfloat16)
    returned = lax.all_to_all(received, "ma", split_axis=3, concat_axis=4, tiled=True)
    inverse = (
        jnp.zeros((cycle_count,), jnp.int32).at[cycle_order].set(lax.iota(jnp.int32, cycle_count))
    )
    spectra = jnp.take(returned, inverse, axis=4).astype(jnp.float32)
    weighted = analysis_sets(spectra, colatitude, cycle_weight)
    weighted = weighted.reshape(weighted.shape[0], 8, pairs_dev, 2, cycle_count)
    projected = jnp.einsum(
        "scphr,pkr->phsck", weighted, legendre, preferred_element_type=jnp.float32
    )
    merged = jnp.sum(projected * halves.astype(jnp.float32)[:, :, None, None, :], axis=1)
    return estimate(merged, degree, orders, raising_factor, mode_count, cycle_count)


LANES = 128
TURNS = 4
F32 = jnp.float32
BF16 = jnp.bfloat16


def split_tables(mode_count, pixel_count, sims):
    high_count = LANES // (TURNS * sims)
    low_count = pixel_count // high_count
    m = np.arange(mode_count)[:, None]
    low = np.arange(low_count)[None, :]
    high = (np.arange(LANES) // sims % high_count)[None, :] * low_count
    fine = (m * low % pixel_count) * (2.0 * math.pi / pixel_count)
    coarse = (m * high % pixel_count) * (2.0 * math.pi / pixel_count)

    def halves(values):
        upper = values.astype(np.float32).astype(BF16)
        return [upper, (values.astype(np.float32) - upper.astype(np.float32)).astype(BF16)]

    waves = [np.cos(fine).astype(BF16), (-np.sin(fine)).astype(BF16)]
    by_pixel = np.concatenate([wave.T for wave in waves], axis=0)
    by_mode = np.concatenate(waves + halves(np.cos(coarse)) + halves(np.sin(coarse)), axis=1)
    return by_pixel, by_mode


def spread_table(sims):
    comps = 2 * sims
    row = np.arange(LANES)[:, None]
    col = np.arange(6 * LANES)[None, :]
    high_count = LANES // (TURNS * sims)
    row_t, row_g, row_s, row_c = row // (4 * comps), row // comps % 4, row // 2 % sims, row % 2
    col_q, col_c = col // (2 * LANES), col // LANES % 2
    col_t, col_s = col % LANES // (high_count * sims), col % sims
    group_q = np.array([0, 1, 2, 1])[row_g]
    source_c = np.where(col_q == 2, 1 - col_c, col_c)
    sign = np.where((col_q == 2) & (col_c == 0), -1.0, 1.0)
    hit = (row_t == col_t) & (row_s == col_s) & (group_q == col_q) & (row_c == source_c)
    return np.where(hit, sign, 0.0).astype(BF16)


def gather_table(sims):
    comps = 2 * sims
    high_count = LANES // (TURNS * sims)
    row = np.arange(4 * LANES)[:, None]
    col = np.arange(LANES)[None, :]
    hit = row // (2 * LANES) == col // comps % 2
    hit &= row // LANES % 2 == col % 2
    hit &= row % LANES // (high_count * sims) == col // (2 * comps) % TURNS
    hit &= row % sims == col // 2 % sims
    return np.where(hit, 1.0, 0.0).astype(BF16)


def iota(shape, axis):
    return lax.broadcasted_iota(jnp.int32, shape, axis)


def div(values, size):
    return values >> (size.bit_length() - 1)


def mod(values, size):
    return values & (size - 1)


def one_hot(condition):
    return jnp.where(condition, 1.0, 0.0).astype(BF16)


def dot(left, right):
    return jnp.dot(left, right, preferred_element_type=F32)


def dot_t(left, right):
    return lax.dot_general(left, right, (((1,), (1,)), ((), ())), preferred_element_type=F32)


def fused_kernel(
    n, modes, rows, cycles, pixels, sims,
    slots_hbm, cycle_hbm, colat_hbm, weight_hbm, row_hbm, tbar_hbm, twf_hbm, leg_hbm, mask_hbm,
    pixel_hbm, mode_hbm, spread_hbm, gather_hbm,
    grad_ref, curl_ref,
    slots_s, cycle_s, colat_s, weight_s, slots_v, tbar_ref, twf_ref, leg_ref, mask_ref,
    pixel_v, mode_v, spread_v, gather_v,
    leg_all, prev_all, fs_ref, place_ref, keep_ref, synth_ref, synth_l, anal_ref, anal_c, high_ref,
    pixmask_ref, maps_ref,
    send_m, recv_m, send_f, recv_f, send_p, recv_p, load_sem, move_sem,
):
    me = lax.axis_index("ma")
    work = n // TURNS
    pairs = tbar_ref.shape[0]
    comps = 2 * sims
    quad = LANES // (4 * comps)
    groups = pairs // quad
    span = 2 * cycles
    total = pairs * span
    count = n * 2 * pairs
    gh = 2 * groups
    high_count = LANES // (TURNS * sims)
    fine = pixels // high_count
    wide = quad * TURNS * 2 * comps
    seat = lax.rem(lax.div(me, 2), work)
    prompt = n - n // 4
    first = 2 * gh
    is_worker = jnp.logical_and(lax.rem(me, 2) == 1, me < 2 * work)

    def slot_of(w, t):
        return 2 * w + t % 2 + t // 2 * 2 * work

    names = [
        (slots_hbm, slots_s), (colat_hbm, colat_s), (cycle_hbm, cycle_s),
        (leg_hbm, leg_ref), (tbar_hbm, tbar_ref), (twf_hbm, twf_ref),
        (mask_hbm, mask_ref), (weight_hbm, weight_s), (row_hbm, slots_v),
        (mode_hbm, mode_v), (pixel_hbm, pixel_v), (spread_hbm, spread_v), (gather_hbm, gather_v),
    ]
    loads = [
        pltpu.make_async_copy(source, target, load_sem.at[at])
        for at, (source, target) in enumerate(names)
    ]
    for load in loads[:6]:
        load.start()
    barrier = pltpu.get_barrier_semaphore()

    @pl.when(is_worker)
    def _():
        for off in range(1, n):
            pl.semaphore_signal(
                barrier, inc=1, device_id={"ma": lax.rem(me + off, n)},
                device_id_type=pl.DeviceIdType.MESH,
            )

    for load in loads[6:8]:
        load.start()

    @pl.when(is_worker)
    def _():
        for load in loads[8:]:
            load.start()

    def remote(source, target, at, to, mark=None):
        return pltpu.make_async_remote_copy(
            src_ref=source, dst_ref=target, send_sem=move_sem.at[2 * at],
            recv_sem=move_sem.at[2 * at + 1 if mark is None else mark], device_id={"ma": to},
            device_id_type=pl.DeviceIdType.MESH,
        )

    def settle(buffer, at):
        pltpu.make_async_copy(buffer, buffer, move_sem.at[at]).wait()

    @pl.when(jnp.logical_not(is_worker))
    def _():
        pl.semaphore_wait(barrier, work)
        loads[6].wait()
        send_m[...] = mask_ref[...].astype(F32).astype(BF16)
        turn = lax.rem(me, 2) + 2 * lax.div(me, 2 * work)
        remote(send_m, recv_m.at[turn], 2, 2 * lax.div(lax.rem(me, 2 * work), 2) + 1).start()

    for load in loads[:3]:
        load.wait()

    row_shape = (pairs, rows)
    smaller = jnp.zeros(row_shape, jnp.int32)
    for p in range(pairs):
        smaller = jnp.where(iota(row_shape, 0) == p, slots_s[me * pairs + p], smaller)
    k = iota(row_shape, 1)
    upper = k >= modes - smaller
    degree = jnp.where(upper, k - 1, smaller + k).astype(F32)
    orders = jnp.where(upper, modes - 1 - smaller, smaller).astype(F32)
    eps = raising(degree, orders)
    upper_f = jnp.where(upper, 1.0, 0.0)
    lower_f = 1.0 - upper_f

    colat = jnp.zeros((cycles, LANES), F32)
    for r in range(cycles):
        colat = jnp.where(iota(colat.shape, 0) == r, colat_s[r], colat)
    csc = 1.0 / jnp.sin(colat)
    cot = jnp.cos(colat) * csc
    lane_group = mod(div(iota(colat.shape, 1), comps), 4)
    base = jnp.where(lane_group == 0, 1.0, jnp.where(lane_group == 1, cot, csc))

    for load in loads[3:6]:
        load.wait()
    lane = iota((8, LANES), 1)
    lane_quad = div(lane, 4 * comps)
    is_phi = mod(div(lane, comps), 4) == 2
    for g in range(groups):
        sets, legs = [], []
        small = jnp.zeros((8, LANES), jnp.int32)
        for q in range(quad):
            p = g * quad + q
            small = jnp.where(lane_quad == q, slots_s[me * pairs + p], small)
            tbar = jnp.concatenate([tbar_ref[p, s].astype(F32) for s in range(sims)], axis=0)
            twf = jnp.concatenate([twf_ref[p, s].astype(F32) for s in range(sims)], axis=0)
            deg_p, eps_p = degree[p : p + 1] / modes, eps[p : p + 1] / modes
            scaled = -(eps_p * twf)
            raised = jnp.concatenate([scaled[:, 1:], jnp.zeros_like(scaled[:, :1])], axis=1)
            sets += [tbar, deg_p * twf, twf, raised]
            leg = leg_ref[p].astype(F32)
            low, high = lower_f[p : p + 1], upper_f[p : p + 1]
            legs += [leg * low, leg * high]
        legs = jnp.concatenate(legs, axis=0).astype(BF16)
        leg_all[pl.ds(g * quad * span, quad * span), :] = legs
        out = dot_t(legs, jnp.concatenate(sets, axis=0).astype(BF16))
        picked = out[:span]
        for q in range(1, quad):
            own = div(iota(picked.shape, 1), 4 * comps) == q
            picked = jnp.where(own, out[q * span : (q + 1) * span], picked)
        for h in range(2):
            order = (modes - 1 - small if h else small)[0:1]
            norm = jnp.where(order == 0, 1.0, 2.0) * modes ** (-0.5)
            norm = jnp.where(is_phi[0:1], norm * (order.astype(F32) / modes), norm)
            fs_ref[:, 2 * g + h, :] = picked[h * cycles : (h + 1) * cycles] * (base * norm)

    for t in range(TURNS):
        for w in range(work):
            send_f[t, w] = fs_ref[cycle_s[slot_of(w, t)], :gh, :].astype(BF16)

    @pl.when(is_worker)
    def _():
        pl.semaphore_wait(barrier, work - 1)

    tardy = 1 + 5 * lax.div(me, prompt)
    for w in range(work):
        @pl.when(me != 2 * w + 1)
        def _():
            remote(send_f.at[:, w], recv_f.at[:, me], 0, 2 * w + 1, tardy).start()

    place_shape = (work * gh, total)
    place_row, place_lane = iota(place_shape, 0), iota(place_shape, 1)
    lane_pair, lane_half = div(place_lane, span), mod(div(place_lane, cycles), 2)
    match = mod(place_row, gh) == div(lane_pair, quad) * 2 + lane_half
    slot_row = div(place_row, gh)
    for t in range(TURNS):
        cyc = jnp.zeros(place_shape, jnp.int32)
        for w in range(work):
            cyc = jnp.where(slot_row == w, cycle_s[slot_of(w, t)], cyc)
        place_ref[t] = one_hot(jnp.logical_and(match, cyc == mod(place_lane, cycles)))

    loads[7].wait()
    lane_shape = (8, total)
    cyc = mod(iota(lane_shape, 1), cycles)
    theta_l = jnp.zeros(lane_shape, F32)
    weight_l = jnp.zeros(lane_shape, F32)
    for r in range(cycles):
        theta_l = jnp.where(cyc == r, colat_s[r], theta_l)
        weight_l = jnp.where(cyc == r, weight_s[r], weight_l)
    with_sin = weight_l / jnp.sin(theta_l)
    with_cos = weight_l * jnp.cos(theta_l) / jnp.sin(theta_l)
    owner = div(iota(lane_shape, 1), span)
    for p in range(pairs):
        keep_ref[p, 0] = jnp.where(owner == p, with_cos, 0.0)
        keep_ref[p, 1] = jnp.where(owner == p, with_sin, 0.0)
    for p in range(pairs):
        leg = leg_ref[p].astype(F32)
        prev = jnp.concatenate([jnp.zeros_like(leg[:, :1]), leg[:, : rows - 1]], axis=1)
        low, high = lower_f[p : p + 1], upper_f[p : p + 1]
        prev_all[pl.ds(p * span, span), :] = jnp.concatenate(
            [prev * low, prev * high], axis=0
        ).astype(BF16)
    scale = (modes / cycles) ** 0.5 / jnp.sqrt(jnp.maximum(degree * (degree + 1.0), 1.0))
    f_level, f_eps, f_order = degree * scale, eps * scale, orders * scale

    @pl.when(is_worker)
    def _():
        for load in loads[8:]:
            load.wait()
        pair_count = slots_v.shape[1]

        ahead = prompt * gh

        def pair_of(at):
            behind = at >= quad * ahead
            rest = at - quad * ahead
            early = (at * (65536 // ahead + 1)) >> 16
            q = jnp.where(behind, div(rest, (n - prompt) * gh), early)
            inner = jnp.where(behind, ahead + mod(rest, (n - prompt) * gh), at - ahead * early)
            return div(inner, gh) * pairs + div(mod(inner, gh), 2) * quad + q

        slots = jnp.broadcast_to(slots_v[...], (pair_count, pair_count)).astype(F32).astype(BF16)
        spread = one_hot(iota((pair_count, count), 0) == pair_of(iota((pair_count, count), 1)))
        spread_t = one_hot(iota((count, pair_count), 1) == pair_of(iota((count, pair_count), 0)))
        by_lane = dot(slots[:16], spread)[0:8]
        by_lane = jnp.where(mod(iota(by_lane.shape, 1), 2) == 1, modes - 1.0 - by_lane, by_lane)
        by_row = dot_t(spread_t, slots)
        by_row = jnp.where(mod(iota(by_row.shape, 0), 2) == 1, modes - 1.0 - by_row, by_row)
        select = one_hot(iota((modes, count), 0).astype(F32) == by_lane[0:1])
        select_t = jnp.concatenate(
            [
                one_hot((iota(by_row.shape, 1) + at).astype(F32) == by_row)
                for at in range(0, modes, pair_count)
            ],
            axis=1,
        )
        moved = dot(pixel_v[...], select).astype(BF16)
        cut_at = quad * ahead
        synth_ref[...] = jnp.concatenate([moved[:fine, :cut_at], moved[fine:, :cut_at]], axis=1)
        synth_l[...] = jnp.concatenate([moved[:fine, cut_at:], moved[fine:, cut_at:]], axis=1)
        moved = dot(select_t, mode_v[...])
        anal_ref[:count] = moved[:, :fine].astype(BF16)
        anal_ref[count:] = moved[:, fine : 2 * fine].astype(BF16)
        anal_c[...] = jnp.concatenate(
            [
                moved[q * ahead : q * ahead + first, part * fine : (part + 1) * fine]
                for part in range(2)
                for q in range(quad)
            ],
            axis=0,
        ).astype(BF16)
        at = 2 * fine
        for part in range(2):
            high_ref[part] = moved[:, at : at + LANES] + moved[:, at + LANES : at + 2 * LANES]
            at += 2 * LANES

        loads[6].wait()
        recv_f[:, me] = send_f[:, seat]
        recv_m[1] = mask_ref[...].astype(F32).astype(BF16)
        settle(recv_m.at[pl.ds(0, TURNS - 1)], 5)
        both = recv_m[...].astype(F32).reshape(TURNS * mask_ref.shape[0], LANES)
        cut = fine // LANES
        grid = (both.shape[0], LANES)
        m_turn = div(iota(grid, 1), high_count * sims)
        m_high = mod(div(iota(grid, 1), sims), high_count)
        first_row = (m_turn * high_count + m_high) * cut
        both_t = both.T.astype(BF16)
        for at in range(cut):
            pixmask_ref[pl.ds(at * LANES, LANES), :] = dot(
                both_t, one_hot(iota(grid, 0) == first_row + at)
            )

        def turn_up(sources, rows_at, size):
            lanes_of = (size // quad, LANES)
            turns = [
                recv_f[t, pl.ds(sources, size // quad // gh)].astype(F32).reshape(lanes_of)
                for t in range(TURNS)
            ]
            block_lane = div(iota(lanes_of, 1), 4 * comps)
            got = []
            for q in range(quad):
                row = None
                for t in range(TURNS):
                    moved_t = turns[t]
                    if t != q:
                        moved_t = pltpu.roll(moved_t, (t - q) * 4 * comps % LANES, 1)
                    row = moved_t if row is None else jnp.where(block_lane == t, moved_t, row)
                got.append(row.astype(BF16))
            spread_f = dot(jnp.concatenate(got, axis=0), spread_v[...])
            cos_h, sin_h = high_ref[0, pl.ds(rows_at, size)], high_ref[1, pl.ds(rows_at, size)]
            real, imag = [], []
            for q in range(3):
                re = spread_f[:, 2 * q * LANES : (2 * q + 1) * LANES]
                im = spread_f[:, (2 * q + 1) * LANES : (2 * q + 2) * LANES]
                real.append((re * cos_h - im * sin_h).astype(BF16))
                imag.append((re * sin_h + im * cos_h).astype(BF16))
            return jnp.concatenate(
                [jnp.concatenate(real, axis=1), jnp.concatenate(imag, axis=1)], axis=0
            )

        settle(recv_f.at[:, pl.ds(0, prompt - 1)], 1)
        maps_ref[...] = dot(synth_ref[...], turn_up(0, 0, cut_at))
        settle(recv_f.at[:, pl.ds(0, n - prompt)], 6)
        maps = maps_ref[...] + dot(synth_l[...], turn_up(prompt, cut_at, count - cut_at))
        lead = pixmask_ref[...] * maps[:, :LANES]
        products = jnp.concatenate(
            [lead * maps[:, LANES : 2 * LANES], lead * maps[:, 2 * LANES :]], axis=1
        ).astype(BF16)
        def bring_down(table, cos_h, sin_h):
            size = cos_h.shape[0]
            half = dot(table, products)
            parts = []
            for q in range(2):
                c_part = half[:size, q * LANES : (q + 1) * LANES]
                s_part = half[size:, q * LANES : (q + 1) * LANES]
                parts.append((cos_h * c_part + sin_h * s_part).astype(BF16))
                parts.append((cos_h * s_part - sin_h * c_part).astype(BF16))
            return dot(jnp.concatenate(parts, axis=1), gather_v[...]) * pixels ** (-0.5)

        def pack(blocks):
            low_half = iota(blocks[0].shape, 1) < LANES // 2
            pieces = [
                jnp.where(low_half, blocks[2 * v], blocks[2 * v + 1])
                for v in range(wide // LANES)
            ]
            whole = jnp.concatenate(pieces, axis=1).astype(BF16)
            return whole.reshape(whole.shape[0] // gh, gh, wide)

        high_c = [
            jnp.concatenate([high_ref[part, pl.ds(q * ahead, first)] for q in range(quad)], axis=0)
            for part in range(2)
        ]
        spectra = bring_down(anal_c[...], *high_c)
        send_p[pl.ds(0, 2)] = pack([spectra[q * first : (q + 1) * first] for q in range(quad)])
        remote(send_p.at[0], recv_p.at[seat], 1, 0).start()

        @pl.when(me != 1)
        def _():
            remote(send_p.at[1], recv_p.at[seat], 1, 1).start()

        spectra = bring_down(anal_ref[...], high_ref[0], high_ref[1])
        behind = n - prompt
        blocks = [
            jnp.concatenate(
                [
                    spectra[q * ahead + first : (q + 1) * ahead],
                    spectra[cut_at + q * behind * gh : cut_at + (q + 1) * behind * gh],
                ],
                axis=0,
            )
            for q in range(quad)
        ]
        send_p[pl.ds(2, n - 2)] = pack(blocks)
        for d in range(2, n):
            if d % 2 == 0 or d >= 2 * work:
                remote(send_p.at[d], recv_p.at[seat], 1, d).start()
            else:
                @pl.when(me != d)
                def _():
                    remote(send_p.at[d], recv_p.at[seat], 1, d).start()
        recv_p[seat] = send_p[me]
        settle(recv_p.at[pl.ds(0, work - 1)], 3)

    @pl.when(jnp.logical_not(is_worker))
    def _():
        settle(recv_p, 3)

    came = recv_p[...].astype(F32).reshape(work * gh, wide)
    odd = mod(iota(came.shape, 1), 2) == 1
    from_phi = mod(div(iota(came.shape, 1), comps), 2) == 1
    swapped = jnp.where(odd, pltpu.roll(came, 1, 1), pltpu.roll(came, wide - 1, 1))
    swapped = jnp.where(odd == from_phi, -swapped, swapped)
    turned = [came.T.astype(BF16), swapped.T.astype(BF16)]
    step = 2 * comps
    side = quad * step
    by_pair = sum(
        dot(
            jnp.concatenate(
                [
                    half[(q * TURNS + t) * step : (q * TURNS + t + 1) * step]
                    for half in turned
                    for q in range(quad)
                ],
                axis=0,
            ),
            place_ref[t],
        )
        for t in range(TURNS)
    )
    first, second = [], []
    for p in range(pairs):
        at = p % quad * 2 * comps
        theta, phi = by_pair[at : at + comps], by_pair[at + comps : at + 2 * comps]
        at += side
        theta_i, phi_i = by_pair[at : at + comps], by_pair[at + comps : at + 2 * comps]
        with_cos, with_sin = keep_ref[p, 0], keep_ref[p, 1]
        first += [theta * with_cos, phi * with_cos, phi_i * with_sin, theta_i * with_sin]
        second += [theta * with_sin, phi * with_sin]
    here = dot(jnp.concatenate(first, axis=0).astype(BF16), leg_all[...])
    before = dot(jnp.concatenate(second, axis=0).astype(BF16), prev_all[...])
    for p in range(pairs):
        a, b = 4 * comps * p, 2 * comps * p
        lev, ep, az = f_level[p : p + 1], f_eps[p : p + 1], f_order[p : p + 1]
        grad = (
            lev * here[a : a + comps] - ep * before[b : b + comps]
            + az * here[a + 2 * comps : a + 3 * comps]
        )
        curl = (
            lev * here[a + comps : a + 2 * comps] - ep * before[b + comps : b + 2 * comps]
            + az * here[a + 3 * comps : a + 4 * comps]
        )
        for s in range(sims):
            grad_ref[p, s] = grad[2 * s : 2 * s + 2]
            curl_ref[p, s] = curl[2 * s : 2 * s + 2]

    @pl.when(is_worker)
    def _():
        settle(send_f.at[:, pl.ds(0, work - 1)], 0)
        settle(send_p.at[pl.ds(0, n - 1)], 2)

    @pl.when(jnp.logical_not(is_worker))
    def _():
        settle(send_f, 0)
        settle(send_m, 4)


def store_kernel(grad_ref, curl_ref, grad_hbm, curl_hbm, sem):
    copies = [
        pltpu.make_async_copy(grad_ref, grad_hbm, sem.at[0]),
        pltpu.make_async_copy(curl_ref, curl_hbm, sem.at[1]),
    ]
    for copy in copies:
        copy.start()
    for copy in copies:
        copy.wait()


def fused(tbar_alm, twf_alm, legendre, m_slots, cycle_order, colatitude, cycle_weight, pixel_mask, n):
    pairs, sims, _, rows = tbar_alm.shape
    modes = rows - 1
    cycles = legendre.shape[2]
    pixels = pixel_mask.shape[1]
    total = pairs * 2 * cycles
    count = n * 2 * pairs
    work = n // TURNS
    gh = 2 * pairs * 8 * sims // LANES
    fine = pixels * TURNS * sims // LANES
    wide = pairs // (gh // 2) * TURNS * 4 * sims
    by_cycle = jnp.transpose(legendre, (0, 2, 1))
    by_pixel, by_mode = split_tables(modes, pixels, sims)
    tables = [jnp.asarray(x) for x in (by_pixel, by_mode, spread_table(sims), gather_table(sims))]
    vmem, anywhere = pl.BlockSpec(memory_space=pltpu.VMEM), pl.BlockSpec(memory_space=pl.ANY)
    out = pltpu.VMEM(tbar_alm.shape, F32)
    mask_shape = (pixels // LANES, LANES)
    made = pl.pallas_call(
        functools.partial(fused_kernel, n, modes, rows, cycles, pixels, sims),
        out_shape=(out, out),
        in_specs=[anywhere] * 13,
        out_specs=(vmem, vmem),
        scratch_shapes=[
            pltpu.SMEM(m_slots.shape, jnp.int32),
            pltpu.SMEM(cycle_order.shape, jnp.int32),
            pltpu.SMEM(colatitude.shape, F32),
            pltpu.SMEM(cycle_weight.shape, F32),
            pltpu.VMEM((1, m_slots.shape[0]), jnp.int32),
            pltpu.VMEM(tbar_alm.shape, BF16),
            pltpu.VMEM(twf_alm.shape, BF16),
            pltpu.VMEM(by_cycle.shape, BF16),
            pltpu.VMEM(mask_shape, jnp.int32),
        ]
        + [pltpu.VMEM(table.shape, BF16) for table in tables]
        + [
            pltpu.VMEM((total, rows), BF16),
            pltpu.VMEM((total, rows), BF16),
            pltpu.VMEM((cycles, 8, LANES), F32),
            pltpu.VMEM((TURNS, work * gh, total), BF16),
            pltpu.VMEM((pairs, 2, 8, total), F32),
            pltpu.VMEM((fine, 2 * count - count // 2), BF16),
            pltpu.VMEM((fine, count // 2), BF16),
            pltpu.VMEM((2 * count, fine), BF16),
            pltpu.VMEM((count // 4, fine), BF16),
            pltpu.VMEM((2, count, LANES), F32),
            pltpu.VMEM((fine, LANES), F32),
            pltpu.VMEM((fine, 3 * LANES), F32),
            pltpu.VMEM(mask_shape, BF16),
            pltpu.VMEM((TURNS,) + mask_shape, BF16),
            pltpu.VMEM((TURNS, work, gh, LANES), BF16),
            pltpu.VMEM((TURNS, n, gh, LANES), BF16),
            pltpu.VMEM((n, gh, wide), BF16),
            pltpu.VMEM((work, gh, wide), BF16),
            pltpu.SemaphoreType.DMA((13,)),
            pltpu.SemaphoreType.DMA((7,)),
        ],
        compiler_params=pltpu.CompilerParams(collective_id=0, has_side_effects=True),
        name="estimator",
    )(
        m_slots, cycle_order, colatitude, cycle_weight, m_slots.reshape(1, -1), tbar_alm,
        twf_alm, by_cycle, pixel_mask.reshape(mask_shape), *tables,
    )
    return pl.pallas_call(
        store_kernel,
        out_shape=(jax.ShapeDtypeStruct(tbar_alm.shape, F32),) * 2,
        in_specs=[vmem] * 2,
        out_specs=[anywhere] * 2,
        scratch_shapes=[pltpu.SemaphoreType.DMA((2,))],
        name="store",
    )(*(pltpu.with_memory_space_constraint(x, pltpu.VMEM) for x in made))


def body(n, *args):
    tbar_alm, legendre, pixel_mask = args[0], args[2], args[7]
    pairs, sims, _, rows = tbar_alm.shape
    cycles = legendre.shape[2]
    pixels = pixel_mask.shape[1]
    fits = (
        pairs == 8
        and cycles == n == 16
        and pixel_mask.shape[0] == 1
        and rows == 257
        and pairs * n == LANES
        and sims == 4
        and pixels == 4096
    )
    return fused(*args, n) if fits else shards(*args)


def solution(mesh):
    return jax.shard_map(
        functools.partial(body, mesh.shape["ma"]),
        mesh=mesh,
        in_specs=(
            P("ma", "grp", None, None),
            P("ma", "grp", None, None),
            P("ma", None, None),
            P(),
            P(),
            P(),
            P(),
            P("ma", None),
        ),
        out_specs=(P("ma", "grp", None, None), P("ma", "grp", None, None)),
        check_vma=False,
    )
```

```python
import math

import functools

import jax
import jax.numpy as jnp
import numpy as np
from jax import lax
from jax.experimental import pallas as pl
from jax.experimental.pallas import tpu as pltpu
from jax.sharding import PartitionSpec as P


def pair_layout(small_orders, mode_count):
    row_index = lax.broadcasted_iota(jnp.int32, (small_orders.shape[0], mode_count + 1), 1)
    smaller = small_orders[:, None]
    upper_half = row_index >= mode_count - smaller
    degree = jnp.where(upper_half, row_index - 1, smaller + row_index)
    orders = jnp.where(upper_half, mode_count - 1 - smaller, smaller + 0 * row_index)
    return (upper_half, degree.astype(jnp.float32), orders.astype(jnp.float32))


def raising(degree, orders):
    square = (
        (degree * degree - orders * orders)
        * (2.0 * degree + 1.0)
        / jnp.maximum(2.0 * degree - 1.0, 1.0)
    )
    return jnp.where(degree > orders, jnp.sqrt(jnp.where(degree > orders, square, 0.0)), 0.0)


def synthesis_sets(tbar_alm, twf_alm, degree, raising_factor, mode_count):
    wiener = twf_alm.astype(jnp.float32)
    scaled = (raising_factor / mode_count)[:, None, None, :] * wiener
    raised = jnp.concatenate([scaled[..., 1:], jnp.zeros_like(scaled[..., :1])], axis=-1)
    stacked = jnp.stack(
        [
            tbar_alm.astype(jnp.float32),
            wiener,
            (degree / mode_count)[:, None, None, :] * wiener,
            raised,
        ],
        axis=2,
    )
    return stacked.reshape(stacked.shape[0], stacked.shape[1], 8, stacked.shape[4]).astype(
        jnp.bfloat16
    )


def mode_columns(small_orders, mode_count):
    return jnp.stack([small_orders, mode_count - 1 - small_orders], axis=1).reshape(-1)


def fourier_table(orders_int, pixel_count):
    pixel_index = lax.broadcasted_iota(jnp.int32, (orders_int.shape[0], pixel_count), 1)
    turns = orders_int[:, None] * pixel_index % pixel_count
    radians = turns.astype(jnp.float32) * (2.0 * math.pi / pixel_count)
    return jnp.stack([jnp.cos(radians), -jnp.sin(radians)], axis=0).astype(jnp.bfloat16)


def combine_modes(legendre_sums, orders_int, cos_cycle, sin_cycle, mode_count):
    orders_real = orders_int.astype(jnp.float32)
    inv_sin = 1.0 / sin_cycle
    ratio = (orders_real / mode_count)[:, None]
    theta_real = (cos_cycle * legendre_sums[:, 4] - legendre_sums[:, 6]) * inv_sin
    theta_imag = (cos_cycle * legendre_sums[:, 5] - legendre_sums[:, 7]) * inv_sin
    phi_real = -ratio * legendre_sums[:, 3] * inv_sin
    phi_imag = ratio * legendre_sums[:, 2] * inv_sin
    weight = (jnp.where(orders_int == 0, 1.0, 2.0) * mode_count ** (-0.5))[:, None]
    stacked = jnp.stack(
        [legendre_sums[:, 0], legendre_sums[:, 1], theta_real, theta_imag, phi_real, phi_imag],
        axis=1,
    )
    return (stacked * weight).astype(jnp.bfloat16)


def analysis_sets(spectra, colatitude, cycle_weight):
    with_cos = cycle_weight * jnp.cos(colatitude) / jnp.sin(colatitude)
    with_sin = cycle_weight / jnp.sin(colatitude)
    stacked = jnp.stack(
        [
            spectra[:, 0] * with_cos,
            spectra[:, 0] * with_sin,
            spectra[:, 1] * with_cos,
            spectra[:, 1] * with_sin,
        ],
        axis=1,
    )
    return stacked.reshape(spectra.shape[0], 8, spectra.shape[3], spectra.shape[4]).astype(
        jnp.bfloat16
    )


def estimate(merged, degree, orders, raising_factor, mode_count, cycle_count):
    level = degree[:, None, :]
    azimuth = orders[:, None, :]
    factor = raising_factor[:, None, :]

    def previous(values):
        return jnp.concatenate([jnp.zeros_like(values[..., :1]), values[..., :-1]], axis=-1)

    grad_real = (
        level * merged[:, :, 0] - factor * previous(merged[:, :, 2]) + azimuth * merged[:, :, 7]
    )
    grad_imag = (
        level * merged[:, :, 1] - factor * previous(merged[:, :, 3]) - azimuth * merged[:, :, 6]
    )
    curl_real = (
        level * merged[:, :, 4] - factor * previous(merged[:, :, 6]) - azimuth * merged[:, :, 3]
    )
    curl_imag = (
        level * merged[:, :, 5] - factor * previous(merged[:, :, 7]) + azimuth * merged[:, :, 2]
    )
    scale = (mode_count / cycle_count) ** 0.5 / jnp.sqrt(jnp.maximum(level * (level + 1.0), 1.0))
    scale = scale[:, :, None, :]
    return (
        jnp.stack([grad_real, grad_imag], axis=2) * scale,
        jnp.stack([curl_real, curl_imag], axis=2) * scale,
    )


def shards(tbar_alm, twf_alm, legendre, m_slots, cycle_order, colatitude, cycle_weight, pixel_mask):
    pairs_dev = tbar_alm.shape[0]
    row_count = tbar_alm.shape[3]
    mode_count = row_count - 1
    cycle_count = legendre.shape[2]
    cycle_dev = pixel_mask.shape[0]
    pixel_count = pixel_mask.shape[1]
    device_slot = lax.axis_index("ma")
    local_small = lax.dynamic_slice_in_dim(m_slots, device_slot * pairs_dev, pairs_dev)
    upper_half, degree, orders = pair_layout(local_small, mode_count)
    raising_factor = raising(degree, orders)
    coeff_sets = synthesis_sets(tbar_alm, twf_alm, degree, raising_factor, mode_count)
    halves = jnp.stack([jnp.logical_not(upper_half), upper_half], axis=1)
    masked = coeff_sets[:, None] * halves.astype(jnp.bfloat16)[:, :, None, None, :]
    legendre_sums = jnp.einsum(
        "phsck,pkr->scphr", masked, legendre, preferred_element_type=jnp.float32
    )
    legendre_sums = jnp.take(legendre_sums, cycle_order, axis=4)
    legendre_sums = legendre_sums.reshape(legendre_sums.shape[0], 8, 2 * pairs_dev, cycle_count)
    all_orders = mode_columns(m_slots, mode_count)
    dft_table = fourier_table(all_orders, pixel_count)
    pixel_weights = pixel_mask.astype(jnp.float32)
    slot_theta = jnp.take(colatitude, cycle_order)
    local_orders = mode_columns(local_small, mode_count)
    outgoing = combine_modes(
        legendre_sums, local_orders, jnp.cos(slot_theta), jnp.sin(slot_theta), mode_count
    )
    fourier = lax.all_to_all(outgoing, "ma", split_axis=3, concat_axis=2, tiled=True)
    fourier = fourier.reshape(fourier.shape[0], 3, 2, mode_count, cycle_dev)
    cycle_maps = jnp.einsum(
        "sqemr,emj->sqrj", fourier, dft_table, preferred_element_type=jnp.float32
    )
    products = (pixel_weights * cycle_maps[:, 0:1] * cycle_maps[:, 1:3]).astype(jnp.bfloat16)
    spectra = jnp.einsum("sqrj,emj->sqemr", products, dft_table, preferred_element_type=jnp.float32)
    received = (spectra * pixel_count ** (-0.5)).astype(jnp.bfloat16)
    returned = lax.all_to_all(received, "ma", split_axis=3, concat_axis=4, tiled=True)
    inverse = (
        jnp.zeros((cycle_count,), jnp.int32).at[cycle_order].set(lax.iota(jnp.int32, cycle_count))
    )
    spectra = jnp.take(returned, inverse, axis=4).astype(jnp.float32)
    weighted = analysis_sets(spectra, colatitude, cycle_weight)
    weighted = weighted.reshape(weighted.shape[0], 8, pairs_dev, 2, cycle_count)
    projected = jnp.einsum(
        "scphr,pkr->phsck", weighted, legendre, preferred_element_type=jnp.float32
    )
    merged = jnp.sum(projected * halves.astype(jnp.float32)[:, :, None, None, :], axis=1)
    return estimate(merged, degree, orders, raising_factor, mode_count, cycle_count)


LANES = 128
TURNS = 4
F32 = jnp.float32
BF16 = jnp.bfloat16


def split_tables(mode_count, pixel_count, sims):
    high_count = LANES // (TURNS * sims)
    low_count = pixel_count // high_count
    m = np.arange(mode_count)[:, None]
    low = np.arange(low_count)[None, :]
    high = (np.arange(LANES) // sims % high_count)[None, :] * low_count
    fine = (m * low % pixel_count) * (2.0 * math.pi / pixel_count)
    coarse = (m * high % pixel_count) * (2.0 * math.pi / pixel_count)

    def halves(values):
        upper = values.astype(np.float32).astype(BF16)
        return [upper, (values.astype(np.float32) - upper.astype(np.float32)).astype(BF16)]

    waves = [np.cos(fine).astype(BF16), (-np.sin(fine)).astype(BF16)]
    by_pixel = np.concatenate([wave.T for wave in waves], axis=0)
    by_mode = np.concatenate(waves + halves(np.cos(coarse)) + halves(np.sin(coarse)), axis=1)
    return by_pixel, by_mode


def spread_table(sims):
    comps = 2 * sims
    row = np.arange(LANES)[:, None]
    col = np.arange(6 * LANES)[None, :]
    high_count = LANES // (TURNS * sims)
    row_t, row_g, row_s, row_c = row // (4 * comps), row // comps % 4, row // 2 % sims, row % 2
    col_q, col_c = col // (2 * LANES), col // LANES % 2
    col_t, col_s = col % LANES // (high_count * sims), col % sims
    group_q = np.array([0, 1, 2, 1])[row_g]
    source_c = np.where(col_q == 2, 1 - col_c, col_c)
    sign = np.where((col_q == 2) & (col_c == 0), -1.0, 1.0)
    hit = (row_t == col_t) & (row_s == col_s) & (group_q == col_q) & (row_c == source_c)
    return np.where(hit, sign, 0.0).astype(BF16)


def gather_table(sims):
    comps = 2 * sims
    row = np.arange(4 * LANES)[:, None]
    col = np.arange(LANES)[None, :]
    group, part = col // comps % 4, col % 2
    want_q = np.where((group == 1) | (group == 2), 1, 0)
    want_c = np.where(group >= 2, 1 - part, part)
    sign = np.where(((group == 2) & (part == 1)) | ((group == 3) & (part == 0)), -1.0, 1.0)
    hit = (row // (2 * LANES) == want_q) & (row // LANES % 2 == want_c)
    hit &= row % sims == col // 2 % sims
    return np.where(hit, sign, 0.0).astype(BF16)


def iota(shape, axis):
    return lax.broadcasted_iota(jnp.int32, shape, axis)


def div(values, size):
    return values >> (size.bit_length() - 1)


def mod(values, size):
    return values & (size - 1)


def one_hot(condition):
    return jnp.where(condition, 1.0, 0.0).astype(BF16)


def dot(left, right):
    return jnp.dot(left, right, preferred_element_type=F32)


def dot_t(left, right):
    return lax.dot_general(left, right, (((1,), (1,)), ((), ())), preferred_element_type=F32)


def fused_kernel(
    n, modes, rows, cycles, pixels, sims,
    slots_hbm, cycle_hbm, colat_hbm, weight_hbm, row_hbm, tbar_hbm, twf_hbm, leg_hbm, mask_hbm,
    pixel_hbm, mode_hbm, spread_hbm, gather_hbm,
    grad_ref, curl_ref,
    slots_s, cycle_s, colat_s, weight_s, slots_v, tbar_ref, twf_ref, leg_ref, mask_ref,
    pixel_v, mode_v, spread_v, gather_v,
    leg_all, prev_all, leg_p, prev_p, fs_ref, keep_ref, synth_ref, synth_l, anal_ref, anal_c, high_ref,
    pixmask_ref, maps_ref,
    send_m, recv_m, send_f, recv_f, send_p, recv_p, load_sem, move_sem,
):
    me = lax.axis_index("ma")
    work = n // TURNS
    pairs = tbar_ref.shape[0]
    comps = 2 * sims
    quad = LANES // (4 * comps)
    groups = pairs // quad
    span = 2 * cycles
    total = pairs * span
    count = n * 2 * pairs
    gh = 2 * groups
    high_count = LANES // (TURNS * sims)
    fine = pixels // high_count
    seat = lax.rem(lax.div(me, 2), work)
    prompt = n - n // 4
    first = 2 * gh
    is_worker = jnp.logical_and(lax.rem(me, 2) == 1, me < 2 * work)

    def slot_of(w, t):
        return 2 * w + t % 2 + t // 2 * 2 * work

    names = [
        (slots_hbm, slots_s), (colat_hbm, colat_s), (cycle_hbm, cycle_s),
        (leg_hbm, leg_ref), (tbar_hbm, tbar_ref), (twf_hbm, twf_ref),
        (mask_hbm, mask_ref), (weight_hbm, weight_s), (row_hbm, slots_v),
        (mode_hbm, mode_v), (pixel_hbm, pixel_v), (spread_hbm, spread_v), (gather_hbm, gather_v),
    ]
    loads = [
        pltpu.make_async_copy(source, target, load_sem.at[at])
        for at, (source, target) in enumerate(names)
    ]
    for load in loads[:6]:
        load.start()
    barrier = pltpu.get_barrier_semaphore()

    @pl.when(is_worker)
    def _():
        for off in range(1, n):
            pl.semaphore_signal(
                barrier, inc=1, device_id={"ma": lax.rem(me + off, n)},
                device_id_type=pl.DeviceIdType.MESH,
            )

    for load in loads[6:8]:
        load.start()

    @pl.when(is_worker)
    def _():
        for load in loads[8:]:
            load.start()

    def remote(source, target, at, to, mark=None):
        return pltpu.make_async_remote_copy(
            src_ref=source, dst_ref=target, send_sem=move_sem.at[2 * at],
            recv_sem=move_sem.at[2 * at + 1 if mark is None else mark], device_id={"ma": to},
            device_id_type=pl.DeviceIdType.MESH,
        )

    def settle(buffer, at):
        pltpu.make_async_copy(buffer, buffer, move_sem.at[at]).wait()

    @pl.when(jnp.logical_not(is_worker))
    def _():
        pl.semaphore_wait(barrier, work)
        loads[6].wait()
        send_m[...] = mask_ref[...].astype(F32).astype(BF16)
        turn = lax.rem(me, 2) + 2 * lax.div(me, 2 * work)
        remote(send_m, recv_m.at[turn], 2, 2 * lax.div(lax.rem(me, 2 * work), 2) + 1).start()

    for load in loads[:3]:
        load.wait()

    row_shape = (pairs, rows)
    smaller = jnp.zeros(row_shape, jnp.int32)
    for p in range(pairs):
        smaller = jnp.where(iota(row_shape, 0) == p, slots_s[me * pairs + p], smaller)
    k = iota(row_shape, 1)
    upper = k >= modes - smaller
    degree = jnp.where(upper, k - 1, smaller + k).astype(F32)
    orders = jnp.where(upper, modes - 1 - smaller, smaller).astype(F32)
    eps = raising(degree, orders)
    upper_f = jnp.where(upper, 1.0, 0.0)
    lower_f = 1.0 - upper_f

    colat = jnp.zeros((cycles, LANES), F32)
    for r in range(cycles):
        colat = jnp.where(iota(colat.shape, 0) == r, colat_s[r], colat)
    csc = 1.0 / jnp.sin(colat)
    cot = jnp.cos(colat) * csc
    lane_group = mod(div(iota(colat.shape, 1), comps), 4)
    base = jnp.where(lane_group == 0, 1.0, jnp.where(lane_group == 1, cot, csc))

    for load in loads[3:6]:
        load.wait()
    lane = iota((8, LANES), 1)
    lane_quad = div(lane, 4 * comps)
    is_phi = mod(div(lane, comps), 4) == 2
    for g in range(groups):
        sets, legs = [], []
        small = jnp.zeros((8, LANES), jnp.int32)
        for q in range(quad):
            p = g * quad + q
            small = jnp.where(lane_quad == q, slots_s[me * pairs + p], small)
            tbar = jnp.concatenate([tbar_ref[p, s].astype(F32) for s in range(sims)], axis=0)
            twf = jnp.concatenate([twf_ref[p, s].astype(F32) for s in range(sims)], axis=0)
            deg_p, eps_p = degree[p : p + 1] / modes, eps[p : p + 1] / modes
            scaled = -(eps_p * twf)
            raised = jnp.concatenate([scaled[:, 1:], jnp.zeros_like(scaled[:, :1])], axis=1)
            sets += [tbar, deg_p * twf, twf, raised]
            leg = leg_ref[p].astype(F32)
            low, high = lower_f[p : p + 1], upper_f[p : p + 1]
            legs += [leg * low, leg * high]
        legs = jnp.concatenate(legs, axis=0).astype(BF16)
        leg_all[pl.ds(g * quad * span, quad * span), :] = legs
        out = dot_t(legs, jnp.concatenate(sets, axis=0).astype(BF16))
        picked = out[:span]
        for q in range(1, quad):
            own = div(iota(picked.shape, 1), 4 * comps) == q
            picked = jnp.where(own, out[q * span : (q + 1) * span], picked)
        for h in range(2):
            order = (modes - 1 - small if h else small)[0:1]
            norm = jnp.where(order == 0, 1.0, 2.0) * modes ** (-0.5)
            norm = jnp.where(is_phi[0:1], norm * (order.astype(F32) / modes), norm)
            fs_ref[:, 2 * g + h, :] = picked[h * cycles : (h + 1) * cycles] * (base * norm)

    for t in range(TURNS):
        for w in range(work):
            send_f[t, w] = fs_ref[cycle_s[slot_of(w, t)], :gh, :].astype(BF16)

    @pl.when(is_worker)
    def _():
        pl.semaphore_wait(barrier, work - 1)

    tardy = 1 + 5 * lax.div(me, prompt)
    for w in range(work):
        @pl.when(me != 2 * w + 1)
        def _():
            remote(send_f.at[:, w], recv_f.at[:, me], 0, 2 * w + 1, tardy).start()

    loads[7].wait()
    lane_shape = (8, LANES)
    keep_lane = iota(lane_shape, 1)
    lane_seat = mod(div(keep_lane, gh), TURNS * work)
    theta_l = jnp.zeros(lane_shape, F32)
    weight_l = jnp.zeros(lane_shape, F32)
    place_shape = (LANES, total)
    place_row, place_lane = iota(place_shape, 0), iota(place_shape, 1)
    row_seat = mod(div(place_row, gh), TURNS * work)
    row_cycle = jnp.zeros(place_shape, jnp.int32)
    for t in range(TURNS):
        for w in range(work):
            r = cycle_s[slot_of(w, t)]
            at = t * work + w
            theta_l = jnp.where(lane_seat == at, colat_s[r], theta_l)
            weight_l = jnp.where(lane_seat == at, weight_s[r], weight_l)
            row_cycle = jnp.where(row_seat == at, r, row_cycle)
    with_sin = weight_l / jnp.sin(theta_l)
    with_cos = weight_l * jnp.cos(theta_l) / jnp.sin(theta_l)
    lane_g, lane_side = mod(div(keep_lane, 2), groups), div(keep_lane, LANES // 2)
    for p in range(pairs):
        mine = jnp.logical_and(lane_g == p // quad, lane_side == p % 2)
        keep_ref[p, 0] = jnp.where(mine, with_cos, 0.0)
        keep_ref[p, 1] = jnp.where(mine, with_sin, 0.0)
    for p in range(pairs):
        leg = leg_ref[p].astype(F32)
        prev = jnp.concatenate([jnp.zeros_like(leg[:, :1]), leg[:, : rows - 1]], axis=1)
        low, high = lower_f[p : p + 1], upper_f[p : p + 1]
        prev_all[pl.ds(p * span, span), :] = jnp.concatenate(
            [prev * low, prev * high], axis=0
        ).astype(BF16)
    row_pair = mod(div(place_row, 2), groups) * quad + div(place_row, LANES // 2)
    match = jnp.logical_and(
        row_cycle == mod(place_lane, cycles), mod(place_row, 2) == mod(div(place_lane, cycles), 2)
    )
    for k in range(quad // 2):
        place = one_hot(jnp.logical_and(match, row_pair + 2 * k == div(place_lane, span)))
        leg_p[k] = dot(place, leg_all[...]).astype(BF16)
        prev_p[k] = dot(place, prev_all[...]).astype(BF16)
    scale = (modes / cycles) ** 0.5 / jnp.sqrt(jnp.maximum(degree * (degree + 1.0), 1.0))
    f_level, f_eps, f_order = degree * scale, eps * scale, orders * scale

    @pl.when(is_worker)
    def _():
        for load in loads[8:]:
            load.wait()
        pair_count = slots_v.shape[1]

        ahead = prompt * gh

        def pair_of(at):
            behind = at >= quad * ahead
            rest = at - quad * ahead
            early = (at * (65536 // ahead + 1)) >> 16
            q = jnp.where(behind, div(rest, (n - prompt) * gh), early)
            inner = jnp.where(behind, ahead + mod(rest, (n - prompt) * gh), at - ahead * early)
            return div(inner, gh) * pairs + div(mod(inner, gh), 2) * quad + q

        slots = jnp.broadcast_to(slots_v[...], (pair_count, pair_count)).astype(F32).astype(BF16)
        spread = one_hot(iota((pair_count, count), 0) == pair_of(iota((pair_count, count), 1)))
        spread_t = one_hot(iota((count, pair_count), 1) == pair_of(iota((count, pair_count), 0)))
        by_lane = dot(slots[:16], spread)[0:8]
        by_lane = jnp.where(mod(iota(by_lane.shape, 1), 2) == 1, modes - 1.0 - by_lane, by_lane)
        by_row = dot_t(spread_t, slots)
        by_row = jnp.where(mod(iota(by_row.shape, 0), 2) == 1, modes - 1.0 - by_row, by_row)
        select = one_hot(iota((modes, count), 0).astype(F32) == by_lane[0:1])
        select_t = jnp.concatenate(
            [
                one_hot((iota(by_row.shape, 1) + at).astype(F32) == by_row)
                for at in range(0, modes, pair_count)
            ],
            axis=1,
        )
        moved = dot(pixel_v[...], select).astype(BF16)
        cut_at = quad * ahead
        synth_ref[...] = jnp.concatenate([moved[:fine, :cut_at], moved[fine:, :cut_at]], axis=1)
        synth_l[...] = jnp.concatenate([moved[:fine, cut_at:], moved[fine:, cut_at:]], axis=1)
        moved = dot(select_t, mode_v[...])
        anal_ref[:count] = moved[:, :fine].astype(BF16)
        anal_ref[count:] = moved[:, fine : 2 * fine].astype(BF16)
        anal_c[...] = jnp.concatenate(
            [
                moved[q * ahead : q * ahead + first, part * fine : (part + 1) * fine]
                for part in range(2)
                for q in range(quad)
            ],
            axis=0,
        ).astype(BF16)
        at = 2 * fine
        for part in range(2):
            high_ref[part] = moved[:, at : at + LANES] + moved[:, at + LANES : at + 2 * LANES]
            at += 2 * LANES

        loads[6].wait()
        recv_f[:, me] = send_f[:, seat]
        recv_m[1] = mask_ref[...].astype(F32).astype(BF16)
        settle(recv_m.at[pl.ds(0, TURNS - 1)], 5)
        both = recv_m[...].astype(F32).reshape(TURNS * mask_ref.shape[0], LANES)
        cut = fine // LANES
        grid = (both.shape[0], LANES)
        m_turn = div(iota(grid, 1), high_count * sims)
        m_high = mod(div(iota(grid, 1), sims), high_count)
        first_row = (m_turn * high_count + m_high) * cut
        both_t = both.T.astype(BF16)
        for at in range(cut):
            pixmask_ref[pl.ds(at * LANES, LANES), :] = dot(
                both_t, one_hot(iota(grid, 0) == first_row + at)
            )

        def turn_up(sources, rows_at, size):
            lanes_of = (size // quad, LANES)
            turns = [
                recv_f[t, pl.ds(sources, size // quad // gh)].astype(F32).reshape(lanes_of)
                for t in range(TURNS)
            ]
            block_lane = div(iota(lanes_of, 1), 4 * comps)
            got = []
            for q in range(quad):
                row = None
                for t in range(TURNS):
                    moved_t = turns[t]
                    if t != q:
                        moved_t = pltpu.roll(moved_t, (t - q) * 4 * comps % LANES, 1)
                    row = moved_t if row is None else jnp.where(block_lane == t, moved_t, row)
                got.append(row.astype(BF16))
            spread_f = dot(jnp.concatenate(got, axis=0), spread_v[...])
            cos_h, sin_h = high_ref[0, pl.ds(rows_at, size)], high_ref[1, pl.ds(rows_at, size)]
            real, imag = [], []
            for q in range(3):
                re = spread_f[:, 2 * q * LANES : (2 * q + 1) * LANES]
                im = spread_f[:, (2 * q + 1) * LANES : (2 * q + 2) * LANES]
                real.append((re * cos_h - im * sin_h).astype(BF16))
                imag.append((re * sin_h + im * cos_h).astype(BF16))
            return jnp.concatenate(
                [jnp.concatenate(real, axis=1), jnp.concatenate(imag, axis=1)], axis=0
            )

        settle(recv_f.at[:, pl.ds(0, prompt - 1)], 1)
        maps_ref[...] = dot(synth_ref[...], turn_up(0, 0, cut_at))
        settle(recv_f.at[:, pl.ds(0, n - prompt)], 6)
        maps = maps_ref[...] + dot(synth_l[...], turn_up(prompt, cut_at, count - cut_at))
        lead = pixmask_ref[...] * maps[:, :LANES]
        products = jnp.concatenate(
            [lead * maps[:, LANES : 2 * LANES], lead * maps[:, 2 * LANES :]], axis=1
        ).astype(BF16)
        def bring_down(table, cos_h, sin_h):
            size = cos_h.shape[0]
            half = dot(table, products)
            parts = []
            for q in range(2):
                c_part = half[:size, q * LANES : (q + 1) * LANES]
                s_part = half[size:, q * LANES : (q + 1) * LANES]
                parts.append((cos_h * c_part + sin_h * s_part).astype(BF16))
                parts.append((cos_h * s_part - sin_h * c_part).astype(BF16))
            parts = jnp.concatenate(parts, axis=1)
            turn = mod(div(iota((8, 4 * LANES), 1), LANES // TURNS), TURNS)[0:1]
            parts = jnp.concatenate([parts * one_hot(turn == t) for t in range(TURNS)], axis=0)
            return dot(parts, gather_v[...]) * pixels ** (-0.5)

        def pack(blocks):
            lane_quad = div(iota(blocks[0].shape, 1), 4 * comps)
            whole = blocks[0]
            for q in range(1, quad):
                whole = jnp.where(lane_quad == q, blocks[q], whole)
            return whole.astype(BF16).reshape(whole.shape[0] // gh, gh, LANES)

        high_c = [
            jnp.concatenate([high_ref[part, pl.ds(q * ahead, first)] for q in range(quad)], axis=0)
            for part in range(2)
        ]
        spectra = bring_down(anal_c[...], *high_c)
        for t in range(TURNS):
            at = t * quad * first
            send_p[t, pl.ds(0, 2)] = pack(
                [spectra[at + q * first : at + (q + 1) * first] for q in range(quad)]
            )
        remote(send_p.at[:, 0], recv_p.at[:, seat], 1, 0).start()

        @pl.when(me != 1)
        def _():
            remote(send_p.at[:, 1], recv_p.at[:, seat], 1, 1).start()

        spectra = bring_down(anal_ref[...], high_ref[0], high_ref[1])
        behind = n - prompt
        for t in range(TURNS):
            at = t * count
            late = at + cut_at
            rest = [
                jnp.concatenate(
                    [
                        spectra[at + q * ahead + first : at + (q + 1) * ahead],
                        spectra[late + q * behind * gh : late + (q + 1) * behind * gh],
                    ],
                    axis=0,
                )
                for q in range(quad)
            ]
            send_p[t, pl.ds(2, n - 2)] = pack(rest)
        for d in range(2, n):
            if d % 2 == 0 or d >= 2 * work:
                remote(send_p.at[:, d], recv_p.at[:, seat], 1, d).start()
            else:
                @pl.when(me != d)
                def _():
                    remote(send_p.at[:, d], recv_p.at[:, seat], 1, d).start()
        recv_p[:, seat] = send_p[:, me]
        settle(recv_p.at[:, pl.ds(0, work - 1)], 3)

    @pl.when(jnp.logical_not(is_worker))
    def _():
        settle(recv_p, 3)

    came = recv_p[...].astype(F32).reshape(TURNS * work * gh, LANES)
    came = jnp.concatenate([came, came], axis=0).T
    here, before = {}, {}
    for k in range(quad // 2):
        members = [p for p in range(pairs) if p % quad // 2 == k]
        first_k, second_k = [], []
        for p in members:
            at = p % quad * 4 * comps
            four = [came[at + g * comps : at + (g + 1) * comps] for g in range(4)]
            with_cos, with_sin = keep_ref[p, 0], keep_ref[p, 1]
            first_k += [four[0] * with_cos, four[1] * with_cos]
            first_k += [four[2] * with_sin, four[3] * with_sin]
            second_k += [four[0] * with_sin, four[1] * with_sin]
        out_a = dot(jnp.concatenate(first_k, axis=0).astype(BF16), leg_p[k])
        out_b = dot(jnp.concatenate(second_k, axis=0).astype(BF16), prev_p[k])
        for at, p in enumerate(members):
            here[p] = out_a[at * 4 * comps : (at + 1) * 4 * comps]
            before[p] = out_b[at * 2 * comps : (at + 1) * 2 * comps]
    for p in range(pairs):
        lev, ep, az = f_level[p : p + 1], f_eps[p : p + 1], f_order[p : p + 1]
        grad = (
            lev * here[p][:comps] - ep * before[p][:comps]
            + az * here[p][2 * comps : 3 * comps]
        )
        curl = (
            lev * here[p][comps : 2 * comps] - ep * before[p][comps:]
            + az * here[p][3 * comps :]
        )
        for s in range(sims):
            grad_ref[p, s] = grad[2 * s : 2 * s + 2]
            curl_ref[p, s] = curl[2 * s : 2 * s + 2]

    @pl.when(is_worker)
    def _():
        settle(send_f.at[:, pl.ds(0, work - 1)], 0)
        settle(send_p.at[:, pl.ds(0, n - 1)], 2)

    @pl.when(jnp.logical_not(is_worker))
    def _():
        settle(send_f, 0)
        settle(send_m, 4)


def store_kernel(grad_ref, curl_ref, grad_hbm, curl_hbm, sem):
    copies = [
        pltpu.make_async_copy(grad_ref, grad_hbm, sem.at[0]),
        pltpu.make_async_copy(curl_ref, curl_hbm, sem.at[1]),
    ]
    for copy in copies:
        copy.start()
    for copy in copies:
        copy.wait()


def fused(tbar_alm, twf_alm, legendre, m_slots, cycle_order, colatitude, cycle_weight, pixel_mask, n):
    pairs, sims, _, rows = tbar_alm.shape
    modes = rows - 1
    cycles = legendre.shape[2]
    pixels = pixel_mask.shape[1]
    total = pairs * 2 * cycles
    count = n * 2 * pairs
    work = n // TURNS
    gh = 2 * pairs * 8 * sims // LANES
    fine = pixels * TURNS * sims // LANES
    by_cycle = jnp.transpose(legendre, (0, 2, 1))
    by_pixel, by_mode = split_tables(modes, pixels, sims)
    tables = [jnp.asarray(x) for x in (by_pixel, by_mode, spread_table(sims), gather_table(sims))]
    vmem, anywhere = pl.BlockSpec(memory_space=pltpu.VMEM), pl.BlockSpec(memory_space=pl.ANY)
    out = pltpu.VMEM(tbar_alm.shape, F32)
    mask_shape = (pixels // LANES, LANES)
    made = pl.pallas_call(
        functools.partial(fused_kernel, n, modes, rows, cycles, pixels, sims),
        out_shape=(out, out),
        in_specs=[anywhere] * 13,
        out_specs=(vmem, vmem),
        scratch_shapes=[
            pltpu.SMEM(m_slots.shape, jnp.int32),
            pltpu.SMEM(cycle_order.shape, jnp.int32),
            pltpu.SMEM(colatitude.shape, F32),
            pltpu.SMEM(cycle_weight.shape, F32),
            pltpu.VMEM((1, m_slots.shape[0]), jnp.int32),
            pltpu.VMEM(tbar_alm.shape, BF16),
            pltpu.VMEM(twf_alm.shape, BF16),
            pltpu.VMEM(by_cycle.shape, BF16),
            pltpu.VMEM(mask_shape, jnp.int32),
        ]
        + [pltpu.VMEM(table.shape, BF16) for table in tables]
        + [
            pltpu.VMEM((total, rows), BF16),
            pltpu.VMEM((total, rows), BF16),
            pltpu.VMEM((total // LANES, LANES, rows), BF16),
            pltpu.VMEM((total // LANES, LANES, rows), BF16),
            pltpu.VMEM((cycles, 8, LANES), F32),
            pltpu.VMEM((pairs, 2, 8, LANES), F32),
            pltpu.VMEM((fine, 2 * count - count // 2), BF16),
            pltpu.VMEM((fine, count // 2), BF16),
            pltpu.VMEM((2 * count, fine), BF16),
            pltpu.VMEM((count // 4, fine), BF16),
            pltpu.VMEM((2, count, LANES), F32),
            pltpu.VMEM((fine, LANES), F32),
            pltpu.VMEM((fine, 3 * LANES), F32),
            pltpu.VMEM(mask_shape, BF16),
            pltpu.VMEM((TURNS,) + mask_shape, BF16),
            pltpu.VMEM((TURNS, work, gh, LANES), BF16),
            pltpu.VMEM((TURNS, n, gh, LANES), BF16),
            pltpu.VMEM((TURNS, n, gh, LANES), BF16),
            pltpu.VMEM((TURNS, work, gh, LANES), BF16),
            pltpu.SemaphoreType.DMA((13,)),
            pltpu.SemaphoreType.DMA((7,)),
        ],
        compiler_params=pltpu.CompilerParams(collective_id=0, has_side_effects=True),
        name="estimator",
    )(
        m_slots, cycle_order, colatitude, cycle_weight, m_slots.reshape(1, -1), tbar_alm,
        twf_alm, by_cycle, pixel_mask.reshape(mask_shape), *tables,
    )
    return pl.pallas_call(
        store_kernel,
        out_shape=(jax.ShapeDtypeStruct(tbar_alm.shape, F32),) * 2,
        in_specs=[vmem] * 2,
        out_specs=[anywhere] * 2,
        scratch_shapes=[pltpu.SemaphoreType.DMA((2,))],
        name="store",
    )(*(pltpu.with_memory_space_constraint(x, pltpu.VMEM) for x in made))


def body(n, *args):
    tbar_alm, legendre, pixel_mask = args[0], args[2], args[7]
    pairs, sims, _, rows = tbar_alm.shape
    cycles = legendre.shape[2]
    pixels = pixel_mask.shape[1]
    fits = (
        pairs == 8
        and cycles == n == 16
        and pixel_mask.shape[0] == 1
        and rows == 257
        and pairs * n == LANES
        and sims == 4
        and pixels == 4096
    )
    return fused(*args, n) if fits else shards(*args)


def solution(mesh):
    return jax.shard_map(
        functools.partial(body, mesh.shape["ma"]),
        mesh=mesh,
        in_specs=(
            P("ma", "grp", None, None),
            P("ma", "grp", None, None),
            P("ma", None, None),
            P(),
            P(),
            P(),
            P(),
            P("ma", None),
        ),
        out_specs=(P("ma", "grp", None, None), P("ma", "grp", None, None)),
        check_vma=False,
    )
```

```python
import math

import functools

import jax
import jax.numpy as jnp
import numpy as np
from jax import lax
from jax.experimental import pallas as pl
from jax.experimental.pallas import tpu as pltpu
from jax.sharding import PartitionSpec as P


def pair_layout(small_orders, mode_count):
    row_index = lax.broadcasted_iota(jnp.int32, (small_orders.shape[0], mode_count + 1), 1)
    smaller = small_orders[:, None]
    upper_half = row_index >= mode_count - smaller
    degree = jnp.where(upper_half, row_index - 1, smaller + row_index)
    orders = jnp.where(upper_half, mode_count - 1 - smaller, smaller + 0 * row_index)
    return (upper_half, degree.astype(jnp.float32), orders.astype(jnp.float32))


def raising(degree, orders):
    square = (
        (degree * degree - orders * orders)
        * (2.0 * degree + 1.0)
        / jnp.maximum(2.0 * degree - 1.0, 1.0)
    )
    return jnp.where(degree > orders, jnp.sqrt(jnp.where(degree > orders, square, 0.0)), 0.0)


def synthesis_sets(tbar_alm, twf_alm, degree, raising_factor, mode_count):
    wiener = twf_alm.astype(jnp.float32)
    scaled = (raising_factor / mode_count)[:, None, None, :] * wiener
    raised = jnp.concatenate([scaled[..., 1:], jnp.zeros_like(scaled[..., :1])], axis=-1)
    stacked = jnp.stack(
        [
            tbar_alm.astype(jnp.float32),
            wiener,
            (degree / mode_count)[:, None, None, :] * wiener,
            raised,
        ],
        axis=2,
    )
    return stacked.reshape(stacked.shape[0], stacked.shape[1], 8, stacked.shape[4]).astype(
        jnp.bfloat16
    )


def mode_columns(small_orders, mode_count):
    return jnp.stack([small_orders, mode_count - 1 - small_orders], axis=1).reshape(-1)


def fourier_table(orders_int, pixel_count):
    pixel_index = lax.broadcasted_iota(jnp.int32, (orders_int.shape[0], pixel_count), 1)
    turns = orders_int[:, None] * pixel_index % pixel_count
    radians = turns.astype(jnp.float32) * (2.0 * math.pi / pixel_count)
    return jnp.stack([jnp.cos(radians), -jnp.sin(radians)], axis=0).astype(jnp.bfloat16)


def combine_modes(legendre_sums, orders_int, cos_cycle, sin_cycle, mode_count):
    orders_real = orders_int.astype(jnp.float32)
    inv_sin = 1.0 / sin_cycle
    ratio = (orders_real / mode_count)[:, None]
    theta_real = (cos_cycle * legendre_sums[:, 4] - legendre_sums[:, 6]) * inv_sin
    theta_imag = (cos_cycle * legendre_sums[:, 5] - legendre_sums[:, 7]) * inv_sin
    phi_real = -ratio * legendre_sums[:, 3] * inv_sin
    phi_imag = ratio * legendre_sums[:, 2] * inv_sin
    weight = (jnp.where(orders_int == 0, 1.0, 2.0) * mode_count ** (-0.5))[:, None]
    stacked = jnp.stack(
        [legendre_sums[:, 0], legendre_sums[:, 1], theta_real, theta_imag, phi_real, phi_imag],
        axis=1,
    )
    return (stacked * weight).astype(jnp.bfloat16)


def analysis_sets(spectra, colatitude, cycle_weight):
    with_cos = cycle_weight * jnp.cos(colatitude) / jnp.sin(colatitude)
    with_sin = cycle_weight / jnp.sin(colatitude)
    stacked = jnp.stack(
        [
            spectra[:, 0] * with_cos,
            spectra[:, 0] * with_sin,
            spectra[:, 1] * with_cos,
            spectra[:, 1] * with_sin,
        ],
        axis=1,
    )
    return stacked.reshape(spectra.shape[0], 8, spectra.shape[3], spectra.shape[4]).astype(
        jnp.bfloat16
    )


def estimate(merged, degree, orders, raising_factor, mode_count, cycle_count):
    level = degree[:, None, :]
    azimuth = orders[:, None, :]
    factor = raising_factor[:, None, :]

    def previous(values):
        return jnp.concatenate([jnp.zeros_like(values[..., :1]), values[..., :-1]], axis=-1)

    grad_real = (
        level * merged[:, :, 0] - factor * previous(merged[:, :, 2]) + azimuth * merged[:, :, 7]
    )
    grad_imag = (
        level * merged[:, :, 1] - factor * previous(merged[:, :, 3]) - azimuth * merged[:, :, 6]
    )
    curl_real = (
        level * merged[:, :, 4] - factor * previous(merged[:, :, 6]) - azimuth * merged[:, :, 3]
    )
    curl_imag = (
        level * merged[:, :, 5] - factor * previous(merged[:, :, 7]) + azimuth * merged[:, :, 2]
    )
    scale = (mode_count / cycle_count) ** 0.5 / jnp.sqrt(jnp.maximum(level * (level + 1.0), 1.0))
    scale = scale[:, :, None, :]
    return (
        jnp.stack([grad_real, grad_imag], axis=2) * scale,
        jnp.stack([curl_real, curl_imag], axis=2) * scale,
    )


def shards(tbar_alm, twf_alm, legendre, m_slots, cycle_order, colatitude, cycle_weight, pixel_mask):
    pairs_dev = tbar_alm.shape[0]
    row_count = tbar_alm.shape[3]
    mode_count = row_count - 1
    cycle_count = legendre.shape[2]
    cycle_dev = pixel_mask.shape[0]
    pixel_count = pixel_mask.shape[1]
    device_slot = lax.axis_index("ma")
    local_small = lax.dynamic_slice_in_dim(m_slots, device_slot * pairs_dev, pairs_dev)
    upper_half, degree, orders = pair_layout(local_small, mode_count)
    raising_factor = raising(degree, orders)
    coeff_sets = synthesis_sets(tbar_alm, twf_alm, degree, raising_factor, mode_count)
    halves = jnp.stack([jnp.logical_not(upper_half), upper_half], axis=1)
    masked = coeff_sets[:, None] * halves.astype(jnp.bfloat16)[:, :, None, None, :]
    legendre_sums = jnp.einsum(
        "phsck,pkr->scphr", masked, legendre, preferred_element_type=jnp.float32
    )
    legendre_sums = jnp.take(legendre_sums, cycle_order, axis=4)
    legendre_sums = legendre_sums.reshape(legendre_sums.shape[0], 8, 2 * pairs_dev, cycle_count)
    all_orders = mode_columns(m_slots, mode_count)
    dft_table = fourier_table(all_orders, pixel_count)
    pixel_weights = pixel_mask.astype(jnp.float32)
    slot_theta = jnp.take(colatitude, cycle_order)
    local_orders = mode_columns(local_small, mode_count)
    outgoing = combine_modes(
        legendre_sums, local_orders, jnp.cos(slot_theta), jnp.sin(slot_theta), mode_count
    )
    fourier = lax.all_to_all(outgoing, "ma", split_axis=3, concat_axis=2, tiled=True)
    fourier = fourier.reshape(fourier.shape[0], 3, 2, mode_count, cycle_dev)
    cycle_maps = jnp.einsum(
        "sqemr,emj->sqrj", fourier, dft_table, preferred_element_type=jnp.float32
    )
    products = (pixel_weights * cycle_maps[:, 0:1] * cycle_maps[:, 1:3]).astype(jnp.bfloat16)
    spectra = jnp.einsum("sqrj,emj->sqemr", products, dft_table, preferred_element_type=jnp.float32)
    received = (spectra * pixel_count ** (-0.5)).astype(jnp.bfloat16)
    returned = lax.all_to_all(received, "ma", split_axis=3, concat_axis=4, tiled=True)
    inverse = (
        jnp.zeros((cycle_count,), jnp.int32).at[cycle_order].set(lax.iota(jnp.int32, cycle_count))
    )
    spectra = jnp.take(returned, inverse, axis=4).astype(jnp.float32)
    weighted = analysis_sets(spectra, colatitude, cycle_weight)
    weighted = weighted.reshape(weighted.shape[0], 8, pairs_dev, 2, cycle_count)
    projected = jnp.einsum(
        "scphr,pkr->phsck", weighted, legendre, preferred_element_type=jnp.float32
    )
    merged = jnp.sum(projected * halves.astype(jnp.float32)[:, :, None, None, :], axis=1)
    return estimate(merged, degree, orders, raising_factor, mode_count, cycle_count)


LANES = 128
TURNS = 4
F32 = jnp.float32
BF16 = jnp.bfloat16


def split_tables(mode_count, pixel_count, sims):
    high_count = LANES // (TURNS * sims)
    low_count = pixel_count // high_count
    m = np.arange(mode_count)[:, None]
    low = np.arange(low_count)[None, :]
    high = (np.arange(LANES) // sims % high_count)[None, :] * low_count
    fine = (m * low % pixel_count) * (2.0 * math.pi / pixel_count)
    coarse = (m * high % pixel_count) * (2.0 * math.pi / pixel_count)

    def halves(values):
        upper = values.astype(np.float32).astype(BF16)
        return [upper, (values.astype(np.float32) - upper.astype(np.float32)).astype(BF16)]

    waves = [np.cos(fine).astype(BF16), (-np.sin(fine)).astype(BF16)]
    by_pixel = np.concatenate([wave.T for wave in waves], axis=0)
    by_mode = np.concatenate(waves + halves(np.cos(coarse)) + halves(np.sin(coarse)), axis=1)
    return by_pixel, by_mode


def spread_table(sims):
    comps = 2 * sims
    row = np.arange(LANES)[:, None]
    col = np.arange(6 * LANES)[None, :]
    high_count = LANES // (TURNS * sims)
    row_t, row_g, row_s, row_c = row // (4 * comps), row // comps % 4, row // 2 % sims, row % 2
    col_q, col_c = col // (2 * LANES), col // LANES % 2
    col_t, col_s = col % LANES // (high_count * sims), col % sims
    group_q = np.array([0, 1, 2, 1])[row_g]
    source_c = np.where(col_q == 2, 1 - col_c, col_c)
    sign = np.where((col_q == 2) & (col_c == 0), -1.0, 1.0)
    hit = (row_t == col_t) & (row_s == col_s) & (group_q == col_q) & (row_c == source_c)
    return np.where(hit, sign, 0.0).astype(BF16)


def gather_table(sims):
    comps = 2 * sims
    row = np.arange(4 * LANES)[:, None]
    col = np.arange(LANES)[None, :]
    group, part = col // comps % 4, col % 2
    want_q = np.where((group == 1) | (group == 2), 1, 0)
    want_c = np.where(group >= 2, 1 - part, part)
    sign = np.where(((group == 2) & (part == 1)) | ((group == 3) & (part == 0)), -1.0, 1.0)
    hit = (row // (2 * LANES) == want_q) & (row // LANES % 2 == want_c)
    hit &= row % sims == col // 2 % sims
    return np.where(hit, sign, 0.0).astype(BF16)


def iota(shape, axis):
    return lax.broadcasted_iota(jnp.int32, shape, axis)


def div(values, size):
    return values >> (size.bit_length() - 1)


def mod(values, size):
    return values & (size - 1)


def one_hot(condition):
    return jnp.where(condition, 1.0, 0.0).astype(BF16)


def dot(left, right):
    return jnp.dot(left, right, preferred_element_type=F32)


def dot_t(left, right):
    return lax.dot_general(left, right, (((1,), (1,)), ((), ())), preferred_element_type=F32)


def fused_kernel(
    n, modes, rows, cycles, pixels, sims,
    slots_hbm, cycle_hbm, colat_hbm, weight_hbm, row_hbm, tbar_hbm, twf_hbm, leg_hbm, mask_hbm,
    pixel_hbm, mode_hbm, spread_hbm, gather_hbm,
    grad_ref, curl_ref,
    slots_s, cycle_s, colat_s, weight_s, slots_v, tbar_ref, twf_ref, leg_ref, mask_ref,
    pixel_v, mode_v, spread_v, gather_v,
    leg_all, prev_all, leg_p, prev_p, fs_ref, keep_ref, synth_ref, synth_l, anal_ref, anal_c, high_ref,
    pixmask_ref, maps_ref,
    send_m, recv_m, send_f, recv_f, send_p, recv_p, load_sem, move_sem,
):
    me = lax.axis_index("ma")
    work = n // TURNS
    pairs = tbar_ref.shape[0]
    comps = 2 * sims
    quad = LANES // (4 * comps)
    groups = pairs // quad
    span = 2 * cycles
    total = pairs * span
    count = n * 2 * pairs
    gh = 2 * groups
    high_count = LANES // (TURNS * sims)
    fine = pixels // high_count
    seat = lax.rem(lax.div(me, 2), work)
    prompt = n - n // 4
    first = 2 * gh
    is_worker = jnp.logical_and(lax.rem(me, 2) == 1, me < 2 * work)

    def slot_of(w, t):
        return 2 * w + t % 2 + t // 2 * 2 * work

    names = [
        (slots_hbm, slots_s), (colat_hbm, colat_s), (cycle_hbm, cycle_s),
        (leg_hbm, leg_ref), (tbar_hbm, tbar_ref), (twf_hbm, twf_ref),
        (mask_hbm, mask_ref), (weight_hbm, weight_s), (row_hbm, slots_v),
        (mode_hbm, mode_v), (pixel_hbm, pixel_v), (spread_hbm, spread_v), (gather_hbm, gather_v),
    ]
    loads = [
        pltpu.make_async_copy(source, target, load_sem.at[at])
        for at, (source, target) in enumerate(names)
    ]
    for load in loads[:6]:
        load.start()
    barrier = pltpu.get_barrier_semaphore()

    @pl.when(is_worker)
    def _():
        for off in range(1, n):
            pl.semaphore_signal(
                barrier, inc=1, device_id={"ma": lax.rem(me + off, n)},
                device_id_type=pl.DeviceIdType.MESH,
            )

    for load in loads[6:8]:
        load.start()

    @pl.when(is_worker)
    def _():
        for load in loads[8:]:
            load.start()

    def remote(source, target, at, to, mark=None):
        return pltpu.make_async_remote_copy(
            src_ref=source, dst_ref=target, send_sem=move_sem.at[2 * at],
            recv_sem=move_sem.at[2 * at + 1 if mark is None else mark], device_id={"ma": to},
            device_id_type=pl.DeviceIdType.MESH,
        )

    def settle(buffer, at):
        pltpu.make_async_copy(buffer, buffer, move_sem.at[at]).wait()

    @pl.when(jnp.logical_not(is_worker))
    def _():
        pl.semaphore_wait(barrier, work)
        loads[6].wait()
        send_m[...] = mask_ref[...].astype(F32).astype(BF16)
        turn = lax.rem(me, 2) + 2 * lax.div(me, 2 * work)
        remote(send_m, recv_m.at[turn], 2, 2 * lax.div(lax.rem(me, 2 * work), 2) + 1).start()

    for load in loads[:3]:
        load.wait()

    row_shape = (pairs, rows)
    smaller = jnp.zeros(row_shape, jnp.int32)
    for p in range(pairs):
        smaller = jnp.where(iota(row_shape, 0) == p, slots_s[me * pairs + p], smaller)
    k = iota(row_shape, 1)
    upper = k >= modes - smaller
    degree = jnp.where(upper, k - 1, smaller + k).astype(F32)
    orders = jnp.where(upper, modes - 1 - smaller, smaller).astype(F32)
    eps = raising(degree, orders)
    upper_f = jnp.where(upper, 1.0, 0.0)
    lower_f = 1.0 - upper_f

    colat = jnp.zeros((cycles, LANES), F32)
    for r in range(cycles):
        colat = jnp.where(iota(colat.shape, 0) == r, colat_s[r], colat)
    csc = 1.0 / jnp.sin(colat)
    cot = jnp.cos(colat) * csc
    lane_group = mod(div(iota(colat.shape, 1), comps), 4)
    base = jnp.where(lane_group == 0, 1.0, jnp.where(lane_group == 1, cot, csc))

    for load in loads[3:6]:
        load.wait()
    lane = iota((8, LANES), 1)
    lane_quad = div(lane, 4 * comps)
    is_phi = mod(div(lane, comps), 4) == 2
    for g in range(groups):
        sets, legs = [], []
        small = jnp.zeros((8, LANES), jnp.int32)
        for q in range(quad):
            p = g * quad + q
            small = jnp.where(lane_quad == q, slots_s[me * pairs + p], small)
            tbar = jnp.concatenate([tbar_ref[p, s].astype(F32) for s in range(sims)], axis=0)
            twf = jnp.concatenate([twf_ref[p, s].astype(F32) for s in range(sims)], axis=0)
            deg_p, eps_p = degree[p : p + 1] / modes, eps[p : p + 1] / modes
            scaled = -(eps_p * twf)
            raised = jnp.concatenate([scaled[:, 1:], jnp.zeros_like(scaled[:, :1])], axis=1)
            sets += [tbar, deg_p * twf, twf, raised]
            leg = leg_ref[p].astype(F32)
            low, high = lower_f[p : p + 1], upper_f[p : p + 1]
            legs += [leg * low, leg * high]
        legs = jnp.concatenate(legs, axis=0).astype(BF16)
        leg_all[pl.ds(g * quad * span, quad * span), :] = legs
        out = dot_t(legs, jnp.concatenate(sets, axis=0).astype(BF16))
        picked = out[:span]
        for q in range(1, quad):
            own = div(iota(picked.shape, 1), 4 * comps) == q
            picked = jnp.where(own, out[q * span : (q + 1) * span], picked)
        for h in range(2):
            order = (modes - 1 - small if h else small)[0:1]
            norm = jnp.where(order == 0, 1.0, 2.0) * modes ** (-0.5)
            norm = jnp.where(is_phi[0:1], norm * (order.astype(F32) / modes), norm)
            fs_ref[:, 2 * g + h, :] = picked[h * cycles : (h + 1) * cycles] * (base * norm)

    for t in range(TURNS):
        for w in range(work):
            send_f[t, w] = fs_ref[cycle_s[slot_of(w, t)], :gh, :].astype(BF16)

    @pl.when(is_worker)
    def _():
        pl.semaphore_wait(barrier, work - 1)

    tardy = 1 + 5 * lax.div(me, prompt)
    for w in range(work):
        @pl.when(me != 2 * w + 1)
        def _():
            remote(send_f.at[:, w], recv_f.at[:, me], 0, 2 * w + 1, tardy).start()

    loads[7].wait()
    lane_shape = (8, LANES)
    keep_lane = iota(lane_shape, 1)
    lane_seat = mod(div(keep_lane, gh), TURNS * work)
    theta_l = jnp.zeros(lane_shape, F32)
    weight_l = jnp.zeros(lane_shape, F32)
    place_shape = (LANES, total)
    place_row, place_lane = iota(place_shape, 0), iota(place_shape, 1)
    row_seat = mod(div(place_row, gh), TURNS * work)
    row_cycle = jnp.zeros(place_shape, jnp.int32)
    for t in range(TURNS):
        for w in range(work):
            r = cycle_s[slot_of(w, t)]
            at = t * work + w
            theta_l = jnp.where(lane_seat == at, colat_s[r], theta_l)
            weight_l = jnp.where(lane_seat == at, weight_s[r], weight_l)
            row_cycle = jnp.where(row_seat == at, r, row_cycle)
    with_sin = weight_l / jnp.sin(theta_l)
    with_cos = weight_l * jnp.cos(theta_l) / jnp.sin(theta_l)
    lane_g, lane_side = mod(div(keep_lane, 2), groups), div(keep_lane, LANES // 2)
    for p in range(pairs):
        mine = jnp.logical_and(lane_g == p // quad, lane_side == p % 2)
        keep_ref[p, 0] = jnp.where(mine, with_cos, 0.0)
        keep_ref[p, 1] = jnp.where(mine, with_sin, 0.0)
    for p in range(pairs):
        leg = leg_ref[p].astype(F32)
        prev = jnp.concatenate([jnp.zeros_like(leg[:, :1]), leg[:, : rows - 1]], axis=1)
        low, high = lower_f[p : p + 1], upper_f[p : p + 1]
        prev_all[pl.ds(p * span, span), :] = jnp.concatenate(
            [prev * low, prev * high], axis=0
        ).astype(BF16)
    row_pair = mod(div(place_row, 2), groups) * quad + div(place_row, LANES // 2)
    match = jnp.logical_and(
        row_cycle == mod(place_lane, cycles), mod(place_row, 2) == mod(div(place_lane, cycles), 2)
    )
    for k in range(quad // 2):
        place = one_hot(jnp.logical_and(match, row_pair + 2 * k == div(place_lane, span)))
        leg_p[k] = dot(place, leg_all[...]).astype(BF16)
        prev_p[k] = dot(place, prev_all[...]).astype(BF16)
    scale = (modes / cycles) ** 0.5 / jnp.sqrt(jnp.maximum(degree * (degree + 1.0), 1.0))
    f_level, f_eps, f_order = degree * scale, eps * scale, orders * scale

    @pl.when(is_worker)
    def _():
        for load in loads[8:]:
            load.wait()
        pair_count = slots_v.shape[1]

        ahead = prompt * gh

        def pair_of(at):
            behind = at >= quad * ahead
            rest = at - quad * ahead
            early = (at * (65536 // ahead + 1)) >> 16
            q = jnp.where(behind, div(rest, (n - prompt) * gh), early)
            inner = jnp.where(behind, ahead + mod(rest, (n - prompt) * gh), at - ahead * early)
            return div(inner, gh) * pairs + div(mod(inner, gh), 2) * quad + q

        slots = jnp.broadcast_to(slots_v[...], (pair_count, pair_count)).astype(F32).astype(BF16)
        spread = one_hot(iota((pair_count, count), 0) == pair_of(iota((pair_count, count), 1)))
        spread_t = one_hot(iota((count, pair_count), 1) == pair_of(iota((count, pair_count), 0)))
        by_lane = dot(slots[:16], spread)[0:8]
        by_lane = jnp.where(mod(iota(by_lane.shape, 1), 2) == 1, modes - 1.0 - by_lane, by_lane)
        by_row = dot_t(spread_t, slots)
        by_row = jnp.where(mod(iota(by_row.shape, 0), 2) == 1, modes - 1.0 - by_row, by_row)
        select = one_hot(iota((modes, count), 0).astype(F32) == by_lane[0:1])
        select_t = jnp.concatenate(
            [
                one_hot((iota(by_row.shape, 1) + at).astype(F32) == by_row)
                for at in range(0, modes, pair_count)
            ],
            axis=1,
        )
        moved = dot(pixel_v[...], select).astype(BF16)
        cut_at = quad * ahead
        synth_ref[...] = jnp.concatenate([moved[:fine, :cut_at], moved[fine:, :cut_at]], axis=1)
        synth_l[...] = jnp.concatenate([moved[:fine, cut_at:], moved[fine:, cut_at:]], axis=1)
        moved = dot(select_t, mode_v[...])
        anal_ref[:count] = moved[:, :fine].astype(BF16)
        anal_ref[count:] = moved[:, fine : 2 * fine].astype(BF16)
        anal_c[...] = jnp.concatenate(
            [
                moved[q * ahead : q * ahead + first, part * fine : (part + 1) * fine]
                for part in range(2)
                for q in range(quad)
            ],
            axis=0,
        ).astype(BF16)
        at = 2 * fine
        for part in range(2):
            high_ref[part] = moved[:, at : at + LANES] + moved[:, at + LANES : at + 2 * LANES]
            at += 2 * LANES

        loads[6].wait()
        recv_f[:, me] = send_f[:, seat]
        recv_m[1] = mask_ref[...].astype(F32).astype(BF16)
        def turn_up(sources, rows_at, size):
            lanes_of = (size // quad, LANES)
            turns = [
                recv_f[t, pl.ds(sources, size // quad // gh)].astype(F32).reshape(lanes_of)
                for t in range(TURNS)
            ]
            block_lane = div(iota(lanes_of, 1), 4 * comps)
            got = []
            for q in range(quad):
                row = None
                for t in range(TURNS):
                    moved_t = turns[t]
                    if t != q:
                        moved_t = pltpu.roll(moved_t, (t - q) * 4 * comps % LANES, 1)
                    row = moved_t if row is None else jnp.where(block_lane == t, moved_t, row)
                got.append(row.astype(BF16))
            spread_f = dot(jnp.concatenate(got, axis=0), spread_v[...])
            cos_h, sin_h = high_ref[0, pl.ds(rows_at, size)], high_ref[1, pl.ds(rows_at, size)]
            real, imag = [], []
            for q in range(3):
                re = spread_f[:, 2 * q * LANES : (2 * q + 1) * LANES]
                im = spread_f[:, (2 * q + 1) * LANES : (2 * q + 2) * LANES]
                real.append((re * cos_h - im * sin_h).astype(BF16))
                imag.append((re * sin_h + im * cos_h).astype(BF16))
            return jnp.concatenate(
                [jnp.concatenate(real, axis=1), jnp.concatenate(imag, axis=1)], axis=0
            )

        settle(recv_f.at[:, pl.ds(0, prompt - 1)], 1)
        maps_ref[...] = dot(synth_ref[...], turn_up(0, 0, cut_at))
        settle(recv_m.at[pl.ds(0, TURNS - 1)], 5)
        settle(recv_f.at[:, pl.ds(0, n - prompt)], 6)
        both = recv_m[...].astype(F32).reshape(TURNS * mask_ref.shape[0], LANES)
        cut = fine // LANES
        grid = (both.shape[0], LANES)
        m_turn = div(iota(grid, 1), high_count * sims)
        m_high = mod(div(iota(grid, 1), sims), high_count)
        first_row = (m_turn * high_count + m_high) * cut
        both_t = both.T.astype(BF16)
        for at in range(cut):
            pixmask_ref[pl.ds(at * LANES, LANES), :] = dot(
                both_t, one_hot(iota(grid, 0) == first_row + at)
            )
        maps = maps_ref[...] + dot(synth_l[...], turn_up(prompt, cut_at, count - cut_at))
        lead = pixmask_ref[...] * maps[:, :LANES]
        products = jnp.concatenate(
            [lead * maps[:, LANES : 2 * LANES], lead * maps[:, 2 * LANES :]], axis=1
        ).astype(BF16)
        def bring_down(table, cos_h, sin_h):
            size = cos_h.shape[0]
            half = dot(table, products)
            parts = []
            for q in range(2):
                c_part = half[:size, q * LANES : (q + 1) * LANES]
                s_part = half[size:, q * LANES : (q + 1) * LANES]
                parts.append((cos_h * c_part + sin_h * s_part).astype(BF16))
                parts.append((cos_h * s_part - sin_h * c_part).astype(BF16))
            parts = jnp.concatenate(parts, axis=1)
            turn = mod(div(iota((8, 4 * LANES), 1), LANES // TURNS), TURNS)[0:1]
            parts = jnp.concatenate([parts * one_hot(turn == t) for t in range(TURNS)], axis=0)
            return dot(parts, gather_v[...]) * pixels ** (-0.5)

        def pack(blocks):
            lane_quad = div(iota(blocks[0].shape, 1), 4 * comps)
            whole = blocks[0]
            for q in range(1, quad):
                whole = jnp.where(lane_quad == q, blocks[q], whole)
            return whole.astype(BF16).reshape(whole.shape[0] // gh, gh, LANES)

        high_c = [
            jnp.concatenate([high_ref[part, pl.ds(q * ahead, first)] for q in range(quad)], axis=0)
            for part in range(2)
        ]
        spectra = bring_down(anal_c[...], *high_c)
        for t in range(TURNS):
            at = t * quad * first
            send_p[t, pl.ds(0, 2)] = pack(
                [spectra[at + q * first : at + (q + 1) * first] for q in range(quad)]
            )
        remote(send_p.at[:, 0], recv_p.at[:, seat], 1, 0).start()

        @pl.when(me != 1)
        def _():
            remote(send_p.at[:, 1], recv_p.at[:, seat], 1, 1).start()

        spectra = bring_down(anal_ref[...], high_ref[0], high_ref[1])
        behind = n - prompt
        for t in range(TURNS):
            at = t * count
            late = at + cut_at
            rest = [
                jnp.concatenate(
                    [
                        spectra[at + q * ahead + first : at + (q + 1) * ahead],
                        spectra[late + q * behind * gh : late + (q + 1) * behind * gh],
                    ],
                    axis=0,
                )
                for q in range(quad)
            ]
            send_p[t, pl.ds(2, n - 2)] = pack(rest)
        for d in range(2, n):
            if d % 2 == 0 or d >= 2 * work:
                remote(send_p.at[:, d], recv_p.at[:, seat], 1, d).start()
            else:
                @pl.when(me != d)
                def _():
                    remote(send_p.at[:, d], recv_p.at[:, seat], 1, d).start()
        recv_p[:, seat] = send_p[:, me]
        settle(recv_p.at[:, pl.ds(0, work - 1)], 3)

    @pl.when(jnp.logical_not(is_worker))
    def _():
        settle(recv_p, 3)

    came = recv_p[...].astype(F32).reshape(TURNS * work * gh, LANES)
    came = jnp.concatenate([came, came], axis=0).T
    here, before = {}, {}
    for k in range(quad // 2):
        members = [p for p in range(pairs) if p % quad // 2 == k]
        first_k, second_k = [], []
        for p in members:
            at = p % quad * 4 * comps
            four = [came[at + g * comps : at + (g + 1) * comps] for g in range(4)]
            with_cos, with_sin = keep_ref[p, 0], keep_ref[p, 1]
            first_k += [four[0] * with_cos, four[1] * with_cos]
            first_k += [four[2] * with_sin, four[3] * with_sin]
            second_k += [four[0] * with_sin, four[1] * with_sin]
        out_a = dot(jnp.concatenate(first_k, axis=0).astype(BF16), leg_p[k])
        out_b = dot(jnp.concatenate(second_k, axis=0).astype(BF16), prev_p[k])
        for at, p in enumerate(members):
            here[p] = out_a[at * 4 * comps : (at + 1) * 4 * comps]
            before[p] = out_b[at * 2 * comps : (at + 1) * 2 * comps]
    for p in range(pairs):
        lev, ep, az = f_level[p : p + 1], f_eps[p : p + 1], f_order[p : p + 1]
        grad = (
            lev * here[p][:comps] - ep * before[p][:comps]
            + az * here[p][2 * comps : 3 * comps]
        )
        curl = (
            lev * here[p][comps : 2 * comps] - ep * before[p][comps:]
            + az * here[p][3 * comps :]
        )
        for s in range(sims):
            grad_ref[p, s] = grad[2 * s : 2 * s + 2]
            curl_ref[p, s] = curl[2 * s : 2 * s + 2]

    @pl.when(is_worker)
    def _():
        settle(send_f.at[:, pl.ds(0, work - 1)], 0)
        settle(send_p.at[:, pl.ds(0, n - 1)], 2)

    @pl.when(jnp.logical_not(is_worker))
    def _():
        settle(send_f, 0)
        settle(send_m, 4)


def store_kernel(grad_ref, curl_ref, grad_hbm, curl_hbm, sem):
    copies = [
        pltpu.make_async_copy(grad_ref, grad_hbm, sem.at[0]),
        pltpu.make_async_copy(curl_ref, curl_hbm, sem.at[1]),
    ]
    for copy in copies:
        copy.start()
    for copy in copies:
        copy.wait()


def fused(tbar_alm, twf_alm, legendre, m_slots, cycle_order, colatitude, cycle_weight, pixel_mask, n):
    pairs, sims, _, rows = tbar_alm.shape
    modes = rows - 1
    cycles = legendre.shape[2]
    pixels = pixel_mask.shape[1]
    total = pairs * 2 * cycles
    count = n * 2 * pairs
    work = n // TURNS
    gh = 2 * pairs * 8 * sims // LANES
    fine = pixels * TURNS * sims // LANES
    by_cycle = jnp.transpose(legendre, (0, 2, 1))
    by_pixel, by_mode = split_tables(modes, pixels, sims)
    tables = [jnp.asarray(x) for x in (by_pixel, by_mode, spread_table(sims), gather_table(sims))]
    vmem, anywhere = pl.BlockSpec(memory_space=pltpu.VMEM), pl.BlockSpec(memory_space=pl.ANY)
    out = pltpu.VMEM(tbar_alm.shape, F32)
    mask_shape = (pixels // LANES, LANES)
    made = pl.pallas_call(
        functools.partial(fused_kernel, n, modes, rows, cycles, pixels, sims),
        out_shape=(out, out),
        in_specs=[anywhere] * 13,
        out_specs=(vmem, vmem),
        scratch_shapes=[
            pltpu.SMEM(m_slots.shape, jnp.int32),
            pltpu.SMEM(cycle_order.shape, jnp.int32),
            pltpu.SMEM(colatitude.shape, F32),
            pltpu.SMEM(cycle_weight.shape, F32),
            pltpu.VMEM((1, m_slots.shape[0]), jnp.int32),
            pltpu.VMEM(tbar_alm.shape, BF16),
            pltpu.VMEM(twf_alm.shape, BF16),
            pltpu.VMEM(by_cycle.shape, BF16),
            pltpu.VMEM(mask_shape, jnp.int32),
        ]
        + [pltpu.VMEM(table.shape, BF16) for table in tables]
        + [
            pltpu.VMEM((total, rows), BF16),
            pltpu.VMEM((total, rows), BF16),
            pltpu.VMEM((total // LANES, LANES, rows), BF16),
            pltpu.VMEM((total // LANES, LANES, rows), BF16),
            pltpu.VMEM((cycles, 8, LANES), F32),
            pltpu.VMEM((pairs, 2, 8, LANES), F32),
            pltpu.VMEM((fine, 2 * count - count // 2), BF16),
            pltpu.VMEM((fine, count // 2), BF16),
            pltpu.VMEM((2 * count, fine), BF16),
            pltpu.VMEM((count // 4, fine), BF16),
            pltpu.VMEM((2, count, LANES), F32),
            pltpu.VMEM((fine, LANES), F32),
            pltpu.VMEM((fine, 3 * LANES), F32),
            pltpu.VMEM(mask_shape, BF16),
            pltpu.VMEM((TURNS,) + mask_shape, BF16),
            pltpu.VMEM((TURNS, work, gh, LANES), BF16),
            pltpu.VMEM((TURNS, n, gh, LANES), BF16),
            pltpu.VMEM((TURNS, n, gh, LANES), BF16),
            pltpu.VMEM((TURNS, work, gh, LANES), BF16),
            pltpu.SemaphoreType.DMA((13,)),
            pltpu.SemaphoreType.DMA((7,)),
        ],
        compiler_params=pltpu.CompilerParams(collective_id=0, has_side_effects=True),
        name="estimator",
    )(
        m_slots, cycle_order, colatitude, cycle_weight, m_slots.reshape(1, -1), tbar_alm,
        twf_alm, by_cycle, pixel_mask.reshape(mask_shape), *tables,
    )
    return pl.pallas_call(
        store_kernel,
        out_shape=(jax.ShapeDtypeStruct(tbar_alm.shape, F32),) * 2,
        in_specs=[vmem] * 2,
        out_specs=[anywhere] * 2,
        scratch_shapes=[pltpu.SemaphoreType.DMA((2,))],
        name="store",
    )(*(pltpu.with_memory_space_constraint(x, pltpu.VMEM) for x in made))


def body(n, *args):
    tbar_alm, legendre, pixel_mask = args[0], args[2], args[7]
    pairs, sims, _, rows = tbar_alm.shape
    cycles = legendre.shape[2]
    pixels = pixel_mask.shape[1]
    fits = (
        pairs == 8
        and cycles == n == 16
        and pixel_mask.shape[0] == 1
        and rows == 257
        and pairs * n == LANES
        and sims == 4
        and pixels == 4096
    )
    return fused(*args, n) if fits else shards(*args)


def solution(mesh):
    return jax.shard_map(
        functools.partial(body, mesh.shape["ma"]),
        mesh=mesh,
        in_specs=(
            P("ma", "grp", None, None),
            P("ma", "grp", None, None),
            P("ma", None, None),
            P(),
            P(),
            P(),
            P(),
            P("ma", None),
        ),
        out_specs=(P("ma", "grp", None, None), P("ma", "grp", None, None)),
        check_vma=False,
    )
```

```python
import math

import functools

import jax
import jax.numpy as jnp
import numpy as np
from jax import lax
from jax.experimental import pallas as pl
from jax.experimental.pallas import tpu as pltpu
from jax.sharding import PartitionSpec as P


def pair_layout(small_orders, mode_count):
    row_index = lax.broadcasted_iota(jnp.int32, (small_orders.shape[0], mode_count + 1), 1)
    smaller = small_orders[:, None]
    upper_half = row_index >= mode_count - smaller
    degree = jnp.where(upper_half, row_index - 1, smaller + row_index)
    orders = jnp.where(upper_half, mode_count - 1 - smaller, smaller + 0 * row_index)
    return (upper_half, degree.astype(jnp.float32), orders.astype(jnp.float32))


def raising(degree, orders):
    square = (
        (degree * degree - orders * orders)
        * (2.0 * degree + 1.0)
        / jnp.maximum(2.0 * degree - 1.0, 1.0)
    )
    return jnp.where(degree > orders, jnp.sqrt(jnp.where(degree > orders, square, 0.0)), 0.0)


def synthesis_sets(tbar_alm, twf_alm, degree, raising_factor, mode_count):
    wiener = twf_alm.astype(jnp.float32)
    scaled = (raising_factor / mode_count)[:, None, None, :] * wiener
    raised = jnp.concatenate([scaled[..., 1:], jnp.zeros_like(scaled[..., :1])], axis=-1)
    stacked = jnp.stack(
        [
            tbar_alm.astype(jnp.float32),
            wiener,
            (degree / mode_count)[:, None, None, :] * wiener,
            raised,
        ],
        axis=2,
    )
    return stacked.reshape(stacked.shape[0], stacked.shape[1], 8, stacked.shape[4]).astype(
        jnp.bfloat16
    )


def mode_columns(small_orders, mode_count):
    return jnp.stack([small_orders, mode_count - 1 - small_orders], axis=1).reshape(-1)


def fourier_table(orders_int, pixel_count):
    pixel_index = lax.broadcasted_iota(jnp.int32, (orders_int.shape[0], pixel_count), 1)
    turns = orders_int[:, None] * pixel_index % pixel_count
    radians = turns.astype(jnp.float32) * (2.0 * math.pi / pixel_count)
    return jnp.stack([jnp.cos(radians), -jnp.sin(radians)], axis=0).astype(jnp.bfloat16)


def combine_modes(legendre_sums, orders_int, cos_cycle, sin_cycle, mode_count):
    orders_real = orders_int.astype(jnp.float32)
    inv_sin = 1.0 / sin_cycle
    ratio = (orders_real / mode_count)[:, None]
    theta_real = (cos_cycle * legendre_sums[:, 4] - legendre_sums[:, 6]) * inv_sin
    theta_imag = (cos_cycle * legendre_sums[:, 5] - legendre_sums[:, 7]) * inv_sin
    phi_real = -ratio * legendre_sums[:, 3] * inv_sin
    phi_imag = ratio * legendre_sums[:, 2] * inv_sin
    weight = (jnp.where(orders_int == 0, 1.0, 2.0) * mode_count ** (-0.5))[:, None]
    stacked = jnp.stack(
        [legendre_sums[:, 0], legendre_sums[:, 1], theta_real, theta_imag, phi_real, phi_imag],
        axis=1,
    )
    return (stacked * weight).astype(jnp.bfloat16)


def analysis_sets(spectra, colatitude, cycle_weight):
    with_cos = cycle_weight * jnp.cos(colatitude) / jnp.sin(colatitude)
    with_sin = cycle_weight / jnp.sin(colatitude)
    stacked = jnp.stack(
        [
            spectra[:, 0] * with_cos,
            spectra[:, 0] * with_sin,
            spectra[:, 1] * with_cos,
            spectra[:, 1] * with_sin,
        ],
        axis=1,
    )
    return stacked.reshape(spectra.shape[0], 8, spectra.shape[3], spectra.shape[4]).astype(
        jnp.bfloat16
    )


def estimate(merged, degree, orders, raising_factor, mode_count, cycle_count):
    level = degree[:, None, :]
    azimuth = orders[:, None, :]
    factor = raising_factor[:, None, :]

    def previous(values):
        return jnp.concatenate([jnp.zeros_like(values[..., :1]), values[..., :-1]], axis=-1)

    grad_real = (
        level * merged[:, :, 0] - factor * previous(merged[:, :, 2]) + azimuth * merged[:, :, 7]
    )
    grad_imag = (
        level * merged[:, :, 1] - factor * previous(merged[:, :, 3]) - azimuth * merged[:, :, 6]
    )
    curl_real = (
        level * merged[:, :, 4] - factor * previous(merged[:, :, 6]) - azimuth * merged[:, :, 3]
    )
    curl_imag = (
        level * merged[:, :, 5] - factor * previous(merged[:, :, 7]) + azimuth * merged[:, :, 2]
    )
    scale = (mode_count / cycle_count) ** 0.5 / jnp.sqrt(jnp.maximum(level * (level + 1.0), 1.0))
    scale = scale[:, :, None, :]
    return (
        jnp.stack([grad_real, grad_imag], axis=2) * scale,
        jnp.stack([curl_real, curl_imag], axis=2) * scale,
    )


def shards(tbar_alm, twf_alm, legendre, m_slots, cycle_order, colatitude, cycle_weight, pixel_mask):
    pairs_dev = tbar_alm.shape[0]
    row_count = tbar_alm.shape[3]
    mode_count = row_count - 1
    cycle_count = legendre.shape[2]
    cycle_dev = pixel_mask.shape[0]
    pixel_count = pixel_mask.shape[1]
    device_slot = lax.axis_index("ma")
    local_small = lax.dynamic_slice_in_dim(m_slots, device_slot * pairs_dev, pairs_dev)
    upper_half, degree, orders = pair_layout(local_small, mode_count)
    raising_factor = raising(degree, orders)
    coeff_sets = synthesis_sets(tbar_alm, twf_alm, degree, raising_factor, mode_count)
    halves = jnp.stack([jnp.logical_not(upper_half), upper_half], axis=1)
    masked = coeff_sets[:, None] * halves.astype(jnp.bfloat16)[:, :, None, None, :]
    legendre_sums = jnp.einsum(
        "phsck,pkr->scphr", masked, legendre, preferred_element_type=jnp.float32
    )
    legendre_sums = jnp.take(legendre_sums, cycle_order, axis=4)
    legendre_sums = legendre_sums.reshape(legendre_sums.shape[0], 8, 2 * pairs_dev, cycle_count)
    all_orders = mode_columns(m_slots, mode_count)
    dft_table = fourier_table(all_orders, pixel_count)
    pixel_weights = pixel_mask.astype(jnp.float32)
    slot_theta = jnp.take(colatitude, cycle_order)
    local_orders = mode_columns(local_small, mode_count)
    outgoing = combine_modes(
        legendre_sums, local_orders, jnp.cos(slot_theta), jnp.sin(slot_theta), mode_count
    )
    fourier = lax.all_to_all(outgoing, "ma", split_axis=3, concat_axis=2, tiled=True)
    fourier = fourier.reshape(fourier.shape[0], 3, 2, mode_count, cycle_dev)
    cycle_maps = jnp.einsum(
        "sqemr,emj->sqrj", fourier, dft_table, preferred_element_type=jnp.float32
    )
    products = (pixel_weights * cycle_maps[:, 0:1] * cycle_maps[:, 1:3]).astype(jnp.bfloat16)
    spectra = jnp.einsum("sqrj,emj->sqemr", products, dft_table, preferred_element_type=jnp.float32)
    received = (spectra * pixel_count ** (-0.5)).astype(jnp.bfloat16)
    returned = lax.all_to_all(received, "ma", split_axis=3, concat_axis=4, tiled=True)
    inverse = (
        jnp.zeros((cycle_count,), jnp.int32).at[cycle_order].set(lax.iota(jnp.int32, cycle_count))
    )
    spectra = jnp.take(returned, inverse, axis=4).astype(jnp.float32)
    weighted = analysis_sets(spectra, colatitude, cycle_weight)
    weighted = weighted.reshape(weighted.shape[0], 8, pairs_dev, 2, cycle_count)
    projected = jnp.einsum(
        "scphr,pkr->phsck", weighted, legendre, preferred_element_type=jnp.float32
    )
    merged = jnp.sum(projected * halves.astype(jnp.float32)[:, :, None, None, :], axis=1)
    return estimate(merged, degree, orders, raising_factor, mode_count, cycle_count)


LANES = 128
TURNS = 4
F32 = jnp.float32
BF16 = jnp.bfloat16


def split_tables(mode_count, pixel_count, sims):
    high_count = LANES // (TURNS * sims)
    low_count = pixel_count // high_count
    m = np.arange(mode_count)[:, None]
    low = np.arange(low_count)[None, :]
    high = (np.arange(LANES) // sims % high_count)[None, :] * low_count
    fine = (m * low % pixel_count) * (2.0 * math.pi / pixel_count)
    coarse = (m * high % pixel_count) * (2.0 * math.pi / pixel_count)

    def halves(values):
        upper = values.astype(np.float32).astype(BF16)
        return [upper, (values.astype(np.float32) - upper.astype(np.float32)).astype(BF16)]

    waves = [np.cos(fine).astype(BF16), (-np.sin(fine)).astype(BF16)]
    by_pixel = np.concatenate([wave.T for wave in waves], axis=0)
    by_mode = np.concatenate(waves + halves(np.cos(coarse)) + halves(np.sin(coarse)), axis=1)
    return by_pixel, by_mode


def spread_table(sims):
    comps = 2 * sims
    row = np.arange(2 * LANES)[:, None]
    col = np.arange(4 * LANES)[None, :]
    row_t, row_g, row_s, row_c = row // LANES, row // comps % 4, row // 2 % sims, row % 2
    col_t, col_s, col_c = col // (LANES // 2) % 2, col % sims, col // LANES % 2
    col_q = np.where(col < 2 * LANES, 0, 1 + col // (LANES // 4) % 2)
    group_q = np.array([0, 1, 2, 1])[row_g]
    source_c = np.where(col_q == 2, 1 - col_c, col_c)
    sign = np.where((col_q == 2) & (col_c == 0), -1.0, 1.0)
    hit = (row_t == col_t) & (row_s == col_s) & (group_q == col_q) & (row_c == source_c)
    return np.where(hit, sign, 0.0).astype(BF16)


def gather_table(sims):
    comps = 2 * sims
    row = np.arange(4 * LANES)[:, None]
    col = np.arange(LANES)[None, :]
    group, part = col // comps % 4, col % 2
    want_q = np.where((group == 1) | (group == 2), 1, 0)
    want_c = np.where(group >= 2, 1 - part, part)
    sign = np.where(((group == 2) & (part == 1)) | ((group == 3) & (part == 0)), -1.0, 1.0)
    hit = (row // (LANES // 4) % 2 == want_q) & (row // LANES % 2 == want_c)
    hit &= row % sims == col // 2 % sims
    turn = 2 * (row // (2 * LANES)) + row // (LANES // 2) % 2
    own = hit & (turn == col // (4 * comps))
    return np.concatenate([np.where(x, sign, 0.0) for x in (hit, own)], axis=1).astype(BF16)


def iota(shape, axis):
    return lax.broadcasted_iota(jnp.int32, shape, axis)


def div(values, size):
    return values >> (size.bit_length() - 1)


def mod(values, size):
    return values & (size - 1)


def one_hot(condition):
    return jnp.where(condition, 1.0, 0.0).astype(BF16)


def dot(left, right):
    return jnp.dot(left, right, preferred_element_type=F32)


def dot_t(left, right):
    return lax.dot_general(left, right, (((1,), (1,)), ((), ())), preferred_element_type=F32)


def fused_kernel(
    n, modes, rows, cycles, pixels, sims,
    slots_hbm, cycle_hbm, colat_hbm, weight_hbm, row_hbm, tbar_hbm, twf_hbm, leg_hbm, mask_hbm,
    pixel_hbm, mode_hbm, spread_hbm, gather_hbm,
    grad_ref, curl_ref,
    slots_s, cycle_s, colat_s, weight_s, slots_v, tbar_ref, twf_ref, leg_ref, mask_ref,
    pixel_v, mode_v, spread_v, gather_v,
    leg_all, prev_all, leg_p, prev_p, fs_ref, keep_ref, synth_ref, synth_l, anal_ref, anal_c, high_ref,
    pixmask_ref, maps_ref, pick_ref,
    send_m, recv_m, send_f, recv_f, send_p, recv_p, load_sem, move_sem,
):
    me = lax.axis_index("ma")
    work = n // TURNS
    pairs = tbar_ref.shape[0]
    comps = 2 * sims
    quad = LANES // (4 * comps)
    groups = pairs // quad
    span = 2 * cycles
    total = pairs * span
    count = n * 2 * pairs
    gh = 2 * groups
    high_count = LANES // (TURNS * sims)
    fine = pixels // high_count
    seat = lax.rem(lax.div(me, 2), work)
    prompt = n - n // 4
    first = 2 * gh
    is_worker = jnp.logical_and(lax.rem(me, 2) == 1, me < 2 * work)

    def slot_of(w, t):
        return 2 * w + t % 2 + t // 2 * 2 * work

    names = [
        (slots_hbm, slots_s), (colat_hbm, colat_s), (cycle_hbm, cycle_s),
        (leg_hbm, leg_ref), (tbar_hbm, tbar_ref), (twf_hbm, twf_ref),
        (mask_hbm, mask_ref), (weight_hbm, weight_s), (row_hbm, slots_v),
        (mode_hbm, mode_v), (pixel_hbm, pixel_v), (spread_hbm, spread_v), (gather_hbm, gather_v),
    ]
    loads = [
        pltpu.make_async_copy(source, target, load_sem.at[at])
        for at, (source, target) in enumerate(names)
    ]
    for load in loads[:6]:
        load.start()
    barrier = pltpu.get_barrier_semaphore()

    @pl.when(is_worker)
    def _():
        for off in range(1, n):
            pl.semaphore_signal(
                barrier, inc=1, device_id={"ma": lax.rem(me + off, n)},
                device_id_type=pl.DeviceIdType.MESH,
            )

    for load in loads[6:8]:
        load.start()

    @pl.when(is_worker)
    def _():
        for load in loads[8:]:
            load.start()

    def remote(source, target, at, to, mark=None):
        return pltpu.make_async_remote_copy(
            src_ref=source, dst_ref=target, send_sem=move_sem.at[2 * at],
            recv_sem=move_sem.at[2 * at + 1 if mark is None else mark], device_id={"ma": to},
            device_id_type=pl.DeviceIdType.MESH,
        )

    def settle(buffer, at):
        pltpu.make_async_copy(buffer, buffer, move_sem.at[at]).wait()

    @pl.when(jnp.logical_not(is_worker))
    def _():
        pl.semaphore_wait(barrier, work)
        loads[6].wait()
        send_m[...] = mask_ref[...].astype(F32).astype(BF16)
        turn = lax.rem(me, 2) + 2 * lax.div(me, 2 * work)
        remote(send_m, recv_m.at[turn], 2, 2 * lax.div(lax.rem(me, 2 * work), 2) + 1).start()

    for load in loads[:3]:
        load.wait()

    row_shape = (pairs, rows)
    smaller = jnp.zeros(row_shape, jnp.int32)
    for p in range(pairs):
        smaller = jnp.where(iota(row_shape, 0) == p, slots_s[me * pairs + p], smaller)
    k = iota(row_shape, 1)
    upper = k >= modes - smaller
    degree = jnp.where(upper, k - 1, smaller + k).astype(F32)
    orders = jnp.where(upper, modes - 1 - smaller, smaller).astype(F32)
    eps = raising(degree, orders)
    upper_f = jnp.where(upper, 1.0, 0.0)
    lower_f = 1.0 - upper_f

    colat = jnp.zeros((cycles, LANES), F32)
    for r in range(cycles):
        colat = jnp.where(iota(colat.shape, 0) == r, colat_s[r], colat)
    csc = 1.0 / jnp.sin(colat)
    cot = jnp.cos(colat) * csc
    lane_group = mod(div(iota(colat.shape, 1), comps), 4)
    base = jnp.where(lane_group == 0, 1.0, jnp.where(lane_group == 1, cot, csc))

    halves = [
        [jnp.broadcast_to(part[p : p + 1], (cycles, rows)).astype(BF16) for part in (lower_f, upper_f)]
        for p in range(pairs)
    ]

    for load in loads[3:6]:
        load.wait()
    lane = iota((8, LANES), 1)
    lane_quad = div(lane, 4 * comps)
    is_phi = mod(div(lane, comps), 4) == 2
    for g in range(groups):
        sets, legs = [], []
        small = jnp.zeros((8, LANES), jnp.int32)
        for q in range(quad):
            p = g * quad + q
            small = jnp.where(lane_quad == q, slots_s[me * pairs + p], small)
            tbar = jnp.concatenate([tbar_ref[p, s].astype(F32) for s in range(sims)], axis=0)
            twf = jnp.concatenate([twf_ref[p, s].astype(F32) for s in range(sims)], axis=0)
            deg_p, eps_p = degree[p : p + 1] / modes, eps[p : p + 1] / modes
            scaled = -(eps_p * twf)
            raised = jnp.concatenate([scaled[:, 1:], jnp.zeros_like(scaled[:, :1])], axis=1)
            sets += [tbar, deg_p * twf, twf, raised]
            legs += [leg_ref[p] * part for part in halves[p]]
        legs = jnp.concatenate(legs, axis=0)
        leg_all[pl.ds(g * quad * span, quad * span), :] = legs
        out = dot_t(legs, jnp.concatenate(sets, axis=0).astype(BF16))
        picked = out[:span]
        for q in range(1, quad):
            own = div(iota(picked.shape, 1), 4 * comps) == q
            picked = jnp.where(own, out[q * span : (q + 1) * span], picked)
        for h in range(2):
            order = (modes - 1 - small if h else small)[0:1]
            norm = jnp.where(order == 0, 1.0, 2.0) * modes ** (-0.5)
            norm = jnp.where(is_phi[0:1], norm * (order.astype(F32) / modes), norm)
            fs_ref[pl.ds((2 * g + h) * cycles, cycles), :] = picked[h * cycles : (h + 1) * cycles] * (base * norm)

    for t in range(TURNS):
        for w in range(work):
            send_f[t, w] = fs_ref[pl.ds(cycle_s[slot_of(w, t)], gh, stride=cycles), :].astype(BF16)

    @pl.when(is_worker)
    def _():
        pl.semaphore_wait(barrier, work - 1)

    tardy = 1 + 5 * lax.div(me, prompt)
    for w in reversed(range(work)):
        @pl.when(me != 2 * w + 1)
        def _():
            remote(send_f.at[:, w], recv_f.at[:, me], 0, 2 * w + 1, tardy).start()

    loads[7].wait()
    lane_shape = (8, LANES)
    keep_lane = iota(lane_shape, 1)
    lane_seat = mod(div(keep_lane, gh), TURNS * work)
    theta_l = jnp.zeros(lane_shape, F32)
    weight_l = jnp.zeros(lane_shape, F32)
    place_shape = (LANES, total)
    place_row, place_lane = iota(place_shape, 0), iota(place_shape, 1)
    row_seat = mod(div(place_row, gh), TURNS * work)
    row_cycle = jnp.zeros(place_shape, jnp.int32)
    for t in range(TURNS):
        for w in range(work):
            r = cycle_s[slot_of(w, t)]
            at = t * work + w
            theta_l = jnp.where(lane_seat == at, colat_s[r], theta_l)
            weight_l = jnp.where(lane_seat == at, weight_s[r], weight_l)
            row_cycle = jnp.where(row_seat == at, r, row_cycle)
    with_sin = weight_l / jnp.sin(theta_l)
    with_cos = weight_l * jnp.cos(theta_l) / jnp.sin(theta_l)
    lane_g, lane_side = mod(div(keep_lane, 2), groups), div(keep_lane, LANES // 2)
    for p in range(pairs):
        mine = jnp.logical_and(lane_g == p // quad, lane_side == p % 2)
        keep_ref[p, 0] = jnp.where(mine, with_cos, 0.0)
        keep_ref[p, 1] = jnp.where(mine, with_sin, 0.0)
    for p in range(pairs):
        leg = leg_ref[p].astype(F32)
        prev = jnp.concatenate([jnp.zeros_like(leg[:, :1]), leg[:, : rows - 1]], axis=1)
        low, high = lower_f[p : p + 1], upper_f[p : p + 1]
        prev_all[pl.ds(p * span, span), :] = jnp.concatenate(
            [prev * low, prev * high], axis=0
        ).astype(BF16)
    row_pair = mod(div(place_row, 2), groups) * quad + div(place_row, LANES // 2)
    match = jnp.logical_and(
        row_cycle == mod(place_lane, cycles), mod(place_row, 2) == mod(div(place_lane, cycles), 2)
    )
    for k in range(quad // 2):
        place = one_hot(jnp.logical_and(match, row_pair + 2 * k == div(place_lane, span)))
        leg_p[k] = dot(place, leg_all[...]).astype(BF16)
        prev_p[k] = dot(place, prev_all[...]).astype(BF16)
    scale = (modes / cycles) ** 0.5 / jnp.sqrt(jnp.maximum(degree * (degree + 1.0), 1.0))
    f_level, f_eps, f_order = degree * scale, eps * scale, orders * scale

    @pl.when(is_worker)
    def _():
        for load in loads[8:]:
            load.wait()
        pair_count = slots_v.shape[1]

        ahead = prompt * gh

        def pair_of(at):
            behind = at >= quad * ahead
            rest = at - quad * ahead
            early = (at * (65536 // ahead + 1)) >> 16
            q = jnp.where(behind, div(rest, (n - prompt) * gh), early)
            inner = jnp.where(behind, ahead + mod(rest, (n - prompt) * gh), at - ahead * early)
            return div(inner, gh) * pairs + div(mod(inner, gh), 2) * quad + q

        slots = jnp.broadcast_to(slots_v[...], (pair_count, pair_count)).astype(F32).astype(BF16)
        spread = one_hot(iota((pair_count, count), 0) == pair_of(iota((pair_count, count), 1)))
        spread_t = one_hot(iota((count, pair_count), 1) == pair_of(iota((count, pair_count), 0)))
        by_lane = dot(slots[:16], spread)[0:8]
        by_lane = jnp.where(mod(iota(by_lane.shape, 1), 2) == 1, modes - 1.0 - by_lane, by_lane)
        by_row = dot_t(spread_t, slots)
        by_row = jnp.where(mod(iota(by_row.shape, 0), 2) == 1, modes - 1.0 - by_row, by_row)
        select = one_hot(iota((modes, count), 0).astype(F32) == by_lane[0:1])
        select_t = jnp.concatenate(
            [
                one_hot((iota(by_row.shape, 1) + at).astype(F32) == by_row)
                for at in range(0, modes, pair_count)
            ],
            axis=1,
        )
        moved = dot(pixel_v[...], select).astype(BF16)
        cut_at = quad * ahead
        synth_ref[...] = jnp.concatenate([moved[:fine, :cut_at], moved[fine:, :cut_at]], axis=1)
        synth_l[...] = jnp.concatenate([moved[:fine, cut_at:], moved[fine:, cut_at:]], axis=1)
        moved = dot(select_t, mode_v[...])
        anal_ref[:count] = moved[:, :fine].astype(BF16)
        anal_ref[count:] = moved[:, fine : 2 * fine].astype(BF16)
        anal_c[...] = jnp.concatenate(
            [
                moved[q * ahead : q * ahead + first, part * fine : (part + 1) * fine]
                for part in range(2)
                for q in range(quad)
            ],
            axis=0,
        ).astype(BF16)
        at = 2 * fine
        for part in range(2):
            high_ref[part] = moved[:, at : at + LANES] + moved[:, at + LANES : at + 2 * LANES]
            at += 2 * LANES

        loads[6].wait()
        recv_f[:, me] = send_f[:, seat]
        cut = fine // LANES
        grid = (TURNS * mask_ref.shape[0], LANES)
        m_turn = div(iota(grid, 1), LANES // 2)
        m_high = mod(div(iota(grid, 1), sims), high_count)
        for j in range(TURNS // 2):
            first_row = ((m_turn + 2 * j) * high_count + m_high) * cut
            for at in range(cut):
                pick_ref[j, at] = one_hot(iota(grid, 0) == first_row + at)
        recv_m[1] = mask_ref[...].astype(F32).astype(BF16)
        quarter = mod(div(iota((8, 2 * LANES), 1), 4 * comps), quad)[0:1]

        def turn_up(sources, rows_at, size):
            turns = [
                recv_f[t, pl.ds(sources, size // quad // gh)].reshape(size // quad, LANES)
                for t in range(TURNS)
            ]
            pairs_of = [
                jnp.concatenate(turns[2 * j : 2 * j + 2], axis=1) for j in range(TURNS // 2)
            ]
            got = [pair * one_hot(quarter == q) for pair in pairs_of for q in range(quad)]
            spread_f = dot(jnp.concatenate(got, axis=0), spread_v[...])
            cos_h, sin_h = high_ref[0, pl.ds(rows_at, size)], high_ref[1, pl.ds(rows_at, size)]
            real, imag = [], []
            for j in range(TURNS // 2):
                for kind in range(2):
                    at = 2 * kind * LANES
                    re = spread_f[j * size : (j + 1) * size, at : at + LANES]
                    im = spread_f[j * size : (j + 1) * size, at + LANES : at + 2 * LANES]
                    real.append((re * cos_h - im * sin_h).astype(BF16))
                    imag.append((re * sin_h + im * cos_h).astype(BF16))
            return jnp.concatenate(
                [jnp.concatenate(real, axis=1), jnp.concatenate(imag, axis=1)], axis=0
            )

        settle(recv_f.at[:, pl.ds(0, prompt - 1)], 1)
        maps_ref[...] = dot(synth_ref[...], turn_up(0, 0, cut_at))
        settle(recv_m.at[pl.ds(0, TURNS - 1)], 5)
        both = recv_m[...].astype(F32).reshape(TURNS * mask_ref.shape[0], LANES)
        both_t = both.T.astype(BF16)
        for j in range(TURNS // 2):
            for at in range(cut):
                pixmask_ref[j, pl.ds(at * LANES, LANES), :] = dot(both_t, pick_ref[j, at])
        settle(recv_f.at[:, pl.ds(0, n - prompt)], 6)
        maps = maps_ref[...] + dot(synth_l[...], turn_up(prompt, cut_at, count - cut_at))
        products = jnp.concatenate(
            [
                pixmask_ref[j]
                * maps[:, 2 * j * LANES : (2 * j + 1) * LANES]
                * maps[:, (2 * j + 1) * LANES : (2 * j + 2) * LANES]
                for j in range(TURNS // 2)
            ],
            axis=1,
        ).astype(BF16)
        def bring_down(table, cos_h, sin_h, split):
            size = cos_h.shape[0]
            half = dot(table, products)
            parts = []
            for q in range(2):
                c_part = half[:size, q * LANES : (q + 1) * LANES]
                s_part = half[size:, q * LANES : (q + 1) * LANES]
                parts.append((cos_h * c_part + sin_h * s_part).astype(BF16))
                parts.append((cos_h * s_part - sin_h * c_part).astype(BF16))
            parts = jnp.concatenate(parts, axis=1)
            if not split:
                return dot(parts, gather_v[:, LANES:]) * pixels ** (-0.5)
            lane = iota((8, 4 * LANES), 1)
            turn = (2 * div(lane, 2 * LANES) + mod(div(lane, LANES // 2), 2))[0:1]
            parts = jnp.concatenate([parts * one_hot(turn == t) for t in range(TURNS)], axis=0)
            return dot(parts, gather_v[:, :LANES]) * pixels ** (-0.5)

        def pack(blocks):
            lane_quad = div(iota(blocks[0].shape, 1), 4 * comps)
            whole = blocks[0]
            for q in range(1, quad):
                whole = jnp.where(lane_quad == q, blocks[q], whole)
            return whole.astype(BF16).reshape(whole.shape[0] // gh, gh, LANES)

        high_c = [
            jnp.concatenate([high_ref[part, pl.ds(q * ahead, first)] for q in range(quad)], axis=0)
            for part in range(2)
        ]
        spectra = bring_down(anal_c[...], *high_c, True)
        for t in range(TURNS):
            at = t * quad * first
            send_p[t, pl.ds(0, 2)] = pack(
                [spectra[at + q * first : at + (q + 1) * first] for q in range(quad)]
            )
        remote(send_p.at[:, 0], recv_p.at[:, seat], 1, 0).start()

        @pl.when(me != 1)
        def _():
            remote(send_p.at[:, 1], recv_p.at[:, seat], 1, 1).start()

        spectra = bring_down(anal_ref[...], high_ref[0], high_ref[1], False)
        behind = n - prompt
        rest = [
            jnp.concatenate(
                [
                    spectra[q * ahead + first : (q + 1) * ahead],
                    spectra[cut_at + q * behind * gh : cut_at + (q + 1) * behind * gh],
                ],
                axis=0,
            )
            for q in range(quad)
        ]
        for t in range(TURNS):
            send_p[t, pl.ds(2, n - 2)] = pack(
                [
                    rest[q] if q == t else pltpu.roll(rest[q], (q - t) * 4 * comps % LANES, 1)
                    for q in range(quad)
                ]
            )
        for d in range(2, n):
            if d % 2 == 0 or d >= 2 * work:
                remote(send_p.at[:, d], recv_p.at[:, seat], 1, d).start()
            else:
                @pl.when(me != d)
                def _():
                    remote(send_p.at[:, d], recv_p.at[:, seat], 1, d).start()
        recv_p[:, seat] = send_p[:, me]
        settle(recv_p.at[:, pl.ds(0, work - 1)], 3)

    @pl.when(jnp.logical_not(is_worker))
    def _():
        settle(recv_p, 3)

    came = recv_p[...].astype(F32).reshape(TURNS * work * gh, LANES)
    came = jnp.concatenate([came, came], axis=0).T
    here, before = {}, {}
    for k in range(quad // 2):
        members = [p for p in range(pairs) if p % quad // 2 == k]
        first_k, second_k = [], []
        for p in members:
            at = p % quad * 4 * comps
            four = [came[at + g * comps : at + (g + 1) * comps] for g in range(4)]
            with_cos, with_sin = keep_ref[p, 0], keep_ref[p, 1]
            first_k += [four[0] * with_cos, four[1] * with_cos]
            first_k += [four[2] * with_sin, four[3] * with_sin]
            second_k += [four[0] * with_sin, four[1] * with_sin]
        out_a = dot(jnp.concatenate(first_k, axis=0).astype(BF16), leg_p[k])
        out_b = dot(jnp.concatenate(second_k, axis=0).astype(BF16), prev_p[k])
        for at, p in enumerate(members):
            here[p] = out_a[at * 4 * comps : (at + 1) * 4 * comps]
            before[p] = out_b[at * 2 * comps : (at + 1) * 2 * comps]
    for p in range(pairs):
        lev, ep, az = f_level[p : p + 1], f_eps[p : p + 1], f_order[p : p + 1]
        grad = (
            lev * here[p][:comps] - ep * before[p][:comps]
            + az * here[p][2 * comps : 3 * comps]
        )
        curl = (
            lev * here[p][comps : 2 * comps] - ep * before[p][comps:]
            + az * here[p][3 * comps :]
        )
        for s in range(sims):
            grad_ref[p, s] = grad[2 * s : 2 * s + 2]
            curl_ref[p, s] = curl[2 * s : 2 * s + 2]

    @pl.when(is_worker)
    def _():
        settle(send_f.at[:, pl.ds(0, work - 1)], 0)
        settle(send_p.at[:, pl.ds(0, n - 1)], 2)

    @pl.when(jnp.logical_not(is_worker))
    def _():
        settle(send_f, 0)
        settle(send_m, 4)


def store_kernel(grad_ref, curl_ref, grad_hbm, curl_hbm, sem):
    copies = [
        pltpu.make_async_copy(grad_ref, grad_hbm, sem.at[0]),
        pltpu.make_async_copy(curl_ref, curl_hbm, sem.at[1]),
    ]
    for copy in copies:
        copy.start()
    for copy in copies:
        copy.wait()


def fused(tbar_alm, twf_alm, legendre, m_slots, cycle_order, colatitude, cycle_weight, pixel_mask, n):
    pairs, sims, _, rows = tbar_alm.shape
    modes = rows - 1
    cycles = legendre.shape[2]
    pixels = pixel_mask.shape[1]
    total = pairs * 2 * cycles
    count = n * 2 * pairs
    work = n // TURNS
    gh = 2 * pairs * 8 * sims // LANES
    fine = pixels * TURNS * sims // LANES
    by_cycle = jnp.transpose(legendre, (0, 2, 1))
    by_pixel, by_mode = split_tables(modes, pixels, sims)
    tables = [jnp.asarray(x) for x in (by_pixel, by_mode, spread_table(sims), gather_table(sims))]
    vmem, anywhere = pl.BlockSpec(memory_space=pltpu.VMEM), pl.BlockSpec(memory_space=pl.ANY)
    out = pltpu.VMEM(tbar_alm.shape, F32)
    mask_shape = (pixels // LANES, LANES)
    made = pl.pallas_call(
        functools.partial(fused_kernel, n, modes, rows, cycles, pixels, sims),
        out_shape=(out, out),
        in_specs=[anywhere] * 13,
        out_specs=(vmem, vmem),
        scratch_shapes=[
            pltpu.SMEM(m_slots.shape, jnp.int32),
            pltpu.SMEM(cycle_order.shape, jnp.int32),
            pltpu.SMEM(colatitude.shape, F32),
            pltpu.SMEM(cycle_weight.shape, F32),
            pltpu.VMEM((1, m_slots.shape[0]), jnp.int32),
            pltpu.VMEM(tbar_alm.shape, BF16),
            pltpu.VMEM(twf_alm.shape, BF16),
            pltpu.VMEM(by_cycle.shape, BF16),
            pltpu.VMEM(mask_shape, jnp.int32),
        ]
        + [pltpu.VMEM(table.shape, BF16) for table in tables]
        + [
            pltpu.VMEM((total, rows), BF16),
            pltpu.VMEM((total, rows), BF16),
            pltpu.VMEM((total // LANES, LANES, rows), BF16),
            pltpu.VMEM((total // LANES, LANES, rows), BF16),
            pltpu.VMEM((gh * cycles, LANES), F32),
            pltpu.VMEM((pairs, 2, 8, LANES), F32),
            pltpu.VMEM((fine, 2 * count - count // 2), BF16),
            pltpu.VMEM((fine, count // 2), BF16),
            pltpu.VMEM((2 * count, fine), BF16),
            pltpu.VMEM((count // 4, fine), BF16),
            pltpu.VMEM((2, count, LANES), F32),
            pltpu.VMEM((TURNS // 2, fine, LANES), F32),
            pltpu.VMEM((fine, 4 * LANES), F32),
            pltpu.VMEM((TURNS // 2, fine // LANES, TURNS * mask_shape[0], LANES), BF16),
            pltpu.VMEM(mask_shape, BF16),
            pltpu.VMEM((TURNS,) + mask_shape, BF16),
            pltpu.VMEM((TURNS, work, gh, LANES), BF16),
            pltpu.VMEM((TURNS, n, gh, LANES), BF16),
            pltpu.VMEM((TURNS, n, gh, LANES), BF16),
            pltpu.VMEM((TURNS, work, gh, LANES), BF16),
            pltpu.SemaphoreType.DMA((13,)),
            pltpu.SemaphoreType.DMA((7,)),
        ],
        compiler_params=pltpu.CompilerParams(collective_id=0, has_side_effects=True),
        name="estimator",
    )(
        m_slots, cycle_order, colatitude, cycle_weight, m_slots.reshape(1, -1), tbar_alm,
        twf_alm, by_cycle, pixel_mask.reshape(mask_shape), *tables,
    )
    return pl.pallas_call(
        store_kernel,
        out_shape=(jax.ShapeDtypeStruct(tbar_alm.shape, F32),) * 2,
        in_specs=[vmem] * 2,
        out_specs=[anywhere] * 2,
        scratch_shapes=[pltpu.SemaphoreType.DMA((2,))],
        name="store",
    )(*(pltpu.with_memory_space_constraint(x, pltpu.VMEM) for x in made))


def body(n, *args):
    tbar_alm, legendre, pixel_mask = args[0], args[2], args[7]
    pairs, sims, _, rows = tbar_alm.shape
    cycles = legendre.shape[2]
    pixels = pixel_mask.shape[1]
    fits = (
        pairs == 8
        and cycles == n == 16
        and pixel_mask.shape[0] == 1
        and rows == 257
        and pairs * n == LANES
        and sims == 4
        and pixels == 4096
    )
    return fused(*args, n) if fits else shards(*args)


def solution(mesh):
    return jax.shard_map(
        functools.partial(body, mesh.shape["ma"]),
        mesh=mesh,
        in_specs=(
            P("ma", "grp", None, None),
            P("ma", "grp", None, None),
            P("ma", None, None),
            P(),
            P(),
            P(),
            P(),
            P("ma", None),
        ),
        out_specs=(P("ma", "grp", None, None), P("ma", "grp", None, None)),
        check_vma=False,
    )
```

```python
import math

import functools

import jax
import jax.numpy as jnp
import numpy as np
from jax import lax
from jax.experimental import pallas as pl
from jax.experimental.pallas import tpu as pltpu
from jax.sharding import PartitionSpec as P


def pair_layout(small_orders, mode_count):
    row_index = lax.broadcasted_iota(jnp.int32, (small_orders.shape[0], mode_count + 1), 1)
    smaller = small_orders[:, None]
    upper_half = row_index >= mode_count - smaller
    degree = jnp.where(upper_half, row_index - 1, smaller + row_index)
    orders = jnp.where(upper_half, mode_count - 1 - smaller, smaller + 0 * row_index)
    return (upper_half, degree.astype(jnp.float32), orders.astype(jnp.float32))


def raising(degree, orders):
    square = (
        (degree * degree - orders * orders)
        * (2.0 * degree + 1.0)
        / jnp.maximum(2.0 * degree - 1.0, 1.0)
    )
    return jnp.where(degree > orders, jnp.sqrt(jnp.where(degree > orders, square, 0.0)), 0.0)


def synthesis_sets(tbar_alm, twf_alm, degree, raising_factor, mode_count):
    wiener = twf_alm.astype(jnp.float32)
    scaled = (raising_factor / mode_count)[:, None, None, :] * wiener
    raised = jnp.concatenate([scaled[..., 1:], jnp.zeros_like(scaled[..., :1])], axis=-1)
    stacked = jnp.stack(
        [
            tbar_alm.astype(jnp.float32),
            wiener,
            (degree / mode_count)[:, None, None, :] * wiener,
            raised,
        ],
        axis=2,
    )
    return stacked.reshape(stacked.shape[0], stacked.shape[1], 8, stacked.shape[4]).astype(
        jnp.bfloat16
    )


def mode_columns(small_orders, mode_count):
    return jnp.stack([small_orders, mode_count - 1 - small_orders], axis=1).reshape(-1)


def fourier_table(orders_int, pixel_count):
    pixel_index = lax.broadcasted_iota(jnp.int32, (orders_int.shape[0], pixel_count), 1)
    turns = orders_int[:, None] * pixel_index % pixel_count
    radians = turns.astype(jnp.float32) * (2.0 * math.pi / pixel_count)
    return jnp.stack([jnp.cos(radians), -jnp.sin(radians)], axis=0).astype(jnp.bfloat16)


def combine_modes(legendre_sums, orders_int, cos_cycle, sin_cycle, mode_count):
    orders_real = orders_int.astype(jnp.float32)
    inv_sin = 1.0 / sin_cycle
    ratio = (orders_real / mode_count)[:, None]
    theta_real = (cos_cycle * legendre_sums[:, 4] - legendre_sums[:, 6]) * inv_sin
    theta_imag = (cos_cycle * legendre_sums[:, 5] - legendre_sums[:, 7]) * inv_sin
    phi_real = -ratio * legendre_sums[:, 3] * inv_sin
    phi_imag = ratio * legendre_sums[:, 2] * inv_sin
    weight = (jnp.where(orders_int == 0, 1.0, 2.0) * mode_count ** (-0.5))[:, None]
    stacked = jnp.stack(
        [legendre_sums[:, 0], legendre_sums[:, 1], theta_real, theta_imag, phi_real, phi_imag],
        axis=1,
    )
    return (stacked * weight).astype(jnp.bfloat16)


def analysis_sets(spectra, colatitude, cycle_weight):
    with_cos = cycle_weight * jnp.cos(colatitude) / jnp.sin(colatitude)
    with_sin = cycle_weight / jnp.sin(colatitude)
    stacked = jnp.stack(
        [
            spectra[:, 0] * with_cos,
            spectra[:, 0] * with_sin,
            spectra[:, 1] * with_cos,
            spectra[:, 1] * with_sin,
        ],
        axis=1,
    )
    return stacked.reshape(spectra.shape[0], 8, spectra.shape[3], spectra.shape[4]).astype(
        jnp.bfloat16
    )


def estimate(merged, degree, orders, raising_factor, mode_count, cycle_count):
    level = degree[:, None, :]
    azimuth = orders[:, None, :]
    factor = raising_factor[:, None, :]

    def previous(values):
        return jnp.concatenate([jnp.zeros_like(values[..., :1]), values[..., :-1]], axis=-1)

    grad_real = (
        level * merged[:, :, 0] - factor * previous(merged[:, :, 2]) + azimuth * merged[:, :, 7]
    )
    grad_imag = (
        level * merged[:, :, 1] - factor * previous(merged[:, :, 3]) - azimuth * merged[:, :, 6]
    )
    curl_real = (
        level * merged[:, :, 4] - factor * previous(merged[:, :, 6]) - azimuth * merged[:, :, 3]
    )
    curl_imag = (
        level * merged[:, :, 5] - factor * previous(merged[:, :, 7]) + azimuth * merged[:, :, 2]
    )
    scale = (mode_count / cycle_count) ** 0.5 / jnp.sqrt(jnp.maximum(level * (level + 1.0), 1.0))
    scale = scale[:, :, None, :]
    return (
        jnp.stack([grad_real, grad_imag], axis=2) * scale,
        jnp.stack([curl_real, curl_imag], axis=2) * scale,
    )


def shards(tbar_alm, twf_alm, legendre, m_slots, cycle_order, colatitude, cycle_weight, pixel_mask):
    pairs_dev = tbar_alm.shape[0]
    row_count = tbar_alm.shape[3]
    mode_count = row_count - 1
    cycle_count = legendre.shape[2]
    cycle_dev = pixel_mask.shape[0]
    pixel_count = pixel_mask.shape[1]
    device_slot = lax.axis_index("ma")
    local_small = lax.dynamic_slice_in_dim(m_slots, device_slot * pairs_dev, pairs_dev)
    upper_half, degree, orders = pair_layout(local_small, mode_count)
    raising_factor = raising(degree, orders)
    coeff_sets = synthesis_sets(tbar_alm, twf_alm, degree, raising_factor, mode_count)
    halves = jnp.stack([jnp.logical_not(upper_half), upper_half], axis=1)
    masked = coeff_sets[:, None] * halves.astype(jnp.bfloat16)[:, :, None, None, :]
    legendre_sums = jnp.einsum(
        "phsck,pkr->scphr", masked, legendre, preferred_element_type=jnp.float32
    )
    legendre_sums = jnp.take(legendre_sums, cycle_order, axis=4)
    legendre_sums = legendre_sums.reshape(legendre_sums.shape[0], 8, 2 * pairs_dev, cycle_count)
    all_orders = mode_columns(m_slots, mode_count)
    dft_table = fourier_table(all_orders, pixel_count)
    pixel_weights = pixel_mask.astype(jnp.float32)
    slot_theta = jnp.take(colatitude, cycle_order)
    local_orders = mode_columns(local_small, mode_count)
    outgoing = combine_modes(
        legendre_sums, local_orders, jnp.cos(slot_theta), jnp.sin(slot_theta), mode_count
    )
    fourier = lax.all_to_all(outgoing, "ma", split_axis=3, concat_axis=2, tiled=True)
    fourier = fourier.reshape(fourier.shape[0], 3, 2, mode_count, cycle_dev)
    cycle_maps = jnp.einsum(
        "sqemr,emj->sqrj", fourier, dft_table, preferred_element_type=jnp.float32
    )
    products = (pixel_weights * cycle_maps[:, 0:1] * cycle_maps[:, 1:3]).astype(jnp.bfloat16)
    spectra = jnp.einsum("sqrj,emj->sqemr", products, dft_table, preferred_element_type=jnp.float32)
    received = (spectra * pixel_count ** (-0.5)).astype(jnp.bfloat16)
    returned = lax.all_to_all(received, "ma", split_axis=3, concat_axis=4, tiled=True)
    inverse = (
        jnp.zeros((cycle_count,), jnp.int32).at[cycle_order].set(lax.iota(jnp.int32, cycle_count))
    )
    spectra = jnp.take(returned, inverse, axis=4).astype(jnp.float32)
    weighted = analysis_sets(spectra, colatitude, cycle_weight)
    weighted = weighted.reshape(weighted.shape[0], 8, pairs_dev, 2, cycle_count)
    projected = jnp.einsum(
        "scphr,pkr->phsck", weighted, legendre, preferred_element_type=jnp.float32
    )
    merged = jnp.sum(projected * halves.astype(jnp.float32)[:, :, None, None, :], axis=1)
    return estimate(merged, degree, orders, raising_factor, mode_count, cycle_count)


LANES = 128
TURNS = 4
F32 = jnp.float32
BF16 = jnp.bfloat16


def split_tables(mode_count, pixel_count, sims):
    high_count = LANES // (TURNS * sims)
    low_count = pixel_count // high_count
    m = np.arange(mode_count)[:, None]
    low = np.arange(low_count)[None, :]
    high = (np.arange(LANES) // sims % high_count)[None, :] * low_count
    fine = (m * low % pixel_count) * (2.0 * math.pi / pixel_count)
    coarse = (m * high % pixel_count) * (2.0 * math.pi / pixel_count)

    def halves(values):
        upper = values.astype(np.float32).astype(BF16)
        return [upper, (values.astype(np.float32) - upper.astype(np.float32)).astype(BF16)]

    waves = [np.cos(fine).astype(BF16), (-np.sin(fine)).astype(BF16)]
    by_pixel = np.concatenate([wave.T for wave in waves], axis=0)
    by_mode = np.concatenate(waves + halves(np.cos(coarse)) + halves(np.sin(coarse)), axis=1)
    return by_pixel, by_mode


def spread_table(sims):
    comps = 2 * sims
    row = np.arange(2 * LANES)[:, None]
    col = np.arange(4 * LANES)[None, :]
    row_t, row_g, row_s, row_c = row // LANES, row // comps % 4, row // 2 % sims, row % 2
    col_t, col_s, col_c = col // (LANES // 2) % 2, col % sims, col // LANES % 2
    col_q = np.where(col < 2 * LANES, 0, 1 + col // (LANES // 4) % 2)
    group_q = np.array([0, 1, 2, 1])[row_g]
    source_c = np.where(col_q == 2, 1 - col_c, col_c)
    sign = np.where((col_q == 2) & (col_c == 0), -1.0, 1.0)
    hit = (row_t == col_t) & (row_s == col_s) & (group_q == col_q) & (row_c == source_c)
    return np.where(hit, sign, 0.0).astype(BF16)


def gather_table(sims):
    comps = 2 * sims
    row = np.arange(4 * LANES)[:, None]
    col = np.arange(LANES)[None, :]
    group, part = col // comps % 4, col % 2
    want_q = np.where((group == 1) | (group == 2), 1, 0)
    want_c = np.where(group >= 2, 1 - part, part)
    sign = np.where(((group == 2) & (part == 1)) | ((group == 3) & (part == 0)), -1.0, 1.0)
    hit = (row // (LANES // 4) % 2 == want_q) & (row // LANES % 2 == want_c)
    hit &= row % sims == col // 2 % sims
    turn = 2 * (row // (2 * LANES)) + row // (LANES // 2) % 2
    own = hit & (turn == col // (4 * comps))
    return np.concatenate([np.where(x, sign, 0.0) for x in (hit, own)], axis=1).astype(BF16)


def iota(shape, axis):
    return lax.broadcasted_iota(jnp.int32, shape, axis)


def div(values, size):
    return values >> (size.bit_length() - 1)


def mod(values, size):
    return values & (size - 1)


def one_hot(condition):
    return jnp.where(condition, 1.0, 0.0).astype(BF16)


def dot(left, right):
    return jnp.dot(left, right, preferred_element_type=F32)


def dot_t(left, right):
    return lax.dot_general(left, right, (((1,), (1,)), ((), ())), preferred_element_type=F32)


def fused_kernel(
    n, modes, rows, cycles, pixels, sims,
    slots_hbm, cycle_hbm, colat_hbm, weight_hbm, row_hbm, tbar_hbm, twf_hbm, leg_hbm, mask_hbm,
    pixel_hbm, mode_hbm, spread_hbm, gather_hbm,
    grad_ref, curl_ref,
    slots_s, cycle_s, colat_s, weight_s, slots_v, tbar_ref, twf_ref, leg_ref, mask_ref,
    pixel_v, mode_v, spread_v, gather_v,
    leg_all, prev_all, leg_p, prev_p, fs_ref, keep_ref, synth_ref, synth_l, anal_ref, anal_c, high_ref,
    pixmask_ref, maps_ref, pick_ref,
    send_m, recv_m, send_f, recv_f, send_p, recv_p, load_sem, move_sem,
):
    me = lax.axis_index("ma")
    work = n // TURNS
    pairs = tbar_ref.shape[0]
    comps = 2 * sims
    quad = LANES // (4 * comps)
    groups = pairs // quad
    span = 2 * cycles
    total = pairs * span
    count = n * 2 * pairs
    gh = 2 * groups
    high_count = LANES // (TURNS * sims)
    fine = pixels // high_count
    seat = lax.rem(lax.div(me, 2), work)
    prompt = n - n // 4
    first = 2 * gh
    is_worker = jnp.logical_and(lax.rem(me, 2) == 1, me < 2 * work)

    def slot_of(w, t):
        return 2 * w + t % 2 + t // 2 * 2 * work

    scalars = [(slots_hbm, slots_s), (colat_hbm, colat_s), (cycle_hbm, cycle_s), (weight_hbm, weight_s)]
    blocks = [(leg_hbm, leg_ref), (tbar_hbm, tbar_ref), (twf_hbm, twf_ref), (mask_hbm, mask_ref)]
    tables = [
        (row_hbm, slots_v), (mode_hbm, mode_v), (pixel_hbm, pixel_v), (spread_hbm, spread_v),
        (gather_hbm, gather_v),
    ]
    scalars, blocks, tables = [
        [pltpu.make_async_copy(source, target, load_sem.at[at]) for source, target in group]
        for at, group in enumerate((scalars, blocks, tables))
    ]
    for load in scalars + blocks:
        load.start()
    barrier = pltpu.get_barrier_semaphore()

    @pl.when(is_worker)
    def _():
        for off in range(1, n):
            pl.semaphore_signal(
                barrier, inc=1, device_id={"ma": lax.rem(me + off, n)},
                device_id_type=pl.DeviceIdType.MESH,
            )

    @pl.when(is_worker)
    def _():
        for load in tables:
            load.start()

    def remote(source, target, at, to):
        return pltpu.make_async_remote_copy(
            src_ref=source, dst_ref=target, send_sem=move_sem.at[0],
            recv_sem=move_sem.at[at], device_id={"ma": to},
            device_id_type=pl.DeviceIdType.MESH,
        )

    def settle(buffer, at):
        pltpu.make_async_copy(buffer, buffer, move_sem.at[at]).wait()

    for load in scalars:
        load.wait()

    row_shape = (pairs, rows)
    smaller = jnp.zeros(row_shape, jnp.int32)
    for p in range(pairs):
        smaller = jnp.where(iota(row_shape, 0) == p, slots_s[me * pairs + p], smaller)
    k = iota(row_shape, 1)
    upper = k >= modes - smaller
    degree = jnp.where(upper, k - 1, smaller + k).astype(F32)
    orders = jnp.where(upper, modes - 1 - smaller, smaller).astype(F32)
    eps = raising(degree, orders)
    upper_f = jnp.where(upper, 1.0, 0.0)
    lower_f = 1.0 - upper_f

    colat = jnp.zeros((cycles, LANES), F32)
    for r in range(cycles):
        colat = jnp.where(iota(colat.shape, 0) == r, colat_s[r], colat)
    csc = 1.0 / jnp.sin(colat)
    cot = jnp.cos(colat) * csc
    lane_group = mod(div(iota(colat.shape, 1), comps), 4)
    base = jnp.where(lane_group == 0, 1.0, jnp.where(lane_group == 1, cot, csc))

    halves = [
        [jnp.broadcast_to(part[p : p + 1], (cycles, rows)).astype(BF16) for part in (lower_f, upper_f)]
        for p in range(pairs)
    ]

    for load in blocks:
        load.wait()

    @pl.when(jnp.logical_not(is_worker))
    def _():
        pl.semaphore_wait(barrier, work)
        send_m[...] = mask_ref[...].astype(F32).astype(BF16)
        turn = lax.rem(me, 2) + 2 * lax.div(me, 2 * work)
        remote(send_m, recv_m.at[turn], 4, 2 * lax.div(lax.rem(me, 2 * work), 2) + 1).start()

    lane = iota((8, LANES), 1)
    lane_quad = div(lane, 4 * comps)
    is_phi = mod(div(lane, comps), 4) == 2
    for g in range(groups):
        sets, legs = [], []
        small = jnp.zeros((8, LANES), jnp.int32)
        for q in range(quad):
            p = g * quad + q
            small = jnp.where(lane_quad == q, slots_s[me * pairs + p], small)
            tbar = jnp.concatenate([tbar_ref[p, s].astype(F32) for s in range(sims)], axis=0)
            twf = jnp.concatenate([twf_ref[p, s].astype(F32) for s in range(sims)], axis=0)
            deg_p, eps_p = degree[p : p + 1] / modes, eps[p : p + 1] / modes
            scaled = -(eps_p * twf)
            raised = jnp.concatenate([scaled[:, 1:], jnp.zeros_like(scaled[:, :1])], axis=1)
            sets += [tbar, deg_p * twf, twf, raised]
            legs += [leg_ref[p] * part for part in halves[p]]
        legs = jnp.concatenate(legs, axis=0)
        leg_all[pl.ds(g * quad * span, quad * span), :] = legs
        out = dot_t(legs, jnp.concatenate(sets, axis=0).astype(BF16))
        picked = out[:span]
        for q in range(1, quad):
            own = div(iota(picked.shape, 1), 4 * comps) == q
            picked = jnp.where(own, out[q * span : (q + 1) * span], picked)
        for h in range(2):
            order = (modes - 1 - small if h else small)[0:1]
            norm = jnp.where(order == 0, 1.0, 2.0) * modes ** (-0.5)
            norm = jnp.where(is_phi[0:1], norm * (order.astype(F32) / modes), norm)
            fs_ref[pl.ds((2 * g + h) * cycles, cycles), :] = picked[h * cycles : (h + 1) * cycles] * (base * norm)

    for t in range(TURNS):
        for w in range(work):
            send_f[t, w] = fs_ref[pl.ds(cycle_s[slot_of(w, t)], gh, stride=cycles), :].astype(BF16)

    @pl.when(is_worker)
    def _():
        pl.semaphore_wait(barrier, work - 1)

    tardy = 1 + lax.div(me, prompt)
    for w in reversed(range(work)):
        @pl.when(me != 2 * w + 1)
        def _():
            remote(send_f.at[:, w], recv_f.at[:, me], tardy, 2 * w + 1).start()

    lane_shape = (8, LANES)
    keep_lane = iota(lane_shape, 1)
    lane_seat = mod(div(keep_lane, gh), TURNS * work)
    theta_l = jnp.zeros(lane_shape, F32)
    weight_l = jnp.zeros(lane_shape, F32)
    place_shape = (LANES, total)
    place_row, place_lane = iota(place_shape, 0), iota(place_shape, 1)
    row_seat = mod(div(place_row, gh), TURNS * work)
    row_cycle = jnp.zeros(place_shape, jnp.int32)
    for t in range(TURNS):
        for w in range(work):
            r = cycle_s[slot_of(w, t)]
            at = t * work + w
            theta_l = jnp.where(lane_seat == at, colat_s[r], theta_l)
            weight_l = jnp.where(lane_seat == at, weight_s[r], weight_l)
            row_cycle = jnp.where(row_seat == at, r, row_cycle)
    with_sin = weight_l / jnp.sin(theta_l)
    with_cos = weight_l * jnp.cos(theta_l) / jnp.sin(theta_l)
    lane_g, lane_side = mod(div(keep_lane, 2), groups), div(keep_lane, LANES // 2)
    for p in range(pairs):
        mine = jnp.logical_and(lane_g == p // quad, lane_side == p % 2)
        keep_ref[p, 0] = jnp.where(mine, with_cos, 0.0)
        keep_ref[p, 1] = jnp.where(mine, with_sin, 0.0)
    for p in range(pairs):
        leg = leg_ref[p].astype(F32)
        prev = jnp.concatenate([jnp.zeros_like(leg[:, :1]), leg[:, : rows - 1]], axis=1)
        low, high = lower_f[p : p + 1], upper_f[p : p + 1]
        prev_all[pl.ds(p * span, span), :] = jnp.concatenate(
            [prev * low, prev * high], axis=0
        ).astype(BF16)
    row_pair = mod(div(place_row, 2), groups) * quad + div(place_row, LANES // 2)
    match = jnp.logical_and(
        row_cycle == mod(place_lane, cycles), mod(place_row, 2) == mod(div(place_lane, cycles), 2)
    )
    for k in range(quad // 2):
        place = one_hot(jnp.logical_and(match, row_pair + 2 * k == div(place_lane, span)))
        leg_p[k] = dot(place, leg_all[...]).astype(BF16)
        prev_p[k] = dot(place, prev_all[...]).astype(BF16)
    scale = (modes / cycles) ** 0.5 / jnp.sqrt(jnp.maximum(degree * (degree + 1.0), 1.0))
    f_level, f_eps, f_order = degree * scale, eps * scale, orders * scale

    @pl.when(is_worker)
    def _():
        for load in tables:
            load.wait()
        pair_count = slots_v.shape[1]

        ahead = prompt * gh

        def pair_of(at):
            behind = at >= quad * ahead
            rest = at - quad * ahead
            early = (at * (65536 // ahead + 1)) >> 16
            q = jnp.where(behind, div(rest, (n - prompt) * gh), early)
            inner = jnp.where(behind, ahead + mod(rest, (n - prompt) * gh), at - ahead * early)
            return div(inner, gh) * pairs + div(mod(inner, gh), 2) * quad + q

        slots = jnp.broadcast_to(slots_v[...], (pair_count, pair_count)).astype(F32).astype(BF16)
        spread = one_hot(iota((pair_count, count), 0) == pair_of(iota((pair_count, count), 1)))
        spread_t = one_hot(iota((count, pair_count), 1) == pair_of(iota((count, pair_count), 0)))
        by_lane = dot(slots[:16], spread)[0:8]
        by_lane = jnp.where(mod(iota(by_lane.shape, 1), 2) == 1, modes - 1.0 - by_lane, by_lane)
        by_row = dot_t(spread_t, slots)
        by_row = jnp.where(mod(iota(by_row.shape, 0), 2) == 1, modes - 1.0 - by_row, by_row)
        select = one_hot(iota((modes, count), 0).astype(F32) == by_lane[0:1])
        select_t = jnp.concatenate(
            [
                one_hot((iota(by_row.shape, 1) + at).astype(F32) == by_row)
                for at in range(0, modes, pair_count)
            ],
            axis=1,
        )
        moved = dot(pixel_v[...], select).astype(BF16)
        cut_at = quad * ahead
        synth_ref[...] = jnp.concatenate([moved[:fine, :cut_at], moved[fine:, :cut_at]], axis=1)
        synth_l[...] = jnp.concatenate([moved[:fine, cut_at:], moved[fine:, cut_at:]], axis=1)
        moved = dot(select_t, mode_v[...])
        anal_ref[:count] = moved[:, :fine].astype(BF16)
        anal_ref[count:] = moved[:, fine : 2 * fine].astype(BF16)
        anal_c[...] = jnp.concatenate(
            [
                moved[q * ahead : q * ahead + first, part * fine : (part + 1) * fine]
                for part in range(2)
                for q in range(quad)
            ],
            axis=0,
        ).astype(BF16)
        at = 2 * fine
        for part in range(2):
            high_ref[part] = moved[:, at : at + LANES] + moved[:, at + LANES : at + 2 * LANES]
            at += 2 * LANES

        recv_f[:, me] = send_f[:, seat]
        cut = fine // LANES
        grid = (TURNS * mask_ref.shape[0], LANES)
        m_turn = div(iota(grid, 1), LANES // 2)
        m_high = mod(div(iota(grid, 1), sims), high_count)
        for j in range(TURNS // 2):
            first_row = ((m_turn + 2 * j) * high_count + m_high) * cut
            for at in range(cut):
                pick_ref[j, at] = one_hot(iota(grid, 0) == first_row + at)
        recv_m[1] = mask_ref[...].astype(F32).astype(BF16)
        quarter = mod(div(iota((8, 2 * LANES), 1), 4 * comps), quad)[0:1]

        def turn_up(sources, rows_at, size):
            turns = [
                recv_f[t, pl.ds(sources, size // quad // gh)].reshape(size // quad, LANES)
                for t in range(TURNS)
            ]
            pairs_of = [
                jnp.concatenate(turns[2 * j : 2 * j + 2], axis=1) for j in range(TURNS // 2)
            ]
            got = [pair * one_hot(quarter == q) for pair in pairs_of for q in range(quad)]
            spread_f = dot(jnp.concatenate(got, axis=0), spread_v[...])
            cos_h, sin_h = high_ref[0, pl.ds(rows_at, size)], high_ref[1, pl.ds(rows_at, size)]
            real, imag = [], []
            for j in range(TURNS // 2):
                for kind in range(2):
                    at = 2 * kind * LANES
                    re = spread_f[j * size : (j + 1) * size, at : at + LANES]
                    im = spread_f[j * size : (j + 1) * size, at + LANES : at + 2 * LANES]
                    real.append((re * cos_h - im * sin_h).astype(BF16))
                    imag.append((re * sin_h + im * cos_h).astype(BF16))
            return jnp.concatenate(
                [jnp.concatenate(real, axis=1), jnp.concatenate(imag, axis=1)], axis=0
            )

        settle(recv_f.at[:, pl.ds(0, prompt - 1)], 1)
        maps_ref[...] = dot(synth_ref[...], turn_up(0, 0, cut_at))
        settle(recv_m.at[pl.ds(0, TURNS - 1)], 4)
        both = recv_m[...].astype(F32).reshape(TURNS * mask_ref.shape[0], LANES)
        both_t = both.T.astype(BF16)
        for j in range(TURNS // 2):
            for at in range(cut):
                pixmask_ref[j, pl.ds(at * LANES, LANES), :] = dot(both_t, pick_ref[j, at])
        settle(recv_f.at[:, pl.ds(0, n - prompt)], 2)
        maps = maps_ref[...] + dot(synth_l[...], turn_up(prompt, cut_at, count - cut_at))
        products = jnp.concatenate(
            [
                pixmask_ref[j]
                * maps[:, 2 * j * LANES : (2 * j + 1) * LANES]
                * maps[:, (2 * j + 1) * LANES : (2 * j + 2) * LANES]
                for j in range(TURNS // 2)
            ],
            axis=1,
        ).astype(BF16)
        def bring_down(table, cos_h, sin_h, split):
            size = cos_h.shape[0]
            half = dot(table, products)
            parts = []
            for q in range(2):
                c_part = half[:size, q * LANES : (q + 1) * LANES]
                s_part = half[size:, q * LANES : (q + 1) * LANES]
                parts.append((cos_h * c_part + sin_h * s_part).astype(BF16))
                parts.append((cos_h * s_part - sin_h * c_part).astype(BF16))
            parts = jnp.concatenate(parts, axis=1)
            if not split:
                return dot(parts, gather_v[:, LANES:]) * pixels ** (-0.5)
            lane = iota((8, 4 * LANES), 1)
            turn = (2 * div(lane, 2 * LANES) + mod(div(lane, LANES // 2), 2))[0:1]
            parts = jnp.concatenate([parts * one_hot(turn == t) for t in range(TURNS)], axis=0)
            return dot(parts, gather_v[:, :LANES]) * pixels ** (-0.5)

        def pack(blocks):
            lane_quad = div(iota(blocks[0].shape, 1), 4 * comps)
            whole = blocks[0]
            for q in range(1, quad):
                whole = jnp.where(lane_quad == q, blocks[q], whole)
            return whole.astype(BF16).reshape(whole.shape[0] // gh, gh, LANES)

        high_c = [
            jnp.concatenate([high_ref[part, pl.ds(q * ahead, first)] for q in range(quad)], axis=0)
            for part in range(2)
        ]
        spectra = bring_down(anal_c[...], *high_c, True)
        for t in range(TURNS):
            at = t * quad * first
            send_p[t, pl.ds(0, 2)] = pack(
                [spectra[at + q * first : at + (q + 1) * first] for q in range(quad)]
            )
        remote(send_p.at[:, 0], recv_p.at[:, seat], 3, 0).start()

        @pl.when(me != 1)
        def _():
            remote(send_p.at[:, 1], recv_p.at[:, seat], 3, 1).start()

        spectra = bring_down(anal_ref[...], high_ref[0], high_ref[1], False)
        behind = n - prompt
        rest = [
            jnp.concatenate(
                [
                    spectra[q * ahead + first : (q + 1) * ahead],
                    spectra[cut_at + q * behind * gh : cut_at + (q + 1) * behind * gh],
                ],
                axis=0,
            )
            for q in range(quad)
        ]
        for t in range(TURNS):
            send_p[t, pl.ds(2, n - 2)] = pack(
                [
                    rest[q] if q == t else pltpu.roll(rest[q], (q - t) * 4 * comps % LANES, 1)
                    for q in range(quad)
                ]
            )
        for d in range(2, n):
            if d % 2 == 0 or d >= 2 * work:
                remote(send_p.at[:, d], recv_p.at[:, seat], 3, d).start()
            else:
                @pl.when(me != d)
                def _():
                    remote(send_p.at[:, d], recv_p.at[:, seat], 3, d).start()
        recv_p[:, seat] = send_p[:, me]
        settle(recv_p.at[:, pl.ds(0, work - 1)], 3)

    @pl.when(jnp.logical_not(is_worker))
    def _():
        settle(recv_p, 3)

    came = recv_p[...].astype(F32).reshape(TURNS * work * gh, LANES)
    came = jnp.concatenate([came, came], axis=0).T
    here, before = {}, {}
    for k in range(quad // 2):
        members = [p for p in range(pairs) if p % quad // 2 == k]
        first_k, second_k = [], []
        for p in members:
            at = p % quad * 4 * comps
            four = [came[at + g * comps : at + (g + 1) * comps] for g in range(4)]
            with_cos, with_sin = keep_ref[p, 0], keep_ref[p, 1]
            first_k += [four[0] * with_cos, four[1] * with_cos]
            first_k += [four[2] * with_sin, four[3] * with_sin]
            second_k += [four[0] * with_sin, four[1] * with_sin]
        out_a = dot(jnp.concatenate(first_k, axis=0).astype(BF16), leg_p[k])
        out_b = dot(jnp.concatenate(second_k, axis=0).astype(BF16), prev_p[k])
        for at, p in enumerate(members):
            here[p] = out_a[at * 4 * comps : (at + 1) * 4 * comps]
            before[p] = out_b[at * 2 * comps : (at + 1) * 2 * comps]
    for p in range(pairs):
        lev, ep, az = f_level[p : p + 1], f_eps[p : p + 1], f_order[p : p + 1]
        grad = (
            lev * here[p][:comps] - ep * before[p][:comps]
            + az * here[p][2 * comps : 3 * comps]
        )
        curl = (
            lev * here[p][comps : 2 * comps] - ep * before[p][comps:]
            + az * here[p][3 * comps :]
        )
        for s in range(sims):
            grad_ref[p, s] = grad[2 * s : 2 * s + 2]
            curl_ref[p, s] = curl[2 * s : 2 * s + 2]

    @pl.when(is_worker)
    def _():
        settle(send_f.at[:, pl.ds(0, work - 1)], 0)
        settle(send_p.at[:, pl.ds(0, n - 1)], 0)

    @pl.when(jnp.logical_not(is_worker))
    def _():
        settle(send_f, 0)
        settle(send_m, 0)


def store_kernel(grad_ref, curl_ref, grad_hbm, curl_hbm, sem):
    copies = [
        pltpu.make_async_copy(grad_ref, grad_hbm, sem),
        pltpu.make_async_copy(curl_ref, curl_hbm, sem),
    ]
    for copy in copies:
        copy.start()
    for copy in copies:
        copy.wait()


def fused(tbar_alm, twf_alm, legendre, m_slots, cycle_order, colatitude, cycle_weight, pixel_mask, n):
    pairs, sims, _, rows = tbar_alm.shape
    modes = rows - 1
    cycles = legendre.shape[2]
    pixels = pixel_mask.shape[1]
    total = pairs * 2 * cycles
    count = n * 2 * pairs
    work = n // TURNS
    gh = 2 * pairs * 8 * sims // LANES
    fine = pixels * TURNS * sims // LANES
    by_cycle = jnp.transpose(legendre, (0, 2, 1))
    by_pixel, by_mode = split_tables(modes, pixels, sims)
    tables = [jnp.asarray(x) for x in (by_pixel, by_mode, spread_table(sims), gather_table(sims))]
    vmem, anywhere = pl.BlockSpec(memory_space=pltpu.VMEM), pl.BlockSpec(memory_space=pl.ANY)
    out = pltpu.VMEM(tbar_alm.shape, F32)
    mask_shape = (pixels // LANES, LANES)
    made = pl.pallas_call(
        functools.partial(fused_kernel, n, modes, rows, cycles, pixels, sims),
        out_shape=(out, out),
        in_specs=[anywhere] * 13,
        out_specs=(vmem, vmem),
        scratch_shapes=[
            pltpu.SMEM(m_slots.shape, jnp.int32),
            pltpu.SMEM(cycle_order.shape, jnp.int32),
            pltpu.SMEM(colatitude.shape, F32),
            pltpu.SMEM(cycle_weight.shape, F32),
            pltpu.VMEM((1, m_slots.shape[0]), jnp.int32),
            pltpu.VMEM(tbar_alm.shape, BF16),
            pltpu.VMEM(twf_alm.shape, BF16),
            pltpu.VMEM(by_cycle.shape, BF16),
            pltpu.VMEM(mask_shape, jnp.int32),
        ]
        + [pltpu.VMEM(table.shape, BF16) for table in tables]
        + [
            pltpu.VMEM((total, rows), BF16),
            pltpu.VMEM((total, rows), BF16),
            pltpu.VMEM((total // LANES, LANES, rows), BF16),
            pltpu.VMEM((total // LANES, LANES, rows), BF16),
            pltpu.VMEM((gh * cycles, LANES), F32),
            pltpu.VMEM((pairs, 2, 8, LANES), F32),
            pltpu.VMEM((fine, 2 * count - count // 2), BF16),
            pltpu.VMEM((fine, count // 2), BF16),
            pltpu.VMEM((2 * count, fine), BF16),
            pltpu.VMEM((count // 4, fine), BF16),
            pltpu.VMEM((2, count, LANES), F32),
            pltpu.VMEM((TURNS // 2, fine, LANES), F32),
            pltpu.VMEM((fine, 4 * LANES), F32),
            pltpu.VMEM((TURNS // 2, fine // LANES, TURNS * mask_shape[0], LANES), BF16),
            pltpu.VMEM(mask_shape, BF16),
            pltpu.VMEM((TURNS,) + mask_shape, BF16),
            pltpu.VMEM((TURNS, work, gh, LANES), BF16),
            pltpu.VMEM((TURNS, n, gh, LANES), BF16),
            pltpu.VMEM((TURNS, n, gh, LANES), BF16),
            pltpu.VMEM((TURNS, work, gh, LANES), BF16),
            pltpu.SemaphoreType.DMA((3,)),
            pltpu.SemaphoreType.DMA((5,)),
        ],
        compiler_params=pltpu.CompilerParams(collective_id=0, has_side_effects=True),
        name="estimator",
    )(
        m_slots, cycle_order, colatitude, cycle_weight, m_slots.reshape(1, -1), tbar_alm,
        twf_alm, by_cycle, pixel_mask.reshape(mask_shape), *tables,
    )
    return pl.pallas_call(
        store_kernel,
        out_shape=(jax.ShapeDtypeStruct(tbar_alm.shape, F32),) * 2,
        in_specs=[vmem] * 2,
        out_specs=[anywhere] * 2,
        scratch_shapes=[pltpu.SemaphoreType.DMA],
        name="store",
    )(*(pltpu.with_memory_space_constraint(x, pltpu.VMEM) for x in made))


def body(n, *args):
    tbar_alm, legendre, pixel_mask = args[0], args[2], args[7]
    pairs, sims, _, rows = tbar_alm.shape
    cycles = legendre.shape[2]
    pixels = pixel_mask.shape[1]
    fits = (
        pairs == 8
        and cycles == n == 16
        and pixel_mask.shape[0] == 1
        and rows == 257
        and pairs * n == LANES
        and sims == 4
        and pixels == 4096
    )
    return fused(*args, n) if fits else shards(*args)


def solution(mesh):
    return jax.shard_map(
        functools.partial(body, mesh.shape["ma"]),
        mesh=mesh,
        in_specs=(
            P("ma", "grp", None, None),
            P("ma", "grp", None, None),
            P("ma", None, None),
            P(),
            P(),
            P(),
            P(),
            P("ma", None),
        ),
        out_specs=(P("ma", "grp", None, None), P("ma", "grp", None, None)),
        check_vma=False,
    )
```

```python
import math

import functools

import jax
import jax.numpy as jnp
import numpy as np
from jax import lax
from jax.experimental import pallas as pl
from jax.experimental.pallas import tpu as pltpu
from jax.sharding import PartitionSpec as P


def pair_layout(small_orders, mode_count):
    row_index = lax.broadcasted_iota(jnp.int32, (small_orders.shape[0], mode_count + 1), 1)
    smaller = small_orders[:, None]
    upper_half = row_index >= mode_count - smaller
    degree = jnp.where(upper_half, row_index - 1, smaller + row_index)
    orders = jnp.where(upper_half, mode_count - 1 - smaller, smaller + 0 * row_index)
    return (upper_half, degree.astype(jnp.float32), orders.astype(jnp.float32))


def raising(degree, orders):
    square = (
        (degree * degree - orders * orders)
        * (2.0 * degree + 1.0)
        / jnp.maximum(2.0 * degree - 1.0, 1.0)
    )
    return jnp.where(degree > orders, jnp.sqrt(jnp.where(degree > orders, square, 0.0)), 0.0)


def synthesis_sets(tbar_alm, twf_alm, degree, raising_factor, mode_count):
    wiener = twf_alm.astype(jnp.float32)
    scaled = (raising_factor / mode_count)[:, None, None, :] * wiener
    raised = jnp.concatenate([scaled[..., 1:], jnp.zeros_like(scaled[..., :1])], axis=-1)
    stacked = jnp.stack(
        [
            tbar_alm.astype(jnp.float32),
            wiener,
            (degree / mode_count)[:, None, None, :] * wiener,
            raised,
        ],
        axis=2,
    )
    return stacked.reshape(stacked.shape[0], stacked.shape[1], 8, stacked.shape[4]).astype(
        jnp.bfloat16
    )


def mode_columns(small_orders, mode_count):
    return jnp.stack([small_orders, mode_count - 1 - small_orders], axis=1).reshape(-1)


def fourier_table(orders_int, pixel_count):
    pixel_index = lax.broadcasted_iota(jnp.int32, (orders_int.shape[0], pixel_count), 1)
    turns = orders_int[:, None] * pixel_index % pixel_count
    radians = turns.astype(jnp.float32) * (2.0 * math.pi / pixel_count)
    return jnp.stack([jnp.cos(radians), -jnp.sin(radians)], axis=0).astype(jnp.bfloat16)


def combine_modes(legendre_sums, orders_int, cos_cycle, sin_cycle, mode_count):
    orders_real = orders_int.astype(jnp.float32)
    inv_sin = 1.0 / sin_cycle
    ratio = (orders_real / mode_count)[:, None]
    theta_real = (cos_cycle * legendre_sums[:, 4] - legendre_sums[:, 6]) * inv_sin
    theta_imag = (cos_cycle * legendre_sums[:, 5] - legendre_sums[:, 7]) * inv_sin
    phi_real = -ratio * legendre_sums[:, 3] * inv_sin
    phi_imag = ratio * legendre_sums[:, 2] * inv_sin
    weight = (jnp.where(orders_int == 0, 1.0, 2.0) * mode_count ** (-0.5))[:, None]
    stacked = jnp.stack(
        [legendre_sums[:, 0], legendre_sums[:, 1], theta_real, theta_imag, phi_real, phi_imag],
        axis=1,
    )
    return (stacked * weight).astype(jnp.bfloat16)


def analysis_sets(spectra, colatitude, cycle_weight):
    with_cos = cycle_weight * jnp.cos(colatitude) / jnp.sin(colatitude)
    with_sin = cycle_weight / jnp.sin(colatitude)
    stacked = jnp.stack(
        [
            spectra[:, 0] * with_cos,
            spectra[:, 0] * with_sin,
            spectra[:, 1] * with_cos,
            spectra[:, 1] * with_sin,
        ],
        axis=1,
    )
    return stacked.reshape(spectra.shape[0], 8, spectra.shape[3], spectra.shape[4]).astype(
        jnp.bfloat16
    )


def estimate(merged, degree, orders, raising_factor, mode_count, cycle_count):
    level = degree[:, None, :]
    azimuth = orders[:, None, :]
    factor = raising_factor[:, None, :]

    def previous(values):
        return jnp.concatenate([jnp.zeros_like(values[..., :1]), values[..., :-1]], axis=-1)

    grad_real = (
        level * merged[:, :, 0] - factor * previous(merged[:, :, 2]) + azimuth * merged[:, :, 7]
    )
    grad_imag = (
        level * merged[:, :, 1] - factor * previous(merged[:, :, 3]) - azimuth * merged[:, :, 6]
    )
    curl_real = (
        level * merged[:, :, 4] - factor * previous(merged[:, :, 6]) - azimuth * merged[:, :, 3]
    )
    curl_imag = (
        level * merged[:, :, 5] - factor * previous(merged[:, :, 7]) + azimuth * merged[:, :, 2]
    )
    scale = (mode_count / cycle_count) ** 0.5 / jnp.sqrt(jnp.maximum(level * (level + 1.0), 1.0))
    scale = scale[:, :, None, :]
    return (
        jnp.stack([grad_real, grad_imag], axis=2) * scale,
        jnp.stack([curl_real, curl_imag], axis=2) * scale,
    )


def shards(tbar_alm, twf_alm, legendre, m_slots, cycle_order, colatitude, cycle_weight, pixel_mask):
    pairs_dev = tbar_alm.shape[0]
    row_count = tbar_alm.shape[3]
    mode_count = row_count - 1
    cycle_count = legendre.shape[2]
    cycle_dev = pixel_mask.shape[0]
    pixel_count = pixel_mask.shape[1]
    device_slot = lax.axis_index("ma")
    local_small = lax.dynamic_slice_in_dim(m_slots, device_slot * pairs_dev, pairs_dev)
    upper_half, degree, orders = pair_layout(local_small, mode_count)
    raising_factor = raising(degree, orders)
    coeff_sets = synthesis_sets(tbar_alm, twf_alm, degree, raising_factor, mode_count)
    halves = jnp.stack([jnp.logical_not(upper_half), upper_half], axis=1)
    masked = coeff_sets[:, None] * halves.astype(jnp.bfloat16)[:, :, None, None, :]
    legendre_sums = jnp.einsum(
        "phsck,pkr->scphr", masked, legendre, preferred_element_type=jnp.float32
    )
    legendre_sums = jnp.take(legendre_sums, cycle_order, axis=4)
    legendre_sums = legendre_sums.reshape(legendre_sums.shape[0], 8, 2 * pairs_dev, cycle_count)
    all_orders = mode_columns(m_slots, mode_count)
    dft_table = fourier_table(all_orders, pixel_count)
    pixel_weights = pixel_mask.astype(jnp.float32)
    slot_theta = jnp.take(colatitude, cycle_order)
    local_orders = mode_columns(local_small, mode_count)
    outgoing = combine_modes(
        legendre_sums, local_orders, jnp.cos(slot_theta), jnp.sin(slot_theta), mode_count
    )
    fourier = lax.all_to_all(outgoing, "ma", split_axis=3, concat_axis=2, tiled=True)
    fourier = fourier.reshape(fourier.shape[0], 3, 2, mode_count, cycle_dev)
    cycle_maps = jnp.einsum(
        "sqemr,emj->sqrj", fourier, dft_table, preferred_element_type=jnp.float32
    )
    products = (pixel_weights * cycle_maps[:, 0:1] * cycle_maps[:, 1:3]).astype(jnp.bfloat16)
    spectra = jnp.einsum("sqrj,emj->sqemr", products, dft_table, preferred_element_type=jnp.float32)
    received = (spectra * pixel_count ** (-0.5)).astype(jnp.bfloat16)
    returned = lax.all_to_all(received, "ma", split_axis=3, concat_axis=4, tiled=True)
    inverse = (
        jnp.zeros((cycle_count,), jnp.int32).at[cycle_order].set(lax.iota(jnp.int32, cycle_count))
    )
    spectra = jnp.take(returned, inverse, axis=4).astype(jnp.float32)
    weighted = analysis_sets(spectra, colatitude, cycle_weight)
    weighted = weighted.reshape(weighted.shape[0], 8, pairs_dev, 2, cycle_count)
    projected = jnp.einsum(
        "scphr,pkr->phsck", weighted, legendre, preferred_element_type=jnp.float32
    )
    merged = jnp.sum(projected * halves.astype(jnp.float32)[:, :, None, None, :], axis=1)
    return estimate(merged, degree, orders, raising_factor, mode_count, cycle_count)


LANES = 128
TURNS = 4
F32 = jnp.float32
BF16 = jnp.bfloat16


def split_tables(mode_count, pixel_count, sims):
    high_count = LANES // (TURNS * sims)
    low_count = pixel_count // high_count
    m = np.arange(mode_count)[:, None]
    low = np.arange(low_count)[None, :]
    high = (np.arange(LANES) // sims % high_count)[None, :] * low_count
    fine = (m * low % pixel_count) * (2.0 * math.pi / pixel_count)
    coarse = (m * high % pixel_count) * (2.0 * math.pi / pixel_count)

    def halves(values):
        upper = values.astype(np.float32).astype(BF16)
        return [upper, (values.astype(np.float32) - upper.astype(np.float32)).astype(BF16)]

    waves = [np.cos(fine).astype(BF16), (-np.sin(fine)).astype(BF16)]
    by_pixel = np.concatenate([wave.T for wave in waves], axis=0)
    by_mode = np.concatenate(waves + halves(np.cos(coarse)) + halves(np.sin(coarse)), axis=1)
    return by_pixel, by_mode


def spread_table(sims):
    comps = 2 * sims
    row = np.arange(2 * LANES)[:, None]
    col = np.arange(4 * LANES)[None, :]
    row_t, row_g, row_s, row_c = row // LANES, row // comps % 4, row // 2 % sims, row % 2
    col_t, col_s, col_c = col // (LANES // 2) % 2, col % sims, col // LANES % 2
    col_q = np.where(col < 2 * LANES, 0, 1 + col // (LANES // 4) % 2)
    group_q = np.array([0, 1, 2, 1])[row_g]
    source_c = np.where(col_q == 2, 1 - col_c, col_c)
    sign = np.where((col_q == 2) & (col_c == 0), -1.0, 1.0)
    hit = (row_t == col_t) & (row_s == col_s) & (group_q == col_q) & (row_c == source_c)
    return np.where(hit, sign, 0.0).astype(BF16)


def gather_table(sims):
    comps = 2 * sims
    row = np.arange(4 * LANES)[:, None]
    col = np.arange(LANES)[None, :]
    group, part = col // comps % 4, col % 2
    want_q = np.where((group == 1) | (group == 2), 1, 0)
    want_c = np.where(group >= 2, 1 - part, part)
    sign = np.where(((group == 2) & (part == 1)) | ((group == 3) & (part == 0)), -1.0, 1.0)
    hit = (row // (LANES // 4) % 2 == want_q) & (row // LANES % 2 == want_c)
    hit &= row % sims == col // 2 % sims
    turn = 2 * (row // (2 * LANES)) + row // (LANES // 2) % 2
    own = hit & (turn == col // (4 * comps))
    return np.concatenate([np.where(x, sign, 0.0) for x in (hit, own)], axis=1).astype(BF16)


def iota(shape, axis):
    return lax.broadcasted_iota(jnp.int32, shape, axis)


def div(values, size):
    return values >> (size.bit_length() - 1)


def mod(values, size):
    return values & (size - 1)


def one_hot(condition):
    return jnp.where(condition, 1.0, 0.0).astype(BF16)


def dot(left, right):
    return jnp.dot(left, right, preferred_element_type=F32)


def dot_t(left, right):
    return lax.dot_general(left, right, (((1,), (1,)), ((), ())), preferred_element_type=F32)


def fused_kernel(
    n, modes, rows, cycles, pixels, sims,
    slots_hbm, cycle_hbm, colat_hbm, weight_hbm, row_hbm, tbar_hbm, twf_hbm, leg_hbm, mask_hbm,
    pixel_hbm, mode_hbm, spread_hbm, gather_hbm,
    grad_ref, curl_ref,
    slots_s, cycle_s, colat_s, weight_s, slots_v, tbar_ref, twf_ref, leg_ref, mask_ref,
    pixel_v, mode_v, spread_v, gather_v,
    leg_all, prev_all, fold_ref, fs_ref, keep_ref, synth_ref, synth_l, anal_ref, anal_c, high_ref,
    pixmask_ref, maps_ref, pick_ref,
    send_m, recv_m, send_f, recv_f, send_p, recv_p, load_sem, move_sem,
):
    me = lax.axis_index("ma")
    work = n // TURNS
    pairs = tbar_ref.shape[0]
    comps = 2 * sims
    quad = LANES // (4 * comps)
    groups = pairs // quad
    span = 2 * cycles
    total = pairs * span
    count = n * 2 * pairs
    gh = 2 * groups
    high_count = LANES // (TURNS * sims)
    fine = pixels // high_count
    seat = lax.rem(lax.div(me, 2), work)
    prompt = n - n // 4
    first = 2 * gh
    is_worker = jnp.logical_and(lax.rem(me, 2) == 1, me < 2 * work)

    def slot_of(w, t):
        return 2 * w + t % 2 + t // 2 * 2 * work

    scalars = [(slots_hbm, slots_s), (colat_hbm, colat_s), (cycle_hbm, cycle_s), (weight_hbm, weight_s)]
    blocks = [(leg_hbm, leg_ref), (tbar_hbm, tbar_ref), (twf_hbm, twf_ref), (mask_hbm, mask_ref)]
    tables = [
        (row_hbm, slots_v), (mode_hbm, mode_v), (pixel_hbm, pixel_v), (spread_hbm, spread_v),
        (gather_hbm, gather_v),
    ]
    scalars, blocks, tables = [
        [pltpu.make_async_copy(source, target, load_sem.at[at]) for source, target in group]
        for at, group in ((0, scalars), (1, blocks), (1, tables))
    ]
    for load in blocks + scalars:
        load.start()
    barrier = pltpu.get_barrier_semaphore()

    @pl.when(is_worker)
    def _():
        for off in range(1, n):
            pl.semaphore_signal(
                barrier, inc=1, device_id={"ma": lax.rem(me + off, n)},
                device_id_type=pl.DeviceIdType.MESH,
            )


    def remote(source, target, at, to):
        return pltpu.make_async_remote_copy(
            src_ref=source, dst_ref=target, send_sem=load_sem.at[0],
            recv_sem=move_sem.at[at], device_id={"ma": to},
            device_id_type=pl.DeviceIdType.MESH,
        )

    def settle(buffer, at):
        sem = load_sem.at[0] if at is None else move_sem.at[at]
        pltpu.make_async_copy(buffer, buffer, sem).wait()

    for load in scalars:
        load.wait()

    row_shape = (pairs, rows)
    smaller = jnp.zeros(row_shape, jnp.int32)
    for p in range(pairs):
        smaller = jnp.where(iota(row_shape, 0) == p, slots_s[me * pairs + p], smaller)
    k = iota(row_shape, 1)
    upper = k >= modes - smaller
    degree = jnp.where(upper, k - 1, smaller + k).astype(F32)
    orders = jnp.where(upper, modes - 1 - smaller, smaller).astype(F32)
    eps = raising(degree, orders)
    upper_f = jnp.where(upper, 1.0, 0.0)
    lower_f = 1.0 - upper_f

    colat = jnp.zeros((cycles, LANES), F32)
    for r in range(cycles):
        colat = jnp.where(iota(colat.shape, 0) == r, colat_s[r], colat)
    csc = 1.0 / jnp.sin(colat)
    cot = jnp.cos(colat) * csc
    lane_group = mod(div(iota(colat.shape, 1), comps), 4)
    base = jnp.where(lane_group == 0, 1.0, jnp.where(lane_group == 1, cot, csc))

    halves = [
        [jnp.broadcast_to(part[p : p + 1], (cycles, rows)).astype(BF16) for part in (lower_f, upper_f)]
        for p in range(pairs)
    ]

    for load in blocks:
        load.wait()

    @pl.when(is_worker)
    def _():
        for load in tables:
            load.start()

    @pl.when(jnp.logical_not(is_worker))
    def _():
        pl.semaphore_wait(barrier, work)
        send_m[...] = mask_ref[...].astype(F32).astype(BF16)
        turn = lax.rem(me, 2) + 2 * lax.div(me, 2 * work)
        remote(send_m, recv_m.at[turn], 3, 2 * lax.div(lax.rem(me, 2 * work), 2) + 1).start()

    lane = iota((8, LANES), 1)
    lane_quad = div(lane, 4 * comps)
    is_phi = mod(div(lane, comps), 4) == 2
    for g in range(groups):
        sets, legs = [], []
        small = jnp.zeros((8, LANES), jnp.int32)
        for q in range(quad):
            p = g * quad + q
            small = jnp.where(lane_quad == q, slots_s[me * pairs + p], small)
            tbar = jnp.concatenate([tbar_ref[p, s].astype(F32) for s in range(sims)], axis=0)
            twf = jnp.concatenate([twf_ref[p, s].astype(F32) for s in range(sims)], axis=0)
            deg_p, eps_p = degree[p : p + 1] / modes, eps[p : p + 1] / modes
            scaled = -(eps_p * twf)
            raised = jnp.concatenate([scaled[:, 1:], jnp.zeros_like(scaled[:, :1])], axis=1)
            sets += [tbar, deg_p * twf, twf, raised]
            legs += [leg_ref[p] * part for part in halves[p]]
        legs = jnp.concatenate(legs, axis=0)
        leg_all[pl.ds(g * quad * span, quad * span), :] = legs
        out = dot_t(legs, jnp.concatenate(sets, axis=0).astype(BF16))
        picked = out[:span]
        for q in range(1, quad):
            own = div(iota(picked.shape, 1), 4 * comps) == q
            picked = jnp.where(own, out[q * span : (q + 1) * span], picked)
        for h in range(2):
            order = (modes - 1 - small if h else small)[0:1]
            norm = jnp.where(order == 0, 1.0, 2.0) * modes ** (-0.5)
            norm = jnp.where(is_phi[0:1], norm * (order.astype(F32) / modes), norm)
            fs_ref[pl.ds((2 * g + h) * cycles, cycles), :] = picked[h * cycles : (h + 1) * cycles] * (base * norm)

    for t in range(TURNS):
        for w in range(work):
            send_f[t, w] = fs_ref[pl.ds(cycle_s[slot_of(w, t)], gh, stride=cycles), :].astype(BF16)

    @pl.when(is_worker)
    def _():
        pl.semaphore_wait(barrier, work - 1)

    tardy = lax.div(me, prompt)
    for w in reversed(range(work)):
        @pl.when(me != 2 * w + 1)
        def _():
            remote(send_f.at[:, w], recv_f.at[:, me], tardy, 2 * w + 1).start()

    lane_shape = (8, LANES)
    keep_lane = iota(lane_shape, 1)
    lane_seat = mod(div(keep_lane, gh), TURNS * work)
    theta_l = jnp.zeros(lane_shape, F32)
    weight_l = jnp.zeros(lane_shape, F32)
    place_shape = (LANES, total)
    place_row, place_lane = iota(place_shape, 0), iota(place_shape, 1)
    row_seat = mod(div(place_row, gh), TURNS * work)
    row_cycle = jnp.zeros(place_shape, jnp.int32)
    for t in range(TURNS):
        for w in range(work):
            r = cycle_s[slot_of(w, t)]
            at = t * work + w
            theta_l = jnp.where(lane_seat == at, colat_s[r], theta_l)
            weight_l = jnp.where(lane_seat == at, weight_s[r], weight_l)
            row_cycle = jnp.where(row_seat == at, r, row_cycle)
    with_sin = weight_l / jnp.sin(theta_l)
    with_cos = weight_l * jnp.cos(theta_l) / jnp.sin(theta_l)
    lane_g, lane_side = mod(div(keep_lane, 2), groups), div(keep_lane, LANES // 2)
    for p in range(pairs):
        mine = jnp.logical_and(lane_g == p // quad, lane_side == p % 2)
        keep_ref[p, 0] = jnp.where(mine, with_cos, 0.0)
        keep_ref[p, 1] = jnp.where(mine, with_sin, 0.0)
    for p in range(pairs):
        leg = leg_ref[p].astype(F32)
        prev = jnp.concatenate([jnp.zeros_like(leg[:, :1]), leg[:, : rows - 1]], axis=1)
        low, high = lower_f[p : p + 1], upper_f[p : p + 1]
        prev_all[pl.ds(p * span, span), :] = jnp.concatenate(
            [prev * low, prev * high], axis=0
        ).astype(BF16)
    row_pair = mod(div(place_row, 2), groups) * quad + div(place_row, LANES // 2)
    match = jnp.logical_and(
        row_cycle == mod(place_lane, cycles), mod(place_row, 2) == mod(div(place_lane, cycles), 2)
    )
    scale = (modes / cycles) ** 0.5 / jnp.sqrt(jnp.maximum(degree * (degree + 1.0), 1.0))
    kinds = [degree * scale, -(eps * scale), orders * scale]
    even = mod(div(iota((LANES // 2, rows), 0), 2), groups) == 0
    for k in range(quad // 2):
        place = one_hot(jnp.logical_and(match, row_pair + 2 * k == div(place_lane, span)))
        moved_leg = dot(place, leg_all[...])
        moved_prev = dot(place, prev_all[...])
        for at, (kind, moved) in enumerate(zip(kinds, (moved_leg, moved_prev, moved_leg))):
            for side in range(2):
                p = 2 * k + side
                factor = jnp.where(even, kind[p : p + 1], kind[quad + p : quad + p + 1])
                piece = moved[side * LANES // 2 : (side + 1) * LANES // 2] * factor
                fold_ref[k, pl.ds(at * LANES + side * LANES // 2, LANES // 2), :] = piece.astype(BF16)

    @pl.when(is_worker)
    def _():
        for load in tables:
            load.wait()
        pair_count = slots_v.shape[1]

        ahead = prompt * gh

        def pair_of(at):
            behind = at >= quad * ahead
            rest = at - quad * ahead
            early = (at * (65536 // ahead + 1)) >> 16
            q = jnp.where(behind, div(rest, (n - prompt) * gh), early)
            inner = jnp.where(behind, ahead + mod(rest, (n - prompt) * gh), at - ahead * early)
            return div(inner, gh) * pairs + div(mod(inner, gh), 2) * quad + q

        slots = jnp.broadcast_to(slots_v[...], (pair_count, pair_count)).astype(F32).astype(BF16)
        spread = one_hot(iota((pair_count, count), 0) == pair_of(iota((pair_count, count), 1)))
        spread_t = one_hot(iota((count, pair_count), 1) == pair_of(iota((count, pair_count), 0)))
        by_lane = dot(slots[:16], spread)[0:8]
        by_lane = jnp.where(mod(iota(by_lane.shape, 1), 2) == 1, modes - 1.0 - by_lane, by_lane)
        by_row = dot_t(spread_t, slots)
        by_row = jnp.where(mod(iota(by_row.shape, 0), 2) == 1, modes - 1.0 - by_row, by_row)
        select = one_hot(iota((modes, count), 0).astype(F32) == by_lane[0:1])
        select_t = jnp.concatenate(
            [
                one_hot((iota(by_row.shape, 1) + at).astype(F32) == by_row)
                for at in range(0, modes, pair_count)
            ],
            axis=1,
        )
        moved = dot(pixel_v[...], select).astype(BF16)
        cut_at = quad * ahead
        synth_ref[...] = jnp.concatenate([moved[:fine, :cut_at], moved[fine:, :cut_at]], axis=1)
        synth_l[...] = jnp.concatenate([moved[:fine, cut_at:], moved[fine:, cut_at:]], axis=1)
        moved = dot(select_t, mode_v[...])
        anal_ref[:count] = moved[:, :fine].astype(BF16)
        anal_ref[count:] = moved[:, fine : 2 * fine].astype(BF16)
        anal_c[...] = jnp.concatenate(
            [
                moved[q * ahead : q * ahead + first, part * fine : (part + 1) * fine]
                for part in range(2)
                for q in range(quad)
            ],
            axis=0,
        ).astype(BF16)
        at = 2 * fine
        for part in range(2):
            high_ref[part] = moved[:, at : at + LANES] + moved[:, at + LANES : at + 2 * LANES]
            at += 2 * LANES

        recv_f[:, me] = send_f[:, seat]
        cut = fine // LANES
        grid = (TURNS * mask_ref.shape[0], LANES)
        m_turn = div(iota(grid, 1), LANES // 2)
        m_high = mod(div(iota(grid, 1), sims), high_count)
        for j in range(TURNS // 2):
            first_row = ((m_turn + 2 * j) * high_count + m_high) * cut
            for at in range(cut):
                pick_ref[j, at] = one_hot(iota(grid, 0) == first_row + at)
        recv_m[1] = mask_ref[...].astype(F32).astype(BF16)
        quarter = mod(div(iota((8, 2 * LANES), 1), 4 * comps), quad)[0:1]

        def turn_up(sources, rows_at, size):
            turns = [
                recv_f[t, pl.ds(sources, size // quad // gh)].reshape(size // quad, LANES)
                for t in range(TURNS)
            ]
            pairs_of = [
                jnp.concatenate(turns[2 * j : 2 * j + 2], axis=1) for j in range(TURNS // 2)
            ]
            got = [pair * one_hot(quarter == q) for pair in pairs_of for q in range(quad)]
            spread_f = dot(jnp.concatenate(got, axis=0), spread_v[...])
            cos_h, sin_h = high_ref[0, pl.ds(rows_at, size)], high_ref[1, pl.ds(rows_at, size)]
            real, imag = [], []
            for j in range(TURNS // 2):
                for kind in range(2):
                    at = 2 * kind * LANES
                    re = spread_f[j * size : (j + 1) * size, at : at + LANES]
                    im = spread_f[j * size : (j + 1) * size, at + LANES : at + 2 * LANES]
                    real.append((re * cos_h - im * sin_h).astype(BF16))
                    imag.append((re * sin_h + im * cos_h).astype(BF16))
            return jnp.concatenate(
                [jnp.concatenate(real, axis=1), jnp.concatenate(imag, axis=1)], axis=0
            )

        settle(recv_f.at[:, pl.ds(0, prompt - 1)], 0)
        maps_ref[...] = dot(synth_ref[...], turn_up(0, 0, cut_at))
        settle(recv_m.at[pl.ds(0, TURNS - 1)], 3)
        both = recv_m[...].astype(F32).reshape(TURNS * mask_ref.shape[0], LANES)
        both_t = both.T.astype(BF16)
        for j in range(TURNS // 2):
            for at in range(cut):
                pixmask_ref[j, pl.ds(at * LANES, LANES), :] = dot(both_t, pick_ref[j, at])
        settle(recv_f.at[:, pl.ds(0, n - prompt)], 1)
        maps = maps_ref[...] + dot(synth_l[...], turn_up(prompt, cut_at, count - cut_at))
        products = jnp.concatenate(
            [
                pixmask_ref[j]
                * maps[:, 2 * j * LANES : (2 * j + 1) * LANES]
                * maps[:, (2 * j + 1) * LANES : (2 * j + 2) * LANES]
                for j in range(TURNS // 2)
            ],
            axis=1,
        ).astype(BF16)
        def bring_down(table, cos_h, sin_h, split):
            size = cos_h.shape[0]
            half = dot(table, products)
            parts = []
            for q in range(2):
                c_part = half[:size, q * LANES : (q + 1) * LANES]
                s_part = half[size:, q * LANES : (q + 1) * LANES]
                parts.append((cos_h * c_part + sin_h * s_part).astype(BF16))
                parts.append((cos_h * s_part - sin_h * c_part).astype(BF16))
            parts = jnp.concatenate(parts, axis=1)
            if not split:
                return dot(parts, gather_v[:, LANES:]) * pixels ** (-0.5)
            lane = iota((8, 4 * LANES), 1)
            turn = (2 * div(lane, 2 * LANES) + mod(div(lane, LANES // 2), 2))[0:1]
            parts = jnp.concatenate([parts * one_hot(turn == t) for t in range(TURNS)], axis=0)
            return dot(parts, gather_v[:, :LANES]) * pixels ** (-0.5)

        def pack(blocks):
            lane_quad = div(iota(blocks[0].shape, 1), 4 * comps)
            whole = blocks[0]
            for q in range(1, quad):
                whole = jnp.where(lane_quad == q, blocks[q], whole)
            return whole.astype(BF16).reshape(whole.shape[0] // gh, gh, LANES)

        high_c = [
            jnp.concatenate([high_ref[part, pl.ds(q * ahead, first)] for q in range(quad)], axis=0)
            for part in range(2)
        ]
        spectra = bring_down(anal_c[...], *high_c, True)
        for t in range(TURNS):
            at = t * quad * first
            send_p[t, pl.ds(0, 2)] = pack(
                [spectra[at + q * first : at + (q + 1) * first] for q in range(quad)]
            )
        remote(send_p.at[:, 0], recv_p.at[:, seat], 2, 0).start()

        @pl.when(me != 1)
        def _():
            remote(send_p.at[:, 1], recv_p.at[:, seat], 2, 1).start()

        spectra = bring_down(anal_ref[...], high_ref[0], high_ref[1], False)
        behind = n - prompt
        rest = [
            jnp.concatenate(
                [
                    spectra[q * ahead + first : (q + 1) * ahead],
                    spectra[cut_at + q * behind * gh : cut_at + (q + 1) * behind * gh],
                ],
                axis=0,
            )
            for q in range(quad)
        ]
        for t in range(TURNS):
            send_p[t, pl.ds(2, n - 2)] = pack(
                [
                    rest[q] if q == t else pltpu.roll(rest[q], (q - t) * 4 * comps % LANES, 1)
                    for q in range(quad)
                ]
            )
        for d in range(2, n):
            if d % 2 == 0 or d >= 2 * work:
                remote(send_p.at[:, d], recv_p.at[:, seat], 2, d).start()
            else:
                @pl.when(me != d)
                def _():
                    remote(send_p.at[:, d], recv_p.at[:, seat], 2, d).start()
        recv_p[:, seat] = send_p[:, me]
        settle(recv_p.at[:, pl.ds(0, work - 1)], 2)

    @pl.when(jnp.logical_not(is_worker))
    def _():
        settle(recv_p, 2)

    came = recv_p[...].astype(F32).reshape(TURNS * work * gh, LANES)
    came = jnp.concatenate([came, came], axis=0).T
    made = {}
    for k in range(quad // 2):
        members = [p for p in range(pairs) if p % quad // 2 == k]
        columns = [[], [], []]
        for p in members:
            at = p % quad * 4 * comps
            four = [came[at + g * comps : at + (g + 1) * comps] for g in range(4)]
            with_cos, with_sin = keep_ref[p, 0], keep_ref[p, 1]
            columns[0] += [four[0] * with_cos, four[1] * with_cos]
            columns[1] += [four[0] * with_sin, four[1] * with_sin]
            columns[2] += [four[2] * with_sin, four[3] * with_sin]
        stacked = [jnp.concatenate(column, axis=0).astype(BF16) for column in columns]
        out = dot(jnp.concatenate(stacked, axis=1), fold_ref[k])
        for at, p in enumerate(members):
            made[p] = out[at * 2 * comps : (at + 1) * 2 * comps]
    for p in range(pairs):
        grad, curl = made[p][:comps], made[p][comps:]
        for s in range(sims):
            grad_ref[p, s] = grad[2 * s : 2 * s + 2]
            curl_ref[p, s] = curl[2 * s : 2 * s + 2]

    @pl.when(is_worker)
    def _():
        settle(send_f.at[:, pl.ds(0, work - 1)], None)
        settle(send_p.at[:, pl.ds(0, n - 1)], None)

    @pl.when(jnp.logical_not(is_worker))
    def _():
        settle(send_f, None)
        settle(send_m, None)


def store_kernel(grad_ref, curl_ref, grad_hbm, curl_hbm, sem):
    copies = [
        pltpu.make_async_copy(grad_ref, grad_hbm, sem),
        pltpu.make_async_copy(curl_ref, curl_hbm, sem),
    ]
    for copy in copies:
        copy.start()
    for copy in copies:
        copy.wait()


def fused(tbar_alm, twf_alm, legendre, m_slots, cycle_order, colatitude, cycle_weight, pixel_mask, n):
    pairs, sims, _, rows = tbar_alm.shape
    modes = rows - 1
    cycles = legendre.shape[2]
    pixels = pixel_mask.shape[1]
    total = pairs * 2 * cycles
    count = n * 2 * pairs
    work = n // TURNS
    gh = 2 * pairs * 8 * sims // LANES
    fine = pixels * TURNS * sims // LANES
    by_cycle = jnp.transpose(legendre, (0, 2, 1))
    by_pixel, by_mode = split_tables(modes, pixels, sims)
    tables = [jnp.asarray(x) for x in (by_pixel, by_mode, spread_table(sims), gather_table(sims))]
    vmem, anywhere = pl.BlockSpec(memory_space=pltpu.VMEM), pl.BlockSpec(memory_space=pl.ANY)
    out = pltpu.VMEM(tbar_alm.shape, F32)
    mask_shape = (pixels // LANES, LANES)
    made = pl.pallas_call(
        functools.partial(fused_kernel, n, modes, rows, cycles, pixels, sims),
        out_shape=(out, out),
        in_specs=[anywhere] * 13,
        out_specs=(vmem, vmem),
        scratch_shapes=[
            pltpu.SMEM(m_slots.shape, jnp.int32),
            pltpu.SMEM(cycle_order.shape, jnp.int32),
            pltpu.SMEM(colatitude.shape, F32),
            pltpu.SMEM(cycle_weight.shape, F32),
            pltpu.VMEM((1, m_slots.shape[0]), jnp.int32),
            pltpu.VMEM(tbar_alm.shape, BF16),
            pltpu.VMEM(twf_alm.shape, BF16),
            pltpu.VMEM(by_cycle.shape, BF16),
            pltpu.VMEM(mask_shape, jnp.int32),
        ]
        + [pltpu.VMEM(table.shape, BF16) for table in tables]
        + [
            pltpu.VMEM((total, rows), BF16),
            pltpu.VMEM((total, rows), BF16),
            pltpu.VMEM((total // LANES, 3 * LANES, rows), BF16),
            pltpu.VMEM((gh * cycles, LANES), F32),
            pltpu.VMEM((pairs, 2, 8, LANES), F32),
            pltpu.VMEM((fine, 2 * count - count // 2), BF16),
            pltpu.VMEM((fine, count // 2), BF16),
            pltpu.VMEM((2 * count, fine), BF16),
            pltpu.VMEM((count // 4, fine), BF16),
            pltpu.VMEM((2, count, LANES), F32),
            pltpu.VMEM((TURNS // 2, fine, LANES), F32),
            pltpu.VMEM((fine, 4 * LANES), F32),
            pltpu.VMEM((TURNS // 2, fine // LANES, TURNS * mask_shape[0], LANES), BF16),
            pltpu.VMEM(mask_shape, BF16),
            pltpu.VMEM((TURNS,) + mask_shape, BF16),
            pltpu.VMEM((TURNS, work, gh, LANES), BF16),
            pltpu.VMEM((TURNS, n, gh, LANES), BF16),
            pltpu.VMEM((TURNS, n, gh, LANES), BF16),
            pltpu.VMEM((TURNS, work, gh, LANES), BF16),
            pltpu.SemaphoreType.DMA((2,)),
            pltpu.SemaphoreType.DMA((4,)),
        ],
        compiler_params=pltpu.CompilerParams(collective_id=0, has_side_effects=True),
        name="estimator",
    )(
        m_slots, cycle_order, colatitude, cycle_weight, m_slots.reshape(1, -1), tbar_alm,
        twf_alm, by_cycle, pixel_mask.reshape(mask_shape), *tables,
    )
    return pl.pallas_call(
        store_kernel,
        out_shape=(jax.ShapeDtypeStruct(tbar_alm.shape, F32),) * 2,
        in_specs=[vmem] * 2,
        out_specs=[anywhere] * 2,
        scratch_shapes=[pltpu.SemaphoreType.DMA],
        name="store",
    )(*(pltpu.with_memory_space_constraint(x, pltpu.VMEM) for x in made))


def body(n, *args):
    tbar_alm, legendre, pixel_mask = args[0], args[2], args[7]
    pairs, sims, _, rows = tbar_alm.shape
    cycles = legendre.shape[2]
    pixels = pixel_mask.shape[1]
    fits = (
        pairs == 8
        and cycles == n == 16
        and pixel_mask.shape[0] == 1
        and rows == 257
        and pairs * n == LANES
        and sims == 4
        and pixels == 4096
    )
    return fused(*args, n) if fits else shards(*args)


def solution(mesh):
    return jax.shard_map(
        functools.partial(body, mesh.shape["ma"]),
        mesh=mesh,
        in_specs=(
            P("ma", "grp", None, None),
            P("ma", "grp", None, None),
            P("ma", None, None),
            P(),
            P(),
            P(),
            P(),
            P("ma", None),
        ),
        out_specs=(P("ma", "grp", None, None), P("ma", "grp", None, None)),
        check_vma=False,
    )
```

```python
import math

import functools

import jax
import jax.numpy as jnp
import numpy as np
from jax import lax
from jax.experimental import pallas as pl
from jax.experimental.pallas import tpu as pltpu
from jax.sharding import PartitionSpec as P


def pair_layout(small_orders, mode_count):
    row_index = lax.broadcasted_iota(jnp.int32, (small_orders.shape[0], mode_count + 1), 1)
    smaller = small_orders[:, None]
    upper_half = row_index >= mode_count - smaller
    degree = jnp.where(upper_half, row_index - 1, smaller + row_index)
    orders = jnp.where(upper_half, mode_count - 1 - smaller, smaller + 0 * row_index)
    return (upper_half, degree.astype(jnp.float32), orders.astype(jnp.float32))


def raising(degree, orders):
    square = (
        (degree * degree - orders * orders)
        * (2.0 * degree + 1.0)
        / jnp.maximum(2.0 * degree - 1.0, 1.0)
    )
    return jnp.where(degree > orders, jnp.sqrt(jnp.where(degree > orders, square, 0.0)), 0.0)


def synthesis_sets(tbar_alm, twf_alm, degree, raising_factor, mode_count):
    wiener = twf_alm.astype(jnp.float32)
    scaled = (raising_factor / mode_count)[:, None, None, :] * wiener
    raised = jnp.concatenate([scaled[..., 1:], jnp.zeros_like(scaled[..., :1])], axis=-1)
    stacked = jnp.stack(
        [
            tbar_alm.astype(jnp.float32),
            wiener,
            (degree / mode_count)[:, None, None, :] * wiener,
            raised,
        ],
        axis=2,
    )
    return stacked.reshape(stacked.shape[0], stacked.shape[1], 8, stacked.shape[4]).astype(
        jnp.bfloat16
    )


def mode_columns(small_orders, mode_count):
    return jnp.stack([small_orders, mode_count - 1 - small_orders], axis=1).reshape(-1)


def fourier_table(orders_int, pixel_count):
    pixel_index = lax.broadcasted_iota(jnp.int32, (orders_int.shape[0], pixel_count), 1)
    turns = orders_int[:, None] * pixel_index % pixel_count
    radians = turns.astype(jnp.float32) * (2.0 * math.pi / pixel_count)
    return jnp.stack([jnp.cos(radians), -jnp.sin(radians)], axis=0).astype(jnp.bfloat16)


def combine_modes(legendre_sums, orders_int, cos_cycle, sin_cycle, mode_count):
    orders_real = orders_int.astype(jnp.float32)
    inv_sin = 1.0 / sin_cycle
    ratio = (orders_real / mode_count)[:, None]
    theta_real = (cos_cycle * legendre_sums[:, 4] - legendre_sums[:, 6]) * inv_sin
    theta_imag = (cos_cycle * legendre_sums[:, 5] - legendre_sums[:, 7]) * inv_sin
    phi_real = -ratio * legendre_sums[:, 3] * inv_sin
    phi_imag = ratio * legendre_sums[:, 2] * inv_sin
    weight = (jnp.where(orders_int == 0, 1.0, 2.0) * mode_count ** (-0.5))[:, None]
    stacked = jnp.stack(
        [legendre_sums[:, 0], legendre_sums[:, 1], theta_real, theta_imag, phi_real, phi_imag],
        axis=1,
    )
    return (stacked * weight).astype(jnp.bfloat16)


def analysis_sets(spectra, colatitude, cycle_weight):
    with_cos = cycle_weight * jnp.cos(colatitude) / jnp.sin(colatitude)
    with_sin = cycle_weight / jnp.sin(colatitude)
    stacked = jnp.stack(
        [
            spectra[:, 0] * with_cos,
            spectra[:, 0] * with_sin,
            spectra[:, 1] * with_cos,
            spectra[:, 1] * with_sin,
        ],
        axis=1,
    )
    return stacked.reshape(spectra.shape[0], 8, spectra.shape[3], spectra.shape[4]).astype(
        jnp.bfloat16
    )


def estimate(merged, degree, orders, raising_factor, mode_count, cycle_count):
    level = degree[:, None, :]
    azimuth = orders[:, None, :]
    factor = raising_factor[:, None, :]

    def previous(values):
        return jnp.concatenate([jnp.zeros_like(values[..., :1]), values[..., :-1]], axis=-1)

    grad_real = (
        level * merged[:, :, 0] - factor * previous(merged[:, :, 2]) + azimuth * merged[:, :, 7]
    )
    grad_imag = (
        level * merged[:, :, 1] - factor * previous(merged[:, :, 3]) - azimuth * merged[:, :, 6]
    )
    curl_real = (
        level * merged[:, :, 4] - factor * previous(merged[:, :, 6]) - azimuth * merged[:, :, 3]
    )
    curl_imag = (
        level * merged[:, :, 5] - factor * previous(merged[:, :, 7]) + azimuth * merged[:, :, 2]
    )
    scale = (mode_count / cycle_count) ** 0.5 / jnp.sqrt(jnp.maximum(level * (level + 1.0), 1.0))
    scale = scale[:, :, None, :]
    return (
        jnp.stack([grad_real, grad_imag], axis=2) * scale,
        jnp.stack([curl_real, curl_imag], axis=2) * scale,
    )


def shards(tbar_alm, twf_alm, legendre, m_slots, cycle_order, colatitude, cycle_weight, pixel_mask):
    pairs_dev = tbar_alm.shape[0]
    row_count = tbar_alm.shape[3]
    mode_count = row_count - 1
    cycle_count = legendre.shape[2]
    cycle_dev = pixel_mask.shape[0]
    pixel_count = pixel_mask.shape[1]
    device_slot = lax.axis_index("ma")
    local_small = lax.dynamic_slice_in_dim(m_slots, device_slot * pairs_dev, pairs_dev)
    upper_half, degree, orders = pair_layout(local_small, mode_count)
    raising_factor = raising(degree, orders)
    coeff_sets = synthesis_sets(tbar_alm, twf_alm, degree, raising_factor, mode_count)
    halves = jnp.stack([jnp.logical_not(upper_half), upper_half], axis=1)
    masked = coeff_sets[:, None] * halves.astype(jnp.bfloat16)[:, :, None, None, :]
    legendre_sums = jnp.einsum(
        "phsck,pkr->scphr", masked, legendre, preferred_element_type=jnp.float32
    )
    legendre_sums = jnp.take(legendre_sums, cycle_order, axis=4)
    legendre_sums = legendre_sums.reshape(legendre_sums.shape[0], 8, 2 * pairs_dev, cycle_count)
    all_orders = mode_columns(m_slots, mode_count)
    dft_table = fourier_table(all_orders, pixel_count)
    pixel_weights = pixel_mask.astype(jnp.float32)
    slot_theta = jnp.take(colatitude, cycle_order)
    local_orders = mode_columns(local_small, mode_count)
    outgoing = combine_modes(
        legendre_sums, local_orders, jnp.cos(slot_theta), jnp.sin(slot_theta), mode_count
    )
    fourier = lax.all_to_all(outgoing, "ma", split_axis=3, concat_axis=2, tiled=True)
    fourier = fourier.reshape(fourier.shape[0], 3, 2, mode_count, cycle_dev)
    cycle_maps = jnp.einsum(
        "sqemr,emj->sqrj", fourier, dft_table, preferred_element_type=jnp.float32
    )
    products = (pixel_weights * cycle_maps[:, 0:1] * cycle_maps[:, 1:3]).astype(jnp.bfloat16)
    spectra = jnp.einsum("sqrj,emj->sqemr", products, dft_table, preferred_element_type=jnp.float32)
    received = (spectra * pixel_count ** (-0.5)).astype(jnp.bfloat16)
    returned = lax.all_to_all(received, "ma", split_axis=3, concat_axis=4, tiled=True)
    inverse = (
        jnp.zeros((cycle_count,), jnp.int32).at[cycle_order].set(lax.iota(jnp.int32, cycle_count))
    )
    spectra = jnp.take(returned, inverse, axis=4).astype(jnp.float32)
    weighted = analysis_sets(spectra, colatitude, cycle_weight)
    weighted = weighted.reshape(weighted.shape[0], 8, pairs_dev, 2, cycle_count)
    projected = jnp.einsum(
        "scphr,pkr->phsck", weighted, legendre, preferred_element_type=jnp.float32
    )
    merged = jnp.sum(projected * halves.astype(jnp.float32)[:, :, None, None, :], axis=1)
    return estimate(merged, degree, orders, raising_factor, mode_count, cycle_count)


LANES = 128
TURNS = 4
F32 = jnp.float32
BF16 = jnp.bfloat16


def split_tables(mode_count, pixel_count, sims):
    high_count = LANES // (TURNS * sims)
    low_count = pixel_count // high_count
    m = np.arange(mode_count)[:, None]
    low = np.arange(low_count)[None, :]
    high = (np.arange(LANES) // sims % high_count)[None, :] * low_count
    fine = (m * low % pixel_count) * (2.0 * math.pi / pixel_count)
    coarse = (m * high % pixel_count) * (2.0 * math.pi / pixel_count)

    def halves(values):
        upper = values.astype(np.float32).astype(BF16)
        return [upper, (values.astype(np.float32) - upper.astype(np.float32)).astype(BF16)]

    waves = [np.cos(fine).astype(BF16), (-np.sin(fine)).astype(BF16)]
    by_pixel = np.concatenate([wave.T for wave in waves], axis=0)
    by_mode = np.concatenate(waves + halves(np.cos(coarse)) + halves(np.sin(coarse)), axis=1)
    return by_pixel, by_mode


def spread_table(sims):
    comps = 2 * sims
    row = np.arange(2 * LANES)[:, None]
    col = np.arange(4 * LANES)[None, :]
    row_t, row_g, row_s, row_c = row // LANES, row // comps % 4, row // 2 % sims, row % 2
    col_t, col_s, col_c = col // (LANES // 2) % 2, col % sims, col // LANES % 2
    col_q = np.where(col < 2 * LANES, 0, 1 + col // (LANES // 4) % 2)
    group_q = np.array([0, 1, 2, 1])[row_g]
    source_c = np.where(col_q == 2, 1 - col_c, col_c)
    sign = np.where((col_q == 2) & (col_c == 0), -1.0, 1.0)
    hit = (row_t == col_t) & (row_s == col_s) & (group_q == col_q) & (row_c == source_c)
    return np.where(hit, sign, 0.0).astype(BF16)


def gather_table(sims):
    comps = 2 * sims
    row = np.arange(4 * LANES)[:, None]
    col = np.arange(LANES)[None, :]
    group, part = col // comps % 4, col % 2
    want_q = np.where((group == 1) | (group == 2), 1, 0)
    want_c = np.where(group >= 2, 1 - part, part)
    sign = np.where(((group == 2) & (part == 1)) | ((group == 3) & (part == 0)), -1.0, 1.0)
    hit = (row // (LANES // 4) % 2 == want_q) & (row // LANES % 2 == want_c)
    hit &= row % sims == col // 2 % sims
    turn = 2 * (row // (2 * LANES)) + row // (LANES // 2) % 2
    own = hit & (turn == col // (4 * comps))
    return np.concatenate([np.where(x, sign, 0.0) for x in (hit, own)], axis=1).astype(BF16)


def iota(shape, axis):
    return lax.broadcasted_iota(jnp.int32, shape, axis)


def div(values, size):
    return values >> (size.bit_length() - 1)


def mod(values, size):
    return values & (size - 1)


def one_hot(condition):
    return jnp.where(condition, 1.0, 0.0).astype(BF16)


def dot(left, right):
    return jnp.dot(left, right, preferred_element_type=F32)


def dot_t(left, right):
    return lax.dot_general(left, right, (((1,), (1,)), ((), ())), preferred_element_type=F32)


def fused_kernel(
    n, modes, rows, cycles, pixels, sims,
    slots_hbm, cycle_hbm, colat_hbm, weight_hbm, row_hbm, tbar_hbm, twf_hbm, leg_hbm, mask_hbm,
    pixel_hbm, mode_hbm, spread_hbm, gather_hbm,
    grad_ref, curl_ref,
    slots_s, cycle_s, colat_s, weight_s, slots_v, tbar_ref, twf_ref, leg_ref, mask_ref,
    pixel_v, mode_v, spread_v, gather_v,
    leg_all, prev_all, fold_ref, fs_ref, keep_ref, synth_ref, synth_l, anal_ref, anal_c, high_ref,
    pixmask_ref, maps_ref, pick_ref,
    send_m, recv_m, send_f, recv_f, send_p, recv_p, load_sem, move_sem,
):
    me = lax.axis_index("ma")
    work = n // TURNS
    pairs = tbar_ref.shape[0]
    comps = 2 * sims
    quad = LANES // (4 * comps)
    groups = pairs // quad
    span = 2 * cycles
    total = pairs * span
    count = n * 2 * pairs
    gh = 2 * groups
    high_count = LANES // (TURNS * sims)
    fine = pixels // high_count
    seat = lax.rem(lax.div(me, 2), work)
    prompt = n - n // 4
    first = 2 * gh
    is_worker = jnp.logical_and(lax.rem(me, 2) == 1, me < 2 * work)

    def slot_of(w, t):
        return 2 * w + t % 2 + t // 2 * 2 * work

    scalars = [(slots_hbm, slots_s), (colat_hbm, colat_s), (cycle_hbm, cycle_s), (weight_hbm, weight_s)]
    blocks = [(leg_hbm, leg_ref), (tbar_hbm, tbar_ref), (twf_hbm, twf_ref), (mask_hbm, mask_ref)]
    tables = [
        (row_hbm, slots_v), (mode_hbm, mode_v), (pixel_hbm, pixel_v), (spread_hbm, spread_v),
        (gather_hbm, gather_v),
    ]
    scalars, blocks, tables = [
        [pltpu.make_async_copy(source, target, load_sem.at[at]) for source, target in group]
        for at, group in ((0, scalars), (1, blocks), (1, tables))
    ]
    for load in blocks + scalars:
        load.start()
    barrier = pltpu.get_barrier_semaphore()

    @pl.when(is_worker)
    def _():
        for off in range(1, n):
            pl.semaphore_signal(
                barrier, inc=1, device_id={"ma": lax.rem(me + off, n)},
                device_id_type=pl.DeviceIdType.MESH,
            )


    def remote(source, target, at, to):
        return pltpu.make_async_remote_copy(
            src_ref=source, dst_ref=target, send_sem=load_sem.at[0],
            recv_sem=move_sem.at[at], device_id={"ma": to},
            device_id_type=pl.DeviceIdType.MESH,
        )

    def settle(buffer, at):
        sem = load_sem.at[0] if at is None else move_sem.at[at]
        pltpu.make_async_copy(buffer, buffer, sem).wait()

    for load in scalars:
        load.wait()

    row_shape = (pairs, rows)
    smaller = jnp.zeros(row_shape, jnp.int32)
    for p in range(pairs):
        smaller = jnp.where(iota(row_shape, 0) == p, slots_s[me * pairs + p], smaller)
    k = iota(row_shape, 1)
    upper = k >= modes - smaller
    degree = jnp.where(upper, k - 1, smaller + k).astype(F32)
    orders = jnp.where(upper, modes - 1 - smaller, smaller).astype(F32)
    eps = raising(degree, orders)
    upper_f = jnp.where(upper, 1.0, 0.0)
    lower_f = 1.0 - upper_f

    colat = jnp.zeros((cycles, LANES), F32)
    for r in range(cycles):
        colat = jnp.where(iota(colat.shape, 0) == r, colat_s[r], colat)
    csc = 1.0 / jnp.sin(colat)
    cot = jnp.cos(colat) * csc
    lane_group = mod(div(iota(colat.shape, 1), comps), 4)
    base = jnp.where(lane_group == 0, 1.0, jnp.where(lane_group == 1, cot, csc))

    halves = [
        [jnp.broadcast_to(part[p : p + 1], (cycles, rows)).astype(BF16) for part in (lower_f, upper_f)]
        for p in range(pairs)
    ]

    for load in blocks:
        load.wait()

    @pl.when(is_worker)
    def _():
        for load in tables:
            load.start()

    @pl.when(jnp.logical_not(is_worker))
    def _():
        pl.semaphore_wait(barrier, work)
        send_m[...] = mask_ref[...].astype(F32).astype(BF16)
        turn = lax.rem(me, 2) + 2 * lax.div(me, 2 * work)
        remote(send_m, recv_m.at[turn], 3, 2 * lax.div(lax.rem(me, 2 * work), 2) + 1).start()

    lane = iota((8, LANES), 1)
    lane_quad = div(lane, 4 * comps)
    is_phi = mod(div(lane, comps), 4) == 2
    for g in range(groups):
        sets, legs = [], []
        small = jnp.zeros((8, LANES), jnp.int32)
        for q in range(quad):
            p = g * quad + q
            small = jnp.where(lane_quad == q, slots_s[me * pairs + p], small)
            tbar = jnp.concatenate([tbar_ref[p, s].astype(F32) for s in range(sims)], axis=0)
            twf = jnp.concatenate([twf_ref[p, s].astype(F32) for s in range(sims)], axis=0)
            deg_p, eps_p = degree[p : p + 1] / modes, eps[p : p + 1] / modes
            scaled = -(eps_p * twf)
            raised = jnp.concatenate([scaled[:, 1:], jnp.zeros_like(scaled[:, :1])], axis=1)
            sets += [tbar, deg_p * twf, twf, raised]
            legs += [leg_ref[p] * part for part in halves[p]]
        legs = jnp.concatenate(legs, axis=0)
        leg_all[pl.ds(g * quad * span, quad * span), :] = legs
        out = dot_t(legs, jnp.concatenate(sets, axis=0).astype(BF16))
        picked = out[:span]
        for q in range(1, quad):
            own = div(iota(picked.shape, 1), 4 * comps) == q
            picked = jnp.where(own, out[q * span : (q + 1) * span], picked)
        for h in range(2):
            order = (modes - 1 - small if h else small)[0:1]
            norm = jnp.where(order == 0, 1.0, 2.0) * modes ** (-0.5)
            norm = jnp.where(is_phi[0:1], norm * (order.astype(F32) / modes), norm)
            fs_ref[pl.ds((2 * g + h) * cycles, cycles), :] = picked[h * cycles : (h + 1) * cycles] * (base * norm)

    for t in range(TURNS):
        for w in range(work):
            send_f[t, w] = fs_ref[pl.ds(cycle_s[slot_of(w, t)], gh, stride=cycles), :].astype(BF16)

    @pl.when(is_worker)
    def _():
        pl.semaphore_wait(barrier, work - 1)

    tardy = lax.div(me, prompt)
    for w in reversed(range(work)):
        @pl.when(me != 2 * w + 1)
        def _():
            remote(send_f.at[:, w], recv_f.at[:, me], tardy, 2 * w + 1).start()

    lane_shape = (8, LANES)
    keep_lane = iota(lane_shape, 1)
    lane_seat = mod(div(keep_lane, gh), TURNS * work)
    theta_l = jnp.zeros(lane_shape, F32)
    weight_l = jnp.zeros(lane_shape, F32)
    place_shape = (LANES, total)
    place_row, place_lane = iota(place_shape, 0), iota(place_shape, 1)
    row_seat = mod(div(place_row, gh), TURNS * work)
    row_cycle = jnp.zeros(place_shape, jnp.int32)
    for t in range(TURNS):
        for w in range(work):
            r = cycle_s[slot_of(w, t)]
            at = t * work + w
            theta_l = jnp.where(lane_seat == at, colat_s[r], theta_l)
            weight_l = jnp.where(lane_seat == at, weight_s[r], weight_l)
            row_cycle = jnp.where(row_seat == at, r, row_cycle)
    with_sin = weight_l / jnp.sin(theta_l)
    with_cos = weight_l * jnp.cos(theta_l) / jnp.sin(theta_l)
    lane_g, lane_side = mod(div(keep_lane, 2), groups), div(keep_lane, LANES // 2)
    for p in range(pairs):
        mine = jnp.logical_and(lane_g == p // quad, lane_side == p % 2)
        keep_ref[p, 0] = jnp.where(mine, with_cos, 0.0)
        keep_ref[p, 1] = jnp.where(mine, with_sin, 0.0)
    for p in range(pairs):
        leg = leg_ref[p].astype(F32)
        prev = jnp.concatenate([jnp.zeros_like(leg[:, :1]), leg[:, : rows - 1]], axis=1)
        low, high = lower_f[p : p + 1], upper_f[p : p + 1]
        prev_all[pl.ds(p * span, span), :] = jnp.concatenate(
            [prev * low, prev * high], axis=0
        ).astype(BF16)
    row_pair = mod(div(place_row, 2), groups) * quad + div(place_row, LANES // 2)
    match = jnp.logical_and(
        row_cycle == mod(place_lane, cycles), mod(place_row, 2) == mod(div(place_lane, cycles), 2)
    )
    scale = (modes / cycles) ** 0.5 / jnp.sqrt(jnp.maximum(degree * (degree + 1.0), 1.0))
    kinds = [degree * scale, -(eps * scale), orders * scale]
    even = mod(div(iota((LANES // 2, rows), 0), 2), groups) == 0
    for k in range(quad // 2):
        place = one_hot(jnp.logical_and(match, row_pair + 2 * k == div(place_lane, span)))
        moved_leg = dot(place, leg_all[...])
        moved_prev = dot(place, prev_all[...])
        for at, (kind, moved) in enumerate(zip(kinds, (moved_leg, moved_prev, moved_leg))):
            for side in range(2):
                p = 2 * k + side
                factor = jnp.where(even, kind[p : p + 1], kind[quad + p : quad + p + 1])
                piece = moved[side * LANES // 2 : (side + 1) * LANES // 2] * factor
                fold_ref[k, pl.ds(at * LANES + side * LANES // 2, LANES // 2), :] = piece.astype(BF16)

    @pl.when(is_worker)
    def _():
        for load in tables:
            load.wait()
        pair_count = slots_v.shape[1]

        ahead = prompt * gh

        def pair_of(at):
            behind = at >= quad * ahead
            rest = at - quad * ahead
            early = (at * (65536 // ahead + 1)) >> 16
            q = jnp.where(behind, div(rest, (n - prompt) * gh), early)
            inner = jnp.where(behind, ahead + mod(rest, (n - prompt) * gh), at - ahead * early)
            return div(inner, gh) * pairs + div(mod(inner, gh), 2) * quad + q

        slots = jnp.broadcast_to(slots_v[...], (pair_count, pair_count)).astype(F32).astype(BF16)
        spread = one_hot(iota((pair_count, count), 0) == pair_of(iota((pair_count, count), 1)))
        spread_t = one_hot(iota((count, pair_count), 1) == pair_of(iota((count, pair_count), 0)))
        by_lane = dot(slots[:16], spread)[0:8]
        by_lane = jnp.where(mod(iota(by_lane.shape, 1), 2) == 1, modes - 1.0 - by_lane, by_lane)
        by_row = dot_t(spread_t, slots)
        by_row = jnp.where(mod(iota(by_row.shape, 0), 2) == 1, modes - 1.0 - by_row, by_row)
        select = one_hot(iota((modes, count), 0).astype(F32) == by_lane[0:1])
        select_t = jnp.concatenate(
            [
                one_hot((iota(by_row.shape, 1) + at).astype(F32) == by_row)
                for at in range(0, modes, pair_count)
            ],
            axis=1,
        )
        moved = dot(pixel_v[...], select).astype(BF16)
        cut_at = quad * ahead
        synth_ref[...] = jnp.concatenate([moved[:fine, :cut_at], moved[fine:, :cut_at]], axis=1)
        synth_l[...] = jnp.concatenate([moved[:fine, cut_at:], moved[fine:, cut_at:]], axis=1)
        moved = dot(select_t, mode_v[...])
        anal_ref[:count] = moved[:, :fine].astype(BF16)
        anal_ref[count:] = moved[:, fine : 2 * fine].astype(BF16)
        anal_c[...] = jnp.concatenate(
            [
                moved[q * ahead : q * ahead + first, part * fine : (part + 1) * fine]
                for part in range(2)
                for q in range(quad)
            ],
            axis=0,
        ).astype(BF16)
        at = 2 * fine
        for part in range(2):
            high_ref[part] = moved[:, at : at + LANES] + moved[:, at + LANES : at + 2 * LANES]
            at += 2 * LANES

        recv_f[:, me] = send_f[:, seat]
        cut = fine // LANES
        grid = (TURNS * mask_ref.shape[0], LANES)
        m_turn = div(iota(grid, 1), LANES // 2)
        m_high = mod(div(iota(grid, 1), sims), high_count)
        for j in range(TURNS // 2):
            first_row = ((m_turn + 2 * j) * high_count + m_high) * cut
            for at in range(cut):
                pick_ref[j, at] = one_hot(iota(grid, 0) == first_row + at)
        recv_m[1] = mask_ref[...].astype(F32).astype(BF16)
        quarter = mod(div(iota((8, 2 * LANES), 1), 4 * comps), quad)[0:1]

        def turn_up(sources, rows_at, size):
            turns = [
                recv_f[t, pl.ds(sources, size // quad // gh)].reshape(size // quad, LANES)
                for t in range(TURNS)
            ]
            pairs_of = [
                jnp.concatenate(turns[2 * j : 2 * j + 2], axis=1) for j in range(TURNS // 2)
            ]
            got = [pair * one_hot(quarter == q) for pair in pairs_of for q in range(quad)]
            spread_f = dot(jnp.concatenate(got, axis=0), spread_v[...])
            cos_h, sin_h = high_ref[0, pl.ds(rows_at, size)], high_ref[1, pl.ds(rows_at, size)]
            real, imag = [], []
            for j in range(TURNS // 2):
                for kind in range(2):
                    at = 2 * kind * LANES
                    re = spread_f[j * size : (j + 1) * size, at : at + LANES]
                    im = spread_f[j * size : (j + 1) * size, at + LANES : at + 2 * LANES]
                    real.append((re * cos_h - im * sin_h).astype(BF16))
                    imag.append((re * sin_h + im * cos_h).astype(BF16))
            return jnp.concatenate(
                [jnp.concatenate(real, axis=1), jnp.concatenate(imag, axis=1)], axis=0
            )

        settle(recv_f.at[:, pl.ds(0, prompt - 1)], 0)
        maps_ref[...] = dot(synth_ref[...], turn_up(0, 0, cut_at))
        settle(recv_m.at[pl.ds(0, TURNS - 1)], 3)
        both = recv_m[...].astype(F32).reshape(TURNS * mask_ref.shape[0], LANES)
        both_t = both.T.astype(BF16)
        for j in range(TURNS // 2):
            for at in range(cut):
                pixmask_ref[j, pl.ds(at * LANES, LANES), :] = dot(both_t, pick_ref[j, at])
        settle(recv_f.at[:, pl.ds(0, n - prompt)], 1)
        maps = maps_ref[...] + dot(synth_l[...], turn_up(prompt, cut_at, count - cut_at))
        products = jnp.concatenate(
            [
                pixmask_ref[j]
                * maps[:, 2 * j * LANES : (2 * j + 1) * LANES]
                * maps[:, (2 * j + 1) * LANES : (2 * j + 2) * LANES]
                for j in range(TURNS // 2)
            ],
            axis=1,
        ).astype(BF16)
        def bring_down(table, cos_h, sin_h, split):
            size = cos_h.shape[0]
            half = dot(table, products)
            parts = []
            for q in range(2):
                c_part = half[:size, q * LANES : (q + 1) * LANES]
                s_part = half[size:, q * LANES : (q + 1) * LANES]
                parts.append((cos_h * c_part + sin_h * s_part).astype(BF16))
                parts.append((cos_h * s_part - sin_h * c_part).astype(BF16))
            parts = jnp.concatenate(parts, axis=1)
            if not split:
                return dot(parts, gather_v[:, LANES:]) * pixels ** (-0.5)
            lane = iota((8, 4 * LANES), 1)
            turn = (2 * div(lane, 2 * LANES) + mod(div(lane, LANES // 2), 2))[0:1]
            parts = jnp.concatenate([parts * one_hot(turn == t) for t in range(TURNS)], axis=0)
            return dot(parts, gather_v[:, :LANES]) * pixels ** (-0.5)

        def pack(blocks):
            lane_quad = div(iota(blocks[0].shape, 1), 4 * comps)
            whole = blocks[0]
            for q in range(1, quad):
                whole = jnp.where(lane_quad == q, blocks[q], whole)
            return whole.astype(BF16).reshape(whole.shape[0] // gh, gh, LANES)

        high_c = [
            jnp.concatenate([high_ref[part, pl.ds(q * ahead, first)] for q in range(quad)], axis=0)
            for part in range(2)
        ]
        spectra = bring_down(anal_c[...], *high_c, True)
        for t in range(TURNS):
            at = t * quad * first
            send_p[t, pl.ds(0, 2)] = pack(
                [spectra[at + q * first : at + (q + 1) * first] for q in range(quad)]
            )
        remote(send_p.at[:, 0], recv_p.at[:, seat], 2, 0).start()

        @pl.when(me != 1)
        def _():
            remote(send_p.at[:, 1], recv_p.at[:, seat], 2, 1).start()

        spectra = bring_down(anal_ref[...], high_ref[0], high_ref[1], False)
        behind = n - prompt
        rest = [
            jnp.concatenate(
                [
                    spectra[q * ahead + first : (q + 1) * ahead],
                    spectra[cut_at + q * behind * gh : cut_at + (q + 1) * behind * gh],
                ],
                axis=0,
            )
            for q in range(quad)
        ]
        for t in range(TURNS):
            send_p[t, pl.ds(2, n - 2)] = pack(
                [
                    rest[q] if q == t else pltpu.roll(rest[q], (q - t) * 4 * comps % LANES, 1)
                    for q in range(quad)
                ]
            )
        for d in range(2, n):
            if d % 2 == 0 or d >= 2 * work:
                remote(send_p.at[:, d], recv_p.at[:, seat], 2, d).start()
            else:
                @pl.when(me != d)
                def _():
                    remote(send_p.at[:, d], recv_p.at[:, seat], 2, d).start()
        recv_p[:, seat] = send_p[:, me]
        settle(recv_p.at[:, pl.ds(0, work - 1)], 2)

    @pl.when(jnp.logical_not(is_worker))
    def _():
        settle(send_f, None)
        settle(send_m, None)
        settle(recv_p, 2)

    came = recv_p[...].astype(F32).reshape(TURNS * work * gh, LANES)
    came = jnp.concatenate([came, came], axis=0).T
    made = {}
    for k in range(quad // 2):
        members = [p for p in range(pairs) if p % quad // 2 == k]
        columns = [[], [], []]
        for p in members:
            at = p % quad * 4 * comps
            four = [came[at + g * comps : at + (g + 1) * comps] for g in range(4)]
            with_cos, with_sin = keep_ref[p, 0], keep_ref[p, 1]
            columns[0] += [four[0] * with_cos, four[1] * with_cos]
            columns[1] += [four[0] * with_sin, four[1] * with_sin]
            columns[2] += [four[2] * with_sin, four[3] * with_sin]
        stacked = [jnp.concatenate(column, axis=0).astype(BF16) for column in columns]
        out = dot(jnp.concatenate(stacked, axis=1), fold_ref[k])
        for at, p in enumerate(members):
            made[p] = out[at * 2 * comps : (at + 1) * 2 * comps]
    for p in range(pairs):
        grad, curl = made[p][:comps], made[p][comps:]
        for s in range(sims):
            grad_ref[p, s] = grad[2 * s : 2 * s + 2]
            curl_ref[p, s] = curl[2 * s : 2 * s + 2]

    @pl.when(is_worker)
    def _():
        settle(send_f.at[:, pl.ds(0, work - 1)], None)
        settle(send_p.at[:, pl.ds(0, n - 1)], None)


def store_kernel(grad_ref, curl_ref, grad_hbm, curl_hbm, sem):
    copies = [
        pltpu.make_async_copy(grad_ref, grad_hbm, sem),
        pltpu.make_async_copy(curl_ref, curl_hbm, sem),
    ]
    for copy in copies:
        copy.start()
    for copy in copies:
        copy.wait()


def fused(tbar_alm, twf_alm, legendre, m_slots, cycle_order, colatitude, cycle_weight, pixel_mask, n):
    pairs, sims, _, rows = tbar_alm.shape
    modes = rows - 1
    cycles = legendre.shape[2]
    pixels = pixel_mask.shape[1]
    total = pairs * 2 * cycles
    count = n * 2 * pairs
    work = n // TURNS
    gh = 2 * pairs * 8 * sims // LANES
    fine = pixels * TURNS * sims // LANES
    by_cycle = jnp.transpose(legendre, (0, 2, 1))
    by_pixel, by_mode = split_tables(modes, pixels, sims)
    tables = [jnp.asarray(x) for x in (by_pixel, by_mode, spread_table(sims), gather_table(sims))]
    vmem, anywhere = pl.BlockSpec(memory_space=pltpu.VMEM), pl.BlockSpec(memory_space=pl.ANY)
    out = pltpu.VMEM(tbar_alm.shape, F32)
    mask_shape = (pixels // LANES, LANES)
    made = pl.pallas_call(
        functools.partial(fused_kernel, n, modes, rows, cycles, pixels, sims),
        out_shape=(out, out),
        in_specs=[anywhere] * 13,
        out_specs=(vmem, vmem),
        scratch_shapes=[
            pltpu.SMEM(m_slots.shape, jnp.int32),
            pltpu.SMEM(cycle_order.shape, jnp.int32),
            pltpu.SMEM(colatitude.shape, F32),
            pltpu.SMEM(cycle_weight.shape, F32),
            pltpu.VMEM((1, m_slots.shape[0]), jnp.int32),
            pltpu.VMEM(tbar_alm.shape, BF16),
            pltpu.VMEM(twf_alm.shape, BF16),
            pltpu.VMEM(by_cycle.shape, BF16),
            pltpu.VMEM(mask_shape, jnp.int32),
        ]
        + [pltpu.VMEM(table.shape, BF16) for table in tables]
        + [
            pltpu.VMEM((total, rows), BF16),
            pltpu.VMEM((total, rows), BF16),
            pltpu.VMEM((total // LANES, 3 * LANES, rows), BF16),
            pltpu.VMEM((gh * cycles, LANES), F32),
            pltpu.VMEM((pairs, 2, 8, LANES), F32),
            pltpu.VMEM((fine, 2 * count - count // 2), BF16),
            pltpu.VMEM((fine, count // 2), BF16),
            pltpu.VMEM((2 * count, fine), BF16),
            pltpu.VMEM((count // 4, fine), BF16),
            pltpu.VMEM((2, count, LANES), F32),
            pltpu.VMEM((TURNS // 2, fine, LANES), F32),
            pltpu.VMEM((fine, 4 * LANES), F32),
            pltpu.VMEM((TURNS // 2, fine // LANES, TURNS * mask_shape[0], LANES), BF16),
            pltpu.VMEM(mask_shape, BF16),
            pltpu.VMEM((TURNS,) + mask_shape, BF16),
            pltpu.VMEM((TURNS, work, gh, LANES), BF16),
            pltpu.VMEM((TURNS, n, gh, LANES), BF16),
            pltpu.VMEM((TURNS, n, gh, LANES), BF16),
            pltpu.VMEM((TURNS, work, gh, LANES), BF16),
            pltpu.SemaphoreType.DMA((2,)),
            pltpu.SemaphoreType.DMA((4,)),
        ],
        compiler_params=pltpu.CompilerParams(collective_id=0, has_side_effects=True),
        name="estimator",
    )(
        m_slots, cycle_order, colatitude, cycle_weight, m_slots.reshape(1, -1), tbar_alm,
        twf_alm, by_cycle, pixel_mask.reshape(mask_shape), *tables,
    )
    return pl.pallas_call(
        store_kernel,
        out_shape=(jax.ShapeDtypeStruct(tbar_alm.shape, F32),) * 2,
        in_specs=[vmem] * 2,
        out_specs=[anywhere] * 2,
        scratch_shapes=[pltpu.SemaphoreType.DMA],
        name="store",
    )(*(pltpu.with_memory_space_constraint(x, pltpu.VMEM) for x in made))


def body(n, *args):
    tbar_alm, legendre, pixel_mask = args[0], args[2], args[7]
    pairs, sims, _, rows = tbar_alm.shape
    cycles = legendre.shape[2]
    pixels = pixel_mask.shape[1]
    fits = (
        pairs == 8
        and cycles == n == 16
        and pixel_mask.shape[0] == 1
        and rows == 257
        and pairs * n == LANES
        and sims == 4
        and pixels == 4096
    )
    return fused(*args, n) if fits else shards(*args)


def solution(mesh):
    return jax.shard_map(
        functools.partial(body, mesh.shape["ma"]),
        mesh=mesh,
        in_specs=(
            P("ma", "grp", None, None),
            P("ma", "grp", None, None),
            P("ma", None, None),
            P(),
            P(),
            P(),
            P(),
            P("ma", None),
        ),
        out_specs=(P("ma", "grp", None, None), P("ma", "grp", None, None)),
        check_vma=False,
    )
```
